8 devices in a mesh: dp: 2 (over z, y), tp: 4 (over x, core).
Axes of the slice: x: 2, y: 2, z: 1, core: 2. Of those that a mesh axis runs over, the one named last changes fastest.
Arguments:
- layer_in: bfloat16 [4096, 1024], P(('dp', 'tp')), parts along dimension 0
- resid_mid: bfloat16 [4096, 1024], P(('dp', 'tp')), parts along dimension 0
- grad_out: bfloat16 [4096, 1024], P(('dp', 'tp')), parts along dimension 0
- ln1_gain: float32 [1024], replicated
- ln2_gain: float32 [1024], replicated
- w_qkv: bfloat16 [1024, 3072], P(None, 'tp')
- w_out: bfloat16 [16, 64, 1024], P('tp')
- w_fc1: bfloat16 [1024, 4096], P(None, 'tp')
- w_fc2: bfloat16 [4096, 1024], P('tp')
Outputs:
- output 1: bfloat16 [4096, 1024], P(('dp', 'tp')), parts along dimension 0
- output 2: bfloat16 [2048, 3072], P('dp', 'tp'), parts along dimension 0
- output 3: bfloat16 [32, 64, 1024], P(('dp', 'tp')), parts along dimension 0
- output 4: bfloat16 [2048, 4096], P('dp', 'tp'), parts along dimension 0
- output 5: bfloat16 [8192, 1024], P(('dp', 'tp')), parts along dimension 0
There are 2 independent parts. The reference program is written for one: setup_inputs(seed, part) draws one part's arguments, and reference() takes and returns one part's arrays. A program takes and returns all parts, laid end to end along the dimension named above; an argument that names none is the same for every part.
All inputs are finite; a program needn't handle non-finite values.
Results may differ from the reference program's by a relative error of at most 0.0151254.
Values are sent between devices in bfloat16 or wider.
A program may use at most 1 GiB of HBM per device.

```python
import jax
import jax.numpy as jnp
from jax import lax

D = 1024
HEADS = 16
HEAD = 64
FF = 4096
TOKENS = 2048
LN_EPS = 1e-5
GELU_COEF = 0.044715
GELU_SCALE = 0.7978845608028654


def ln_forward(rows):
    row_mean = jnp.mean(rows, axis=-1, keepdims=True)
    centered = rows - row_mean
    row_rstd = lax.rsqrt(jnp.mean(centered * centered, axis=-1, keepdims=True) + LN_EPS)
    return centered * row_rstd, row_rstd


def ln_backward(x_hat, row_rstd, ln_gain, grad_norm):
    grad_hat = grad_norm * ln_gain
    proj_one = jnp.mean(grad_hat, axis=-1, keepdims=True)
    proj_two = jnp.mean(grad_hat * x_hat, axis=-1, keepdims=True)
    return row_rstd * (grad_hat - proj_one - x_hat * proj_two)


def gelu_pair(pre_act):
    tanh_val = jnp.tanh(GELU_SCALE * (pre_act + GELU_COEF * pre_act * pre_act * pre_act))
    gelu_val = 0.5 * pre_act * (1.0 + tanh_val)
    gelu_der = 0.5 * (1.0 + tanh_val) + 0.5 * pre_act * (1.0 - tanh_val * tanh_val) * GELU_SCALE * (1.0 + 3.0 * GELU_COEF * pre_act * pre_act)
    return gelu_val, gelu_der


def head_grads(head_args):
    qkv_head, grad_attn = head_args
    q_rows = qkv_head[0]
    k_rows = qkv_head[1]
    v_rows = qkv_head[2]
    score_scale = HEAD ** -0.5
    scores = jnp.dot(q_rows, k_rows.T, preferred_element_type=jnp.float32) * score_scale
    causal = jnp.arange(TOKENS)[:, None] >= jnp.arange(TOKENS)[None, :]
    attn_prob = jax.nn.softmax(jnp.where(causal, scores, -1e30), axis=-1)
    prob_low = attn_prob.astype(jnp.bfloat16)
    attn_out = jnp.dot(prob_low, v_rows, preferred_element_type=jnp.float32).astype(jnp.bfloat16)
    grad_v = jnp.dot(prob_low.T, grad_attn, preferred_element_type=jnp.float32).astype(jnp.bfloat16)
    grad_prob = jnp.dot(grad_attn, v_rows.T, preferred_element_type=jnp.float32)
    row_dot = jnp.sum(attn_prob * grad_prob, axis=-1, keepdims=True)
    grad_score = (attn_prob * (grad_prob - row_dot) * score_scale).astype(jnp.bfloat16)
    grad_q = jnp.dot(grad_score, k_rows, preferred_element_type=jnp.float32).astype(jnp.bfloat16)
    grad_k = jnp.dot(grad_score.T, q_rows, preferred_element_type=jnp.float32).astype(jnp.bfloat16)
    return attn_out, jnp.stack([grad_q, grad_k, grad_v])


def setup_inputs(seed: int = 0, part: int = 0) -> dict:
    part_keys = jax.random.split(jax.random.fold_in(jax.random.key(seed), part), 3)
    shared_keys = jax.random.split(jax.random.key(seed + 1), 6)
    col_kind = (jnp.arange(3 * D) // HEAD) % 3
    qk_scale = jnp.where(col_kind < 2, 1.6, 1.0)
    return {
        'layer_in': jax.random.normal(part_keys[0], (TOKENS, D), jnp.float32).astype(jnp.bfloat16),
        'resid_mid': jax.random.normal(part_keys[1], (TOKENS, D), jnp.float32).astype(jnp.bfloat16),
        'grad_out': jax.random.normal(part_keys[2], (TOKENS, D), jnp.float32).astype(jnp.bfloat16),
        'ln1_gain': 1.0 + 0.25 * jax.random.normal(shared_keys[0], (D,), jnp.float32),
        'ln2_gain': 1.0 + 0.25 * jax.random.normal(shared_keys[1], (D,), jnp.float32),
        'w_qkv': (jax.random.normal(shared_keys[2], (D, 3 * D), jnp.float32) * qk_scale * D ** -0.5).astype(jnp.bfloat16),
        'w_out': (jax.random.normal(shared_keys[3], (HEADS, HEAD, D), jnp.float32) * D ** -0.5).astype(jnp.bfloat16),
        'w_fc1': (jax.random.normal(shared_keys[4], (D, FF), jnp.float32) * D ** -0.5).astype(jnp.bfloat16),
        'w_fc2': (jax.random.normal(shared_keys[5], (FF, D), jnp.float32) * FF ** -0.5).astype(jnp.bfloat16),
    }


def reference(layer_in, resid_mid, grad_out, ln1_gain, ln2_gain, w_qkv, w_out, w_fc1, w_fc2):
    mid_hat, mid_rstd = ln_forward(resid_mid.astype(jnp.float32))
    ln2_out = (mid_hat * ln2_gain).astype(jnp.bfloat16)
    pre_act = jnp.dot(ln2_out, w_fc1, preferred_element_type=jnp.float32)
    gelu_val, gelu_der = gelu_pair(pre_act)
    act_low = gelu_val.astype(jnp.bfloat16)
    grad_wfc2 = jnp.dot(act_low.T, grad_out, preferred_element_type=jnp.float32).astype(jnp.bfloat16)
    grad_act = jnp.dot(grad_out, w_fc2.T, preferred_element_type=jnp.float32)
    grad_pre = (grad_act * gelu_der).astype(jnp.bfloat16)
    grad_wfc1 = jnp.dot(ln2_out.T, grad_pre, preferred_element_type=jnp.float32).astype(jnp.bfloat16)
    grad_norm2 = jnp.dot(grad_pre, w_fc1.T, preferred_element_type=jnp.float32)
    grad_mid = grad_out.astype(jnp.float32) + ln_backward(mid_hat, mid_rstd, ln2_gain, grad_norm2)
    grad_mid_low = grad_mid.astype(jnp.bfloat16)
    in_hat, in_rstd = ln_forward(layer_in.astype(jnp.float32))
    ln1_out = (in_hat * ln1_gain).astype(jnp.bfloat16)
    qkv_rows = jnp.dot(ln1_out, w_qkv, preferred_element_type=jnp.float32).astype(jnp.bfloat16)
    qkv_heads = qkv_rows.reshape(TOKENS, HEADS, 3, HEAD).transpose(1, 2, 0, 3)
    grad_attn = jnp.dot(grad_mid_low, w_out.reshape(D, D).T, preferred_element_type=jnp.float32).astype(jnp.bfloat16)
    grad_attn_heads = grad_attn.reshape(TOKENS, HEADS, HEAD).transpose(1, 0, 2)
    attn_heads, grad_qkv_heads = lax.map(head_grads, (qkv_heads, grad_attn_heads))
    attn_out = attn_heads.transpose(1, 0, 2).reshape(TOKENS, D)
    grad_qkv = grad_qkv_heads.transpose(2, 0, 1, 3).reshape(TOKENS, 3 * D)
    grad_wout = jnp.dot(attn_out.T, grad_mid_low, preferred_element_type=jnp.float32).astype(jnp.bfloat16).reshape(HEADS, HEAD, D)
    grad_wqkv = jnp.dot(ln1_out.T, grad_qkv, preferred_element_type=jnp.float32).astype(jnp.bfloat16)
    grad_norm1 = jnp.dot(grad_qkv, w_qkv.T, preferred_element_type=jnp.float32)
    grad_in = (grad_mid + ln_backward(in_hat, in_rstd, ln1_gain, grad_norm1)).astype(jnp.bfloat16)
    return (grad_in, grad_wqkv, grad_wout, grad_wfc1, grad_wfc2)
```

```python
import jax
import jax.numpy as jnp
from jax import lax
from jax.experimental import pallas as pl
from jax.experimental.pallas import tpu as pltpu
from jax.sharding import PartitionSpec as P

LN_EPS = 1e-5
GELU_COEF = 0.044715
GELU_SCALE = 0.7978845608028654
LOG2E = 1.4426950408889634
F32 = jnp.float32
BF16 = jnp.bfloat16
BLK = 512


def ln_forward(rows):
    row_mean = jnp.mean(rows, axis=-1, keepdims=True)
    centered = rows - row_mean
    row_rstd = lax.rsqrt(jnp.mean(centered * centered, axis=-1, keepdims=True) + LN_EPS)
    return centered * row_rstd, row_rstd


def ln_backward(x_hat, row_rstd, ln_gain, grad_norm):
    grad_hat = grad_norm * ln_gain
    proj_one = jnp.mean(grad_hat, axis=-1, keepdims=True)
    proj_two = jnp.mean(grad_hat * x_hat, axis=-1, keepdims=True)
    return row_rstd * (grad_hat - proj_one - x_hat * proj_two)


def gelu_pair(pre_act):
    tanh_val = jnp.tanh(GELU_SCALE * (pre_act + GELU_COEF * pre_act * pre_act * pre_act))
    gelu_val = 0.5 * pre_act * (1.0 + tanh_val)
    gelu_der = 0.5 * (1.0 + tanh_val) + 0.5 * pre_act * (1.0 - tanh_val * tanh_val) * GELU_SCALE * (1.0 + 3.0 * GELU_COEF * pre_act * pre_act)
    return gelu_val, gelu_der


def nn(a, b):
    return lax.dot_general(a, b, (((1,), (0,)), ((), ())), preferred_element_type=F32)


def nt(a, b):
    return lax.dot_general(a, b, (((1,), (1,)), ((), ())), preferred_element_type=F32)


def qkv_block(i, n1, wqkvt, ct, nat):
    sl = pl.ds(pl.multiple_of(i * BLK, BLK), BLK)
    for n in range(4):
        c = nt(wqkvt[n * 192:(n + 1) * 192, :], n1[sl, :]).astype(BF16)
        for j in range(3):
            part = c[j * 64:(j + 1) * 64, :]
            if j == 0:
                part = part * jnp.asarray(0.125, BF16)
            ct[(3 * n + j) * 64:(3 * n + j + 1) * 64, sl] = part
            nat[3 * n + j, sl, :] = part.T


def attn_fwd_block(qi, ct, nat, ot, stat):
    qs = pl.ds(pl.multiple_of(qi * BLK, BLK), BLK)
    for h in range(4):
        ot[h * 64:(h + 1) * 64, qs] = jnp.zeros((64, BLK), F32)
        stat[h:h + 1, qs] = jnp.full((1, BLK), -1e30, F32)
        stat[4 + h:5 + h, qs] = jnp.zeros((1, BLK), F32)

    def tile(ki, diag):
        ks = pl.ds(pl.multiple_of(ki * BLK, BLK), BLK)
        for h in range(4):
            s = nn(nat[3 * h + 1, ks, :], ct[3 * h * 64:3 * h * 64 + 64, qs])
            if diag:
                key = lax.broadcasted_iota(jnp.int32, (BLK, BLK), 0)
                query = lax.broadcasted_iota(jnp.int32, (BLK, BLK), 1)
                s = jnp.where(key <= query, s, -1e30)
            m_old = stat[h:h + 1, qs]
            m_new = jnp.maximum(m_old, jnp.max(s, axis=0, keepdims=True))
            alpha = jnp.exp2((m_old - m_new) * LOG2E)
            e = jnp.exp2((s - m_new) * LOG2E)
            stat[h:h + 1, qs] = m_new
            stat[4 + h:5 + h, qs] = stat[4 + h:5 + h, qs] * alpha + jnp.sum(e, axis=0, keepdims=True)
            hs = slice(h * 64, (h + 1) * 64)
            vt = ct[(3 * h + 2) * 64:(3 * h + 3) * 64, ks]
            ot[hs, qs] = ot[hs, qs] * alpha + nn(vt, e.astype(BF16))

    @pl.loop(0, qi)
    def _(ki):
        tile(ki, False)

    tile(qi, True)
    for h in range(4):
        inv = 1.0 / stat[4 + h:5 + h, qs]
        stat[4 + h:5 + h, qs] = inv
        ot[h * 64:(h + 1) * 64, qs] = ot[h * 64:(h + 1) * 64, qs] * inv


def do_block(i, e, wo, ot, dot_t, nat, stat):
    sl = pl.ds(pl.multiple_of(i * BLK, BLK), BLK)
    d = nt(wo[...], e[sl, :]).astype(BF16)
    dot_t[:, sl] = d
    for h in range(4):
        part = d[h * 64:(h + 1) * 64, :]
        nat[12 + h, sl, :] = part.T
        stat[8 + h:9 + h, sl] = jnp.sum(part.astype(F32) * ot[h * 64:(h + 1) * 64, sl], axis=0, keepdims=True)


def attn_bwd_tile(ki, qi, diag, ct, nat, dot_t, stat, dqt, dk, dv):
    ks = pl.ds(pl.multiple_of(ki * BLK, BLK), BLK)
    qs = pl.ds(pl.multiple_of(qi * BLK, BLK), BLK)
    for h in range(4):
        s = nn(nat[3 * h + 1, ks, :], ct[3 * h * 64:3 * h * 64 + 64, qs])
        r = nn(nat[3 * h + 2, ks, :], dot_t[h * 64:(h + 1) * 64, qs])
        p = jnp.exp2((s - stat[h:h + 1, qs]) * LOG2E) * stat[4 + h:5 + h, qs]
        if diag:
            key = lax.broadcasted_iota(jnp.int32, (BLK, BLK), 0)
            query = lax.broadcasted_iota(jnp.int32, (BLK, BLK), 1)
            p = jnp.where(key <= query, p, 0.0)
        ds = (p * (r - stat[8 + h:9 + h, qs])).astype(BF16)
        dv[h, ks, :] += nn(p.astype(BF16), nat[12 + h, qs, :])
        dk[h, ks, :] += nn(ds, nat[3 * h, qs, :])
        hs = slice(h * 64, (h + 1) * 64)
        dqt[hs, qs] += nn(ct[(3 * h + 1) * 64:(3 * h + 2) * 64, ks], ds)


def pack_dc(i, dqt, dk, dv, dct):
    sl = pl.ds(pl.multiple_of(i * BLK, BLK), BLK)
    for h in range(4):
        dct[3 * h * 64:3 * h * 64 + 64, sl] = (dqt[h * 64:(h + 1) * 64, sl] * 0.125).astype(BF16)
        dct[(3 * h + 1) * 64:(3 * h + 2) * 64, sl] = dk[h, sl, :].astype(BF16).T
        dct[(3 * h + 2) * 64:(3 * h + 3) * 64, sl] = dv[h, sl, :].astype(BF16).T


def attn_kernel(n1, e, wqkvt, wo, dn1, dwqkv, dwo, ct, nat, dot_t, ot, stat, dqt, dk, dv, dct):
    tokens = n1.shape[0]
    blocks = tokens // BLK

    @pl.loop(0, blocks)
    def _(i):
        qkv_block(i, n1, wqkvt, ct, nat)

    @pl.loop(0, blocks)
    def _(i):
        attn_fwd_block(i, ct, nat, ot, stat)
        do_block(i, e, wo, ot, dot_t, nat, stat)

    dk[...] = jnp.zeros_like(dk)
    dv[...] = jnp.zeros_like(dv)
    dqt[...] = jnp.zeros_like(dqt)

    @pl.loop(0, blocks)
    def _(qi):
        @pl.loop(0, qi)
        def _(ki):
            attn_bwd_tile(ki, qi, False, ct, nat, dot_t, stat, dqt, dk, dv)

        attn_bwd_tile(qi, qi, True, ct, nat, dot_t, stat, dqt, dk, dv)

    @pl.loop(0, blocks)
    def _(i):
        pack_dc(i, dqt, dk, dv, dct)
        sl = pl.ds(pl.multiple_of(i * BLK, BLK), BLK)
        dn1[sl, :] = nn(dct[:, sl].T, wqkvt[...]).astype(BF16)

    @pl.loop(0, 4)
    def _(i):
        sl = pl.ds(pl.multiple_of(i * 256, 256), 256)
        dwo[:, sl] = nn(ot[...].astype(BF16), e[:, sl]).astype(BF16)
        dwqkv[sl, :] = nn(dct[...], n1[:, sl]).astype(BF16).T


def attention(n1, e, wqkvt, wo):
    tokens = n1.shape[0]
    return pl.pallas_call(
        attn_kernel,
        name="attn",
        out_shape=(jax.ShapeDtypeStruct((tokens, 1024), BF16), jax.ShapeDtypeStruct((1024, 768), BF16), jax.ShapeDtypeStruct((256, 1024), BF16)),
        in_specs=[pl.BlockSpec(memory_space=pltpu.VMEM)] * 4,
        out_specs=[pl.BlockSpec(memory_space=pltpu.VMEM)] * 3,
        scratch_shapes=[
            pltpu.VMEM((768, tokens), BF16),
            pltpu.VMEM((16, tokens, 64), BF16),
            pltpu.VMEM((256, tokens), BF16),
            pltpu.VMEM((256, tokens), F32),
            pltpu.VMEM((16, tokens), F32),
            pltpu.VMEM((256, tokens), F32),
            pltpu.VMEM((4, tokens, 64), F32),
            pltpu.VMEM((4, tokens, 64), F32),
            pltpu.VMEM((768, tokens), BF16),
        ],
        compiler_params=pltpu.CompilerParams(vmem_limit_bytes=62 * 1024 * 1024),
        cost_estimate=pl.CostEstimate(flops=40_000_000_000, bytes_accessed=16_000_000, transcendentals=20_000_000),
    )(n1, e, wqkvt, wo)


def solution(mesh):
    row_spec = P(('dp', 'tp'), None)
    in_specs = (row_spec, row_spec, row_spec, P(None), P(None), P(None, 'tp'), P('tp', None, None), P(None, 'tp'), P('tp', None))
    out_specs = (row_spec, P('dp', 'tp'), P(('dp', 'tp'), None, None), P('dp', 'tp'), P(('dp', 'tp'), None))

    def device_step(in_rows, mid_rows, gout_rows, ln1_gain, ln2_gain, wqkv_loc, wout_loc, wfc1_loc, wfc2_loc):
        mid_hat, mid_rstd = ln_forward(mid_rows.astype(jnp.float32))
        ln2_loc = (mid_hat * ln2_gain).astype(jnp.bfloat16)
        ln2_all = lax.all_gather(ln2_loc, 'tp', axis=0, tiled=True)
        gout_all = lax.all_gather(gout_rows, 'tp', axis=0, tiled=True)
        pre_act = jnp.dot(ln2_all, wfc1_loc, preferred_element_type=jnp.float32)
        gelu_val, gelu_der = gelu_pair(pre_act)
        act_low = gelu_val.astype(jnp.bfloat16)
        grad_wfc2 = jnp.einsum('tf,tm->fm', act_low, gout_all, preferred_element_type=jnp.float32).astype(jnp.bfloat16)
        grad_act = jnp.einsum('tm,fm->tf', gout_all, wfc2_loc, preferred_element_type=jnp.float32)
        grad_pre = (grad_act * gelu_der).astype(jnp.bfloat16)
        grad_wfc1 = jnp.einsum('tm,tf->mf', ln2_all, grad_pre, preferred_element_type=jnp.float32).astype(jnp.bfloat16)
        norm2_part = jnp.einsum('tf,mf->tm', grad_pre, wfc1_loc, preferred_element_type=jnp.float32).astype(jnp.bfloat16)
        grad_norm2 = lax.psum_scatter(norm2_part, 'tp', scatter_dimension=0, tiled=True)
        grad_mid = gout_rows.astype(jnp.float32) + ln_backward(mid_hat, mid_rstd, ln2_gain, grad_norm2.astype(jnp.float32))
        in_hat, in_rstd = ln_forward(in_rows.astype(jnp.float32))
        ln1_loc = (in_hat * ln1_gain).astype(jnp.bfloat16)
        ln1_all = lax.all_gather(ln1_loc, 'tp', axis=0, tiled=True)
        grad_mid_all = lax.all_gather(grad_mid.astype(jnp.bfloat16), 'tp', axis=0, tiled=True)
        norm1_part, grad_wqkv, grad_wout = attention(ln1_all, grad_mid_all, wqkv_loc.T, wout_loc.reshape(256, 1024))
        grad_norm1 = lax.psum_scatter(norm1_part, 'tp', scatter_dimension=0, tiled=True)
        grad_in = (grad_mid + ln_backward(in_hat, in_rstd, ln1_gain, grad_norm1.astype(jnp.float32))).astype(jnp.bfloat16)
        return grad_in, grad_wqkv, grad_wout.reshape(4, 64, 1024), grad_wfc1, grad_wfc2

    return jax.shard_map(device_step, mesh=mesh, in_specs=in_specs, out_specs=out_specs, check_vma=False)
```

```python
import jax
import jax.numpy as jnp
from jax import lax
from jax.experimental import pallas as pl
from jax.experimental.pallas import tpu as pltpu
from jax.sharding import PartitionSpec as P

LN_EPS = 1e-5
GELU_COEF = 0.044715
GELU_SCALE = 0.7978845608028654
LOG2E = 1.4426950408889634
F32 = jnp.float32
BF16 = jnp.bfloat16
BLK = 512


def ln_forward(rows):
    row_mean = jnp.mean(rows, axis=-1, keepdims=True)
    centered = rows - row_mean
    row_rstd = lax.rsqrt(jnp.mean(centered * centered, axis=-1, keepdims=True) + LN_EPS)
    return centered * row_rstd, row_rstd


def ln_backward(x_hat, row_rstd, ln_gain, grad_norm):
    grad_hat = grad_norm * ln_gain
    proj_one = jnp.mean(grad_hat, axis=-1, keepdims=True)
    proj_two = jnp.mean(grad_hat * x_hat, axis=-1, keepdims=True)
    return row_rstd * (grad_hat - proj_one - x_hat * proj_two)


def gelu_pair(pre_act):
    tanh_val = jnp.tanh(GELU_SCALE * (pre_act + GELU_COEF * pre_act * pre_act * pre_act))
    gelu_val = 0.5 * pre_act * (1.0 + tanh_val)
    gelu_der = 0.5 * (1.0 + tanh_val) + 0.5 * pre_act * (1.0 - tanh_val * tanh_val) * GELU_SCALE * (1.0 + 3.0 * GELU_COEF * pre_act * pre_act)
    return gelu_val, gelu_der


def nn(a, b):
    return lax.dot_general(a, b, (((1,), (0,)), ((), ())), preferred_element_type=F32)


def nt(a, b):
    return lax.dot_general(a, b, (((1,), (1,)), ((), ())), preferred_element_type=F32)


def qkv_block(i, n1, wqkvt, ct, nat):
    sl = pl.ds(pl.multiple_of(i * BLK, BLK), BLK)
    for n in range(4):
        c = nt(wqkvt[n * 192:(n + 1) * 192, :], n1[sl, :]).astype(BF16)
        for j in range(3):
            part = c[j * 64:(j + 1) * 64, :]
            if j == 0:
                part = part * jnp.asarray(0.125, BF16)
            ct[(3 * n + j) * 64:(3 * n + j + 1) * 64, sl] = part
            nat[3 * n + j, sl, :] = part.T


def attn_fwd_block(qi, ct, nat, ot, stat):
    qs = pl.ds(pl.multiple_of(qi * BLK, BLK), BLK)
    for h in range(4):
        ot[h * 64:(h + 1) * 64, qs] = jnp.zeros((64, BLK), F32)
        stat[h:h + 1, qs] = jnp.full((1, BLK), -1e30, F32)
        stat[4 + h:5 + h, qs] = jnp.zeros((1, BLK), F32)

    def tile(ki, diag):
        ks = pl.ds(pl.multiple_of(ki * BLK, BLK), BLK)
        for h in range(4):
            s = nn(nat[3 * h + 1, ks, :], ct[3 * h * 64:3 * h * 64 + 64, qs])
            if diag:
                key = lax.broadcasted_iota(jnp.int32, (BLK, BLK), 0)
                query = lax.broadcasted_iota(jnp.int32, (BLK, BLK), 1)
                s = jnp.where(key <= query, s, -1e30)
            m_old = stat[h:h + 1, qs]
            m_new = jnp.maximum(m_old, jnp.max(s, axis=0, keepdims=True))
            alpha = jnp.exp2((m_old - m_new) * LOG2E)
            e = jnp.exp2((s - m_new) * LOG2E)
            stat[h:h + 1, qs] = m_new
            stat[4 + h:5 + h, qs] = stat[4 + h:5 + h, qs] * alpha + jnp.sum(e, axis=0, keepdims=True)
            hs = slice(h * 64, (h + 1) * 64)
            vt = ct[(3 * h + 2) * 64:(3 * h + 3) * 64, ks]
            ot[hs, qs] = ot[hs, qs] * alpha + nn(vt, e.astype(BF16))

    @pl.loop(0, qi)
    def _(ki):
        tile(ki, False)

    tile(qi, True)
    for h in range(4):
        inv = 1.0 / stat[4 + h:5 + h, qs]
        stat[4 + h:5 + h, qs] = inv
        ot[h * 64:(h + 1) * 64, qs] = ot[h * 64:(h + 1) * 64, qs] * inv


def do_block(i, e, wo, ot, dot_t, nat_do, stat):
    sl = pl.ds(pl.multiple_of(i * BLK, BLK), BLK)
    d = nt(wo[...], e[sl, :]).astype(BF16)
    dot_t[:, sl] = d
    for h in range(4):
        part = d[h * 64:(h + 1) * 64, :]
        nat_do[h, sl, :] = part.T
        stat[8 + h:9 + h, sl] = jnp.sum(part.astype(F32) * ot[h * 64:(h + 1) * 64, sl], axis=0, keepdims=True)


def attn_bwd_tile(ki, qi, diag, ct, nat, nat_do, dot_t, stat, dqt, dk, dv):
    ks = pl.ds(pl.multiple_of(ki * BLK, BLK), BLK)
    qs = pl.ds(pl.multiple_of(qi * BLK, BLK), BLK)
    for h in range(4):
        s = nn(nat[3 * h + 1, ks, :], ct[3 * h * 64:3 * h * 64 + 64, qs])
        r = nn(nat[3 * h + 2, ks, :], dot_t[h * 64:(h + 1) * 64, qs])
        p = jnp.exp2((s - stat[h:h + 1, qs]) * LOG2E) * stat[4 + h:5 + h, qs]
        if diag:
            key = lax.broadcasted_iota(jnp.int32, (BLK, BLK), 0)
            query = lax.broadcasted_iota(jnp.int32, (BLK, BLK), 1)
            p = jnp.where(key <= query, p, 0.0)
        ds = (p * (r - stat[8 + h:9 + h, qs])).astype(BF16)
        dv[h, ks, :] += nn(p.astype(BF16), nat_do[h, qs, :])
        dk[h, ks, :] += nn(ds, nat[3 * h, qs, :])
        hs = slice(h * 64, (h + 1) * 64)
        dqt[hs, qs] += nn(ct[(3 * h + 1) * 64:(3 * h + 2) * 64, ks], ds)


def pack_dc(i, dqt, dk, dv, dct):
    sl = pl.ds(pl.multiple_of(i * BLK, BLK), BLK)
    for h in range(4):
        dct[3 * h * 64:3 * h * 64 + 64, sl] = (dqt[h * 64:(h + 1) * 64, sl] * 0.125).astype(BF16)
        dct[(3 * h + 1) * 64:(3 * h + 2) * 64, sl] = dk[h, sl, :].astype(BF16).T
        dct[(3 * h + 2) * 64:(3 * h + 3) * 64, sl] = dv[h, sl, :].astype(BF16).T


MESH_ID = pl.DeviceIdType.MESH


def place():
    me = lax.axis_index('tp')
    chip = me // 2
    core = me - chip * 2
    return me, chip, core, chip * 2 + (1 - core), (1 - chip) * 2 + core, (1 - chip) * 2 + (1 - core)


def entry_barrier(others):
    barrier = pltpu.get_barrier_semaphore()
    for other in others:
        pl.semaphore_signal(barrier, inc=1, device_id={'tp': other}, device_id_type=MESH_ID)
    pl.semaphore_wait(barrier, 3)


def send(src, dst, ssem, rsem, to):
    return pltpu.make_async_remote_copy(src_ref=src, dst_ref=dst, send_sem=ssem, recv_sem=rsem, device_id={'tp': to}, device_id_type=MESH_ID)


def rows(start, size):
    return pl.ds(pl.multiple_of(start, size), size)


def fwd_kernel(n1, wqkvt, ct, nat, ot, stat):
    blocks = n1.shape[0] // BLK

    @pl.loop(0, blocks)
    def _(i):
        qkv_block(i, n1, wqkvt, ct, nat)

    @pl.loop(0, blocks)
    def _(i):
        attn_fwd_block(i, ct, nat, ot, stat)


def attention_fwd(n1, wqkvt):
    tokens = n1.shape[0]
    return pl.pallas_call(
        fwd_kernel,
        name="attn_fwd",
        out_shape=(jax.ShapeDtypeStruct((768, tokens), BF16), jax.ShapeDtypeStruct((12, tokens, 64), BF16), jax.ShapeDtypeStruct((256, tokens), F32), jax.ShapeDtypeStruct((16, tokens), F32)),
        in_specs=[pl.BlockSpec(memory_space=pltpu.VMEM)] * 2,
        out_specs=[pl.BlockSpec(memory_space=pltpu.VMEM)] * 4,
        compiler_params=pltpu.CompilerParams(vmem_limit_bytes=48 * 1024 * 1024),
        cost_estimate=pl.CostEstimate(flops=20_000_000_000, bytes_accessed=16_000_000, transcendentals=20_000_000),
    )(n1, wqkvt)


def bwd_kernel(e_own, dh1_hbm, x_hbm, gain, n1_hbm, ct_hbm, nat_hbm, ot_hbm, stat_hbm, wqkvt_hbm, wo_hbm,
               dx_hbm, dwqkv_hbm, dwo_hbm,
               e, n1, ct, nat, nat_do, ot, stat, dot_t, dqt, dk, dv, dct, dct_far, dct_own, w_own, w_pair, wo, part, d1_send, d1_recv,
               dh1, x, dx, dwqkv, dwo, lsem, ssem, rsem):
    me, chip, core, pair, peer, diag = place()
    own = rows(me * BLK, BLK)

    local = []
    for n, (src, dst) in enumerate(((e_own, e.at[own, :]), (wo_hbm, wo), (ot_hbm, ot), (stat_hbm, stat), (ct_hbm, ct), (nat_hbm, nat), (wqkvt_hbm, w_own), (n1_hbm, n1), (x_hbm, x), (dh1_hbm, dh1))):
        copy = pltpu.make_async_copy(src, dst, lsem.at[n])
        copy.start()
        local.append(copy)
    l_e, l_wo, l_ot, l_stat, l_ct, l_nat, l_w, l_n1, l_x, l_dh1 = local

    entry_barrier((pair, peer, diag))
    l_e.wait()
    to_pair = send(e.at[own, :], e.at[own, :], ssem.at[0], rsem.at[0], pair)
    to_pair.start()
    half = BLK // 2
    to_peer = []
    for n in range(2):
        chunk = rows(me * BLK + n * half, half)
        copy = send(e.at[chunk, :], e.at[chunk, :], ssem.at[1 + n], rsem.at[1 + n], peer)
        copy.start()
        to_peer.append(copy)
    l_w.wait()
    w_swap = send(w_own, w_pair, ssem.at[5], rsem.at[5], pair)
    w_swap.start()

    dk[...] = jnp.zeros_like(dk)
    dv[...] = jnp.zeros_like(dv)
    dqt[...] = jnp.zeros_like(dqt)
    for copy in (l_wo, l_ot, l_stat, l_ct, l_nat):
        copy.wait()

    def query_block(qi):
        @pl.loop(0, qi)
        def _(ki):
            attn_bwd_tile(ki, qi, False, ct, nat, nat_do, dot_t, stat, dqt, dk, dv)

        attn_bwd_tile(qi, qi, True, ct, nat, nat_do, dot_t, stat, dqt, dk, dv)

    do_block(me, e, wo, ot, dot_t, nat_do, stat)
    to_pair.wait_recv()
    do_block(pair, e, wo, ot, dot_t, nat_do, stat)

    @pl.loop(0, 2)
    def _(n):
        query_block(chip * 2 + n)

    forward = []
    for n in range(2):
        to_peer[n].wait_recv()
        chunk = rows(peer * BLK + n * half, half)
        copy = send(e.at[chunk, :], e.at[chunk, :], ssem.at[3 + n], rsem.at[3 + n], pair)
        copy.start()
        forward.append(copy)
    do_block(peer, e, wo, ot, dot_t, nat_do, stat)
    for copy in forward:
        copy.wait_recv()
    do_block(diag, e, wo, ot, dot_t, nat_do, stat)
    w_swap.wait_recv()

    far = (1 - chip) * 2
    for n in range(2):
        block = far + 1 - n
        query_block(block)
        pack_dc(block, dqt, dk, dv, dct)
        mine = rows(block * BLK + core * half, half)
        theirs = rows(block * BLK + (1 - core) * half, half)
        swap = send(dct.at[:, theirs], dct_far.at[n], ssem.at[6 + n], rsem.at[6 + n], pair)
        swap.start()
        part[0:half, :] = nn(dct[:, mine].T, w_own[...])
        swap.wait_recv()
        d1_send[n] = (part[0:half, :] + nn(dct_far[n].T, w_pair[...])).astype(BF16)
        out = send(d1_send.at[n], d1_recv.at[core], ssem.at[9 + n], rsem.at[9 + core], block)
        out.start()
        swap.wait_send()

    for n in range(2):
        pack_dc(chip * 2 + n, dqt, dk, dv, dct)
    swap = send(dct.at[:, rows(pair * BLK, BLK)], dct_own, ssem.at[8], rsem.at[8], pair)
    swap.start()
    part[...] = nn(dct[:, own].T, w_own[...])
    swap.wait_recv()
    part[...] += nn(dct_own[...].T, w_pair[...])
    l_n1.wait()

    @pl.loop(0, 4)
    def _(i):
        sl = rows(i * 256, 256)
        dwo[:, sl] = nn(ot[...].astype(BF16), e[:, sl]).astype(BF16)
        dwqkv[sl, :] = nn(dct[...], n1[:, sl]).astype(BF16).T

    out_wqkv = pltpu.make_async_copy(dwqkv, dwqkv_hbm, lsem.at[10])
    out_wqkv.start()
    out_wo = pltpu.make_async_copy(dwo, dwo_hbm, lsem.at[11])
    out_wo.start()
    l_x.wait()
    l_dh1.wait()
    for n in range(2):
        send(d1_send.at[n], d1_recv.at[n], ssem.at[9 + n], rsem.at[9 + n], peer).wait_recv()
        sl = slice(n * half, (n + 1) * half)
        x_hat, rstd = ln_forward(x[sl, :].astype(F32))
        grad = part[sl, :] + d1_recv[n].astype(F32)
        dx[sl, :] = (dh1[sl, :] + ln_backward(x_hat, rstd, gain[...], grad)).astype(BF16)
    out_dx = pltpu.make_async_copy(dx, dx_hbm, lsem.at[12])
    out_dx.start()

    to_pair.wait_send()
    for copy in to_peer + forward:
        copy.wait_send()
    w_swap.wait_send()
    swap.wait_send()
    for n in range(2):
        send(d1_send.at[n], d1_recv.at[n], ssem.at[9 + n], rsem.at[9 + n], peer).wait_send()
    out_wqkv.wait()
    out_wo.wait()
    out_dx.wait()


def attention_bwd(e_own, dh1, x, gain, n1, ct, nat, ot, stat, wqkvt, wo):
    tokens = n1.shape[0]
    vmem = pltpu.VMEM
    return pl.pallas_call(
        bwd_kernel,
        name="attn_bwd",
        out_shape=(jax.ShapeDtypeStruct((BLK, 1024), BF16), jax.ShapeDtypeStruct((1024, 768), BF16), jax.ShapeDtypeStruct((256, 1024), BF16)),
        in_specs=[pl.BlockSpec(memory_space=pl.ANY)] * 3 + [pl.BlockSpec(memory_space=vmem)] + [pl.BlockSpec(memory_space=pl.ANY)] * 7,
        out_specs=[pl.BlockSpec(memory_space=pl.ANY)] * 3,
        scratch_shapes=[
            vmem((tokens, 1024), BF16),
            vmem((tokens, 1024), BF16),
            vmem((768, tokens), BF16),
            vmem((12, tokens, 64), BF16),
            vmem((4, tokens, 64), BF16),
            vmem((256, tokens), F32),
            vmem((16, tokens), F32),
            vmem((256, tokens), BF16),
            vmem((256, tokens), F32),
            vmem((4, tokens, 64), F32),
            vmem((4, tokens, 64), F32),
            vmem((768, tokens), BF16),
            vmem((2, 768, BLK // 2), BF16),
            vmem((768, BLK), BF16),
            vmem((768, 1024), BF16),
            vmem((768, 1024), BF16),
            vmem((256, 1024), BF16),
            vmem((BLK, 1024), F32),
            vmem((2, BLK // 2, 1024), BF16),
            vmem((2, BLK // 2, 1024), BF16),
            vmem((BLK, 1024), F32),
            vmem((BLK, 1024), BF16),
            vmem((BLK, 1024), BF16),
            vmem((1024, 768), BF16),
            vmem((256, 1024), BF16),
            pltpu.SemaphoreType.DMA((13,)),
            pltpu.SemaphoreType.DMA((11,)),
            pltpu.SemaphoreType.DMA((11,)),
        ],
        compiler_params=pltpu.CompilerParams(collective_id=1, has_side_effects=True, vmem_limit_bytes=63 * 1024 * 1024),
        cost_estimate=pl.CostEstimate(flops=40_000_000_000, bytes_accessed=40_000_000, transcendentals=20_000_000),
    )(e_own, dh1, x, gain, n1, ct, nat, ot, stat, wqkvt, wo)

def solution(mesh):
    row_spec = P(('dp', 'tp'), None)
    in_specs = (row_spec, row_spec, row_spec, P(None), P(None), P(None, 'tp'), P('tp', None, None), P(None, 'tp'), P('tp', None))
    out_specs = (row_spec, P('dp', 'tp'), P(('dp', 'tp'), None, None), P('dp', 'tp'), P(('dp', 'tp'), None))

    def device_step(in_rows, mid_rows, gout_rows, ln1_gain, ln2_gain, wqkv_loc, wout_loc, wfc1_loc, wfc2_loc):
        mid_hat, mid_rstd = ln_forward(mid_rows.astype(jnp.float32))
        ln2_loc = (mid_hat * ln2_gain).astype(jnp.bfloat16)
        ln2_all = lax.all_gather(ln2_loc, 'tp', axis=0, tiled=True)
        gout_all = lax.all_gather(gout_rows, 'tp', axis=0, tiled=True)
        pre_act = jnp.dot(ln2_all, wfc1_loc, preferred_element_type=jnp.float32)
        gelu_val, gelu_der = gelu_pair(pre_act)
        act_low = gelu_val.astype(jnp.bfloat16)
        grad_wfc2 = jnp.einsum('tf,tm->fm', act_low, gout_all, preferred_element_type=jnp.float32).astype(jnp.bfloat16)
        grad_act = jnp.einsum('tm,fm->tf', gout_all, wfc2_loc, preferred_element_type=jnp.float32)
        grad_pre = (grad_act * gelu_der).astype(jnp.bfloat16)
        grad_wfc1 = jnp.einsum('tm,tf->mf', ln2_all, grad_pre, preferred_element_type=jnp.float32).astype(jnp.bfloat16)
        norm2_part = jnp.einsum('tf,mf->tm', grad_pre, wfc1_loc, preferred_element_type=jnp.float32).astype(jnp.bfloat16)
        grad_norm2 = lax.psum_scatter(norm2_part, 'tp', scatter_dimension=0, tiled=True)
        grad_mid = gout_rows.astype(jnp.float32) + ln_backward(mid_hat, mid_rstd, ln2_gain, grad_norm2.astype(jnp.float32))
        in_hat, in_rstd = ln_forward(in_rows.astype(jnp.float32))
        ln1_loc = (in_hat * ln1_gain).astype(jnp.bfloat16)
        ln1_all = lax.all_gather(ln1_loc, 'tp', axis=0, tiled=True)
        wqkvt = wqkv_loc.T
        ct, nat, ot, stat = attention_fwd(ln1_all, wqkvt)
        grad_in, grad_wqkv, grad_wout = attention_bwd(grad_mid.astype(BF16), grad_mid, in_rows, ln1_gain.reshape(1, 1024), ln1_all, ct, nat, ot, stat, wqkvt, wout_loc.reshape(256, 1024))
        return grad_in, grad_wqkv, grad_wout.reshape(4, 64, 1024), grad_wfc1, grad_wfc2

    return jax.shard_map(device_step, mesh=mesh, in_specs=in_specs, out_specs=out_specs, check_vma=False)
```

```python
import jax
import jax.numpy as jnp
from jax import lax
from jax.experimental import pallas as pl
from jax.experimental.pallas import tpu as pltpu
from jax.sharding import PartitionSpec as P

LN_EPS = 1e-5
GELU_COEF = 0.044715
GELU_SCALE = 0.7978845608028654
LOG2E = 1.4426950408889634
F32 = jnp.float32
BF16 = jnp.bfloat16
BLK = 512
HALF = 256


def ln_forward(rows):
    row_mean = jnp.mean(rows, axis=-1, keepdims=True)
    centered = rows - row_mean
    row_rstd = lax.rsqrt(jnp.mean(centered * centered, axis=-1, keepdims=True) + LN_EPS)
    return centered * row_rstd, row_rstd


def ln_backward(x_hat, row_rstd, ln_gain, grad_norm):
    grad_hat = grad_norm * ln_gain
    proj_one = jnp.mean(grad_hat, axis=-1, keepdims=True)
    proj_two = jnp.mean(grad_hat * x_hat, axis=-1, keepdims=True)
    return row_rstd * (grad_hat - proj_one - x_hat * proj_two)


def gelu_pair(pre_act):
    tanh_val = jnp.tanh(GELU_SCALE * (pre_act + GELU_COEF * pre_act * pre_act * pre_act))
    gelu_val = 0.5 * pre_act * (1.0 + tanh_val)
    gelu_der = 0.5 * (1.0 + tanh_val) + 0.5 * pre_act * (1.0 - tanh_val * tanh_val) * GELU_SCALE * (1.0 + 3.0 * GELU_COEF * pre_act * pre_act)
    return gelu_val, gelu_der


def nn(a, b):
    return lax.dot_general(a, b, (((1,), (0,)), ((), ())), preferred_element_type=F32)


def nt(a, b):
    return lax.dot_general(a, b, (((1,), (1,)), ((), ())), preferred_element_type=F32)


def qkv_block(i, n1, wqkvt, ct, nat):
    sl = pl.ds(pl.multiple_of(i * BLK, BLK), BLK)
    for n in range(4):
        c = nt(wqkvt[n * 192:(n + 1) * 192, :], n1[sl, :]).astype(BF16)
        for j in range(3):
            part = c[j * 64:(j + 1) * 64, :]
            if j == 0:
                part = part * jnp.asarray(0.125, BF16)
            ct[(3 * n + j) * 64:(3 * n + j + 1) * 64, sl] = part
            nat[3 * n + j, sl, :] = part.T


def fwd_init(ot, stat):
    ot[...] = jnp.zeros_like(ot)
    stat[0:4, :] = jnp.full((4, stat.shape[1]), -1e30, F32)
    stat[4:16, :] = jnp.zeros((12, stat.shape[1]), F32)


def fwd_tile(ki, qi, diag, ct, nat, ot, stat):
    qs = pl.ds(pl.multiple_of(qi * BLK, BLK), BLK)
    ks = pl.ds(pl.multiple_of(ki * BLK, BLK), BLK)
    for h in range(4):
        s = nn(nat[3 * h + 1, ks, :], ct[3 * h * 64:3 * h * 64 + 64, qs])
        if diag:
            key = lax.broadcasted_iota(jnp.int32, (BLK, BLK), 0)
            query = lax.broadcasted_iota(jnp.int32, (BLK, BLK), 1)
            s = jnp.where(key <= query, s, -1e30)
        m_old = stat[h:h + 1, qs]
        m_new = jnp.maximum(m_old, jnp.max(s, axis=0, keepdims=True))
        alpha = jnp.exp2((m_old - m_new) * LOG2E)
        e = jnp.exp2((s - m_new) * LOG2E)
        stat[h:h + 1, qs] = m_new
        stat[4 + h:5 + h, qs] = stat[4 + h:5 + h, qs] * alpha + jnp.sum(e, axis=0, keepdims=True)
        hs = slice(h * 64, (h + 1) * 64)
        vt = ct[(3 * h + 2) * 64:(3 * h + 3) * 64, ks]
        ot[hs, qs] = ot[hs, qs] * alpha + nn(vt, e.astype(BF16))


def fwd_finish(ot, stat):
    for h in range(4):
        inv = 1.0 / stat[4 + h:5 + h, :]
        stat[4 + h:5 + h, :] = inv
        ot[h * 64:(h + 1) * 64, :] = ot[h * 64:(h + 1) * 64, :] * inv


def do_block(i, e, wo, ot, dot_t, nat_do, stat):
    sl = pl.ds(pl.multiple_of(i * BLK, BLK), BLK)
    d = nt(wo[...], e[sl, :]).astype(BF16)
    dot_t[:, sl] = d
    for h in range(4):
        part = d[h * 64:(h + 1) * 64, :]
        nat_do[h, sl, :] = part.T
        stat[8 + h:9 + h, sl] = jnp.sum(part.astype(F32) * ot[h * 64:(h + 1) * 64, sl], axis=0, keepdims=True)


def attn_bwd_tile(ki, qi, diag, ct, nat, nat_do, dot_t, stat, dqt, dk, dv):
    ks = pl.ds(pl.multiple_of(ki * BLK, BLK), BLK)
    qs = pl.ds(pl.multiple_of(qi * BLK, BLK), BLK)
    for h in range(4):
        s = nn(nat[3 * h + 1, ks, :], ct[3 * h * 64:3 * h * 64 + 64, qs])
        r = nn(nat[3 * h + 2, ks, :], dot_t[h * 64:(h + 1) * 64, qs])
        p = jnp.exp2((s - stat[h:h + 1, qs]) * LOG2E) * stat[4 + h:5 + h, qs]
        if diag:
            key = lax.broadcasted_iota(jnp.int32, (BLK, BLK), 0)
            query = lax.broadcasted_iota(jnp.int32, (BLK, BLK), 1)
            p = jnp.where(key <= query, p, 0.0)
        ds = (p * (r - stat[8 + h:9 + h, qs])).astype(BF16)
        dv[h, ks, :] += nn(p.astype(BF16), nat_do[h, qs, :])
        dk[h, ks, :] += nn(ds, nat[3 * h, qs, :])
        hs = slice(h * 64, (h + 1) * 64)
        dqt[hs, qs] += nn(ct[(3 * h + 1) * 64:(3 * h + 2) * 64, ks], ds)


def pack_dc(i, dqt, dk, dv, dct):
    sl = pl.ds(pl.multiple_of(i * BLK, BLK), BLK)
    for h in range(4):
        dct[3 * h * 64:3 * h * 64 + 64, sl] = (dqt[h * 64:(h + 1) * 64, sl] * 0.125).astype(BF16)
        dct[(3 * h + 1) * 64:(3 * h + 2) * 64, sl] = dk[h, sl, :].astype(BF16).T
        dct[(3 * h + 2) * 64:(3 * h + 3) * 64, sl] = dv[h, sl, :].astype(BF16).T


MESH_ID = pl.DeviceIdType.MESH


def place():
    me = lax.axis_index('tp')
    chip = me // 2
    core = me - chip * 2
    return me, chip, core, chip * 2 + (1 - core), (1 - chip) * 2 + core, (1 - chip) * 2 + (1 - core)


def entry_barrier(others):
    barrier = pltpu.get_barrier_semaphore()
    for other in others:
        pl.semaphore_signal(barrier, inc=1, device_id={'tp': other}, device_id_type=MESH_ID)
    pl.semaphore_wait(barrier, 3)


def send(src, dst, ssem, rsem, to):
    return pltpu.make_async_remote_copy(src_ref=src, dst_ref=dst, send_sem=ssem, recv_sem=rsem, device_id={'tp': to}, device_id_type=MESH_ID)


def rows(start, size):
    return pl.ds(pl.multiple_of(start, size), size)


def tn(a, b):
    return lax.dot_general(a, b, (((0,), (0,)), ((), ())), preferred_element_type=F32)


def ln_rows(src, gain, dst, start):
    @pl.loop(0, 4)
    def _(i):
        hat, _ = ln_forward(src[rows(i * 128, 128), :].astype(F32))
        dst[rows(start + i * 128, 128), :] = (hat * gain[...]).astype(BF16)


def mlp_rows(start, n2, dy, w1, w2t, act, da):
    sl = rows(start, HALF)
    for c in range(4):
        cs = slice(c * 256, (c + 1) * 256)
        gelu_val, gelu_der = gelu_pair(nn(n2[sl, :], w1[:, cs]))
        act[sl, cs] = gelu_val.astype(BF16)
        da[sl, cs] = (nn(dy[sl, :], w2t[:, cs]) * gelu_der).astype(BF16)


def mlp_kernel(h1_hbm, dy_hbm, x_hbm, g1, g2, wqkv_hbm, w1_hbm, w2_hbm,
               e_hbm, dh1_hbm, n1_hbm, ct_hbm, nat_hbm, ot_hbm, stat_hbm, wqkvt_hbm, dw1_hbm, dw2_hbm,
               n2, dy, n1, w1, w1_pair, w2t, wqkv, wqkvt, act, da, da_pair, d2_send, d2_recv, h1, dh1, e, ct, nat, ot, stat, dw1, dw2,
               lsem, ssem, rsem):
    me, chip, core, pair, peer, diag = place()
    own = rows(me * BLK, BLK)
    local = []
    for n, (src, dst) in enumerate(((h1_hbm, h1), (x_hbm, e), (dy_hbm, dy.at[own, :]), (w1_hbm, w1), (w2_hbm, dw2), (wqkv_hbm, wqkv))):
        copy = pltpu.make_async_copy(src, dst, lsem.at[n])
        copy.start()
        local.append(copy)
    l_h1, l_x, l_dy, l_w1, l_w2, l_wqkv = local

    l_h1.wait()
    ln_rows(h1, g2, n2, me * BLK)
    l_x.wait()
    ln_rows(e, g1, n1, me * BLK)
    l_dy.wait()
    l_w1.wait()
    entry_barrier((pair, peer, diag))

    def chunk_copy(ref, block, n, first, to):
        sl = rows(block * BLK + n * HALF, HALF)
        return send(ref.at[sl, :], ref.at[sl, :], ssem.at[first + n], rsem.at[first + n], to)

    to_pair = [send(ref.at[own, :], ref.at[own, :], ssem.at[n], rsem.at[n], pair) for n, ref in enumerate((n2, dy, n1))]
    to_pair.append(send(w1, w1_pair, ssem.at[3], rsem.at[3], pair))
    to_pair[0].start()
    to_pair[1].start()
    for n in range(2):
        chunk_copy(n2, me, n, 4, peer).start()
        chunk_copy(dy, me, n, 6, peer).start()
    for n in range(2):
        chunk_copy(n1, me, n, 8, peer).start()
    to_pair[2].start()
    to_pair[3].start()

    l_w2.wait()
    w2t[...] = dw2[...].T

    @pl.loop(0, 4)
    def _(i):
        @pl.when(i == 2)
        def _():
            to_pair[0].wait_recv()
            to_pair[1].wait_recv()

        second = i // 2
        mlp_rows((me + second * (pair - me)) * BLK + (i - 2 * second) * HALF, n2, dy, w1, w2t, act, da)

    da_swap = send(da.at[rows(pair * BLK, BLK), :], da_pair.at[0:BLK, :], ssem.at[16], rsem.at[16], pair)
    da_swap.start()
    l_wqkv.wait()
    wqkvt[...] = wqkv[...].T
    out_w = pltpu.make_async_copy(wqkvt, wqkvt_hbm, lsem.at[6])
    out_w.start()
    fwd_init(ot, stat)
    to_pair[2].wait_recv()

    @pl.loop(0, 2)
    def _(n):
        qkv_block(chip * 2 + n, n1, wqkvt, ct, nat)

    def da_far(n):
        return send(da.at[rows(diag * BLK + n * HALF, HALF), :], da_pair.at[rows(BLK + n * HALF, HALF), :], ssem.at[17 + n], rsem.at[17 + n], pair)

    def d2_far(n):
        return send(d2_send.at[n], d2_recv.at[n], ssem.at[19 + n], rsem.at[19 + n], peer)

    to_pair[3].wait_recv()

    @pl.loop(0, 2)
    def _(n):
        chunk_copy(n2, peer, n, 4, peer).wait_recv()
        chunk_copy(n2, peer, n, 10, pair).start()
        chunk_copy(dy, peer, n, 6, peer).wait_recv()
        chunk_copy(dy, peer, n, 12, pair).start()

        @pl.loop(0, 2)
        def _(j):
            @pl.when(j == 1)
            def _():
                chunk_copy(n2, diag, n, 10, pair).wait_recv()
                chunk_copy(dy, diag, n, 12, pair).wait_recv()

            mlp_rows((peer + j * (diag - peer)) * BLK + n * HALF, n2, dy, w1, w2t, act, da)

        da_far(n).start()
        first = nt(da[rows(peer * BLK + n * HALF, HALF), :], w1[...])
        da_far(n).wait_recv()
        d2_send[n] = (first + nt(da_pair[rows(BLK + n * HALF, HALF), :], w1_pair[...])).astype(BF16)
        d2_far(n).start()

        @pl.when(n == 0)
        def _():
            da_swap.wait_recv()

            @pl.loop(0, 2)
            def _(i):
                sl = rows(i * HALF, HALF)
                dh1[sl, :] = nt(da[rows(me * BLK + i * HALF, HALF), :], w1[...]) + nt(da_pair[sl, :], w1_pair[...])

            @pl.loop(0, 2)
            def _(i):
                qi = chip * 2 + i

                @pl.loop(chip * 2, qi)
                def _(ki):
                    fwd_tile(ki, qi, False, ct, nat, ot, stat)

                fwd_tile(qi, qi, True, ct, nat, ot, stat)

    @pl.loop(0, 4)
    def _(i):
        sl = rows(i * 256, 256)
        dw2[sl, :] = tn(act[:, sl], dy[...]).astype(BF16)
        dw1[sl, :] = tn(n2[:, sl], da[...]).astype(BF16)

    outs = [out_w]
    for n, (src, dst) in enumerate(((dw1, dw1_hbm), (dw2, dw2_hbm))):
        outs.append(pltpu.make_async_copy(src, dst, lsem.at[7 + n]))
        outs[-1].start()

    for n in range(2):
        chunk_copy(n1, peer, n, 8, peer).wait_recv()
        chunk_copy(n1, peer, n, 14, pair).start()
    qkv_block(peer, n1, wqkvt, ct, nat)
    for n in range(2):
        chunk_copy(n1, diag, n, 14, pair).wait_recv()
    qkv_block(diag, n1, wqkvt, ct, nat)
    for n, (src, dst) in enumerate(((n1, n1_hbm), (ct, ct_hbm), (nat, nat_hbm))):
        outs.append(pltpu.make_async_copy(src, dst, lsem.at[9 + n]))
        outs[-1].start()

    @pl.loop(0, 4)
    def _(i):
        is_own = i // 2
        qi = (1 - chip) * 2 + is_own * (4 * chip - 2) + i - 2 * is_own

        @pl.loop(0, is_own * chip * 2 + (1 - is_own) * qi)
        def _(ki):
            fwd_tile(ki, qi, False, ct, nat, ot, stat)

        @pl.when(is_own == 0)
        def _():
            fwd_tile(qi, qi, True, ct, nat, ot, stat)

    fwd_finish(ot, stat)
    for n, (src, dst) in enumerate(((ot, ot_hbm), (stat, stat_hbm))):
        outs.append(pltpu.make_async_copy(src, dst, lsem.at[12 + n]))
        outs[-1].start()

    for n in range(2):
        d2_far(n).wait_recv()
        sl = slice(n * HALF, (n + 1) * HALF)
        hat, rstd = ln_forward(h1[sl, :].astype(F32))
        grad = dy[rows(me * BLK + n * HALF, HALF), :].astype(F32) + ln_backward(hat, rstd, g2[...], dh1[sl, :] + d2_recv[n].astype(F32))
        dh1[sl, :] = grad
        e[sl, :] = grad.astype(BF16)
    for n, (src, dst) in enumerate(((e, e_hbm), (dh1, dh1_hbm))):
        outs.append(pltpu.make_async_copy(src, dst, lsem.at[14 + n]))
        outs[-1].start()

    for copy in to_pair:
        copy.wait_send()
    da_swap.wait_send()
    for n in range(2):
        for ref, first in ((n2, 4), (dy, 6), (n1, 8)):
            chunk_copy(ref, me, n, first, peer).wait_send()
        for ref, first in ((n2, 10), (dy, 12), (n1, 14)):
            chunk_copy(ref, peer, n, first, pair).wait_send()
        da_far(n).wait_send()
        d2_far(n).wait_send()
    for copy in outs:
        copy.wait()


def mlp_and_forward(h1, dy, x, g1, g2, wqkv, w1, w2):
    tokens = 4 * BLK
    vmem = pltpu.VMEM
    shape = jax.ShapeDtypeStruct
    return pl.pallas_call(
        mlp_kernel,
        name="mlp_fwd",
        out_shape=(shape((BLK, 1024), BF16), shape((BLK, 1024), F32), shape((tokens, 1024), BF16), shape((768, tokens), BF16), shape((12, tokens, 64), BF16),
                   shape((256, tokens), F32), shape((16, tokens), F32), shape((768, 1024), BF16), shape((1024, 1024), BF16), shape((1024, 1024), BF16)),
        in_specs=[pl.BlockSpec(memory_space=pl.ANY)] * 3 + [pl.BlockSpec(memory_space=vmem)] * 2 + [pl.BlockSpec(memory_space=pl.ANY)] * 3,
        out_specs=[pl.BlockSpec(memory_space=pl.ANY)] * 10,
        scratch_shapes=[
            vmem((tokens, 1024), BF16),
            vmem((tokens, 1024), BF16),
            vmem((tokens, 1024), BF16),
            vmem((1024, 1024), BF16),
            vmem((1024, 1024), BF16),
            vmem((1024, 1024), BF16),
            vmem((1024, 768), BF16),
            vmem((768, 1024), BF16),
            vmem((tokens, 1024), BF16),
            vmem((tokens, 1024), BF16),
            vmem((2 * BLK, 1024), BF16),
            vmem((2, HALF, 1024), BF16),
            vmem((2, HALF, 1024), BF16),
            vmem((BLK, 1024), BF16),
            vmem((BLK, 1024), F32),
            vmem((BLK, 1024), BF16),
            vmem((768, tokens), BF16),
            vmem((12, tokens, 64), BF16),
            vmem((256, tokens), F32),
            vmem((16, tokens), F32),
            vmem((1024, 1024), BF16),
            vmem((1024, 1024), BF16),
            pltpu.SemaphoreType.DMA((16,)),
            pltpu.SemaphoreType.DMA((21,)),
            pltpu.SemaphoreType.DMA((21,)),
        ],
        compiler_params=pltpu.CompilerParams(collective_id=0, has_side_effects=True, vmem_limit_bytes=63 * 1024 * 1024),
        cost_estimate=pl.CostEstimate(flops=40_000_000_000, bytes_accessed=40_000_000, transcendentals=20_000_000),
    )(h1, dy, x, g1, g2, wqkv, w1, w2)


def bwd_kernel(e_own, dh1_hbm, x_hbm, gain, n1_hbm, ct_hbm, nat_hbm, ot_hbm, stat_hbm, wqkvt_hbm, wo_hbm,
               dx_hbm, dwqkv_hbm, dwo_hbm,
               e, n1, ct, nat, nat_do, ot, stat, dot_t, dqt, dk, dv, dct, dct_far, dct_own, w_own, w_pair, wo, part, d1_send, d1_recv,
               dh1, x, dx, dwqkv, dwo, lsem, ssem, rsem):
    me, chip, core, pair, peer, diag = place()
    own = rows(me * BLK, BLK)

    local = []
    for n, (src, dst) in enumerate(((e_own, e.at[own, :]), (wo_hbm, wo), (ot_hbm, ot), (stat_hbm, stat), (ct_hbm, ct), (nat_hbm, nat), (wqkvt_hbm, w_own), (n1_hbm, n1), (x_hbm, x), (dh1_hbm, dh1))):
        copy = pltpu.make_async_copy(src, dst, lsem.at[n])
        copy.start()
        local.append(copy)
    l_e, l_wo, l_ot, l_stat, l_ct, l_nat, l_w, l_n1, l_x, l_dh1 = local

    entry_barrier((pair, peer, diag))
    l_e.wait()
    to_pair = send(e.at[own, :], e.at[own, :], ssem.at[0], rsem.at[0], pair)
    to_pair.start()
    half = BLK // 2
    to_peer = []
    for n in range(2):
        chunk = rows(me * BLK + n * half, half)
        copy = send(e.at[chunk, :], e.at[chunk, :], ssem.at[1 + n], rsem.at[1 + n], peer)
        copy.start()
        to_peer.append(copy)
    l_w.wait()
    w_swap = send(w_own, w_pair, ssem.at[5], rsem.at[5], pair)
    w_swap.start()

    dk[...] = jnp.zeros_like(dk)
    dv[...] = jnp.zeros_like(dv)
    dqt[...] = jnp.zeros_like(dqt)
    for copy in (l_wo, l_ot, l_stat, l_ct, l_nat):
        copy.wait()

    def query_block(qi):
        @pl.loop(0, qi)
        def _(ki):
            attn_bwd_tile(ki, qi, False, ct, nat, nat_do, dot_t, stat, dqt, dk, dv)

        attn_bwd_tile(qi, qi, True, ct, nat, nat_do, dot_t, stat, dqt, dk, dv)

    do_block(me, e, wo, ot, dot_t, nat_do, stat)
    to_pair.wait_recv()
    do_block(pair, e, wo, ot, dot_t, nat_do, stat)

    @pl.loop(0, 2)
    def _(n):
        query_block(chip * 2 + n)

    forward = []
    for n in range(2):
        to_peer[n].wait_recv()
        chunk = rows(peer * BLK + n * half, half)
        copy = send(e.at[chunk, :], e.at[chunk, :], ssem.at[3 + n], rsem.at[3 + n], pair)
        copy.start()
        forward.append(copy)
    do_block(peer, e, wo, ot, dot_t, nat_do, stat)
    for copy in forward:
        copy.wait_recv()
    do_block(diag, e, wo, ot, dot_t, nat_do, stat)
    w_swap.wait_recv()

    far = (1 - chip) * 2
    for n in range(2):
        block = far + 1 - n
        query_block(block)
        pack_dc(block, dqt, dk, dv, dct)
        mine = rows(block * BLK + core * half, half)
        theirs = rows(block * BLK + (1 - core) * half, half)
        swap = send(dct.at[:, theirs], dct_far.at[n], ssem.at[6 + n], rsem.at[6 + n], pair)
        swap.start()
        part[0:half, :] = nn(dct[:, mine].T, w_own[...])
        swap.wait_recv()
        d1_send[n] = (part[0:half, :] + nn(dct_far[n].T, w_pair[...])).astype(BF16)
        out = send(d1_send.at[n], d1_recv.at[core], ssem.at[9 + n], rsem.at[9 + core], block)
        out.start()
        swap.wait_send()

    for n in range(2):
        pack_dc(chip * 2 + n, dqt, dk, dv, dct)
    swap = send(dct.at[:, rows(pair * BLK, BLK)], dct_own, ssem.at[8], rsem.at[8], pair)
    swap.start()
    part[...] = nn(dct[:, own].T, w_own[...])
    swap.wait_recv()
    part[...] += nn(dct_own[...].T, w_pair[...])
    l_n1.wait()

    @pl.loop(0, 4)
    def _(i):
        sl = rows(i * 256, 256)
        dwo[:, sl] = nn(ot[...].astype(BF16), e[:, sl]).astype(BF16)
        dwqkv[sl, :] = nn(dct[...], n1[:, sl]).astype(BF16).T

    out_wqkv = pltpu.make_async_copy(dwqkv, dwqkv_hbm, lsem.at[10])
    out_wqkv.start()
    out_wo = pltpu.make_async_copy(dwo, dwo_hbm, lsem.at[11])
    out_wo.start()
    l_x.wait()
    l_dh1.wait()
    for n in range(2):
        send(d1_send.at[n], d1_recv.at[n], ssem.at[9 + n], rsem.at[9 + n], peer).wait_recv()
        sl = slice(n * half, (n + 1) * half)
        x_hat, rstd = ln_forward(x[sl, :].astype(F32))
        grad = part[sl, :] + d1_recv[n].astype(F32)
        dx[sl, :] = (dh1[sl, :] + ln_backward(x_hat, rstd, gain[...], grad)).astype(BF16)
    out_dx = pltpu.make_async_copy(dx, dx_hbm, lsem.at[12])
    out_dx.start()

    to_pair.wait_send()
    for copy in to_peer + forward:
        copy.wait_send()
    w_swap.wait_send()
    swap.wait_send()
    for n in range(2):
        send(d1_send.at[n], d1_recv.at[n], ssem.at[9 + n], rsem.at[9 + n], peer).wait_send()
    out_wqkv.wait()
    out_wo.wait()
    out_dx.wait()


def attention_bwd(e_own, dh1, x, gain, n1, ct, nat, ot, stat, wqkvt, wo):
    tokens = n1.shape[0]
    vmem = pltpu.VMEM
    return pl.pallas_call(
        bwd_kernel,
        name="attn_bwd",
        out_shape=(jax.ShapeDtypeStruct((BLK, 1024), BF16), jax.ShapeDtypeStruct((1024, 768), BF16), jax.ShapeDtypeStruct((256, 1024), BF16)),
        in_specs=[pl.BlockSpec(memory_space=pl.ANY)] * 3 + [pl.BlockSpec(memory_space=vmem)] + [pl.BlockSpec(memory_space=pl.ANY)] * 7,
        out_specs=[pl.BlockSpec(memory_space=pl.ANY)] * 3,
        scratch_shapes=[
            vmem((tokens, 1024), BF16),
            vmem((tokens, 1024), BF16),
            vmem((768, tokens), BF16),
            vmem((12, tokens, 64), BF16),
            vmem((4, tokens, 64), BF16),
            vmem((256, tokens), F32),
            vmem((16, tokens), F32),
            vmem((256, tokens), BF16),
            vmem((256, tokens), F32),
            vmem((4, tokens, 64), F32),
            vmem((4, tokens, 64), F32),
            vmem((768, tokens), BF16),
            vmem((2, 768, BLK // 2), BF16),
            vmem((768, BLK), BF16),
            vmem((768, 1024), BF16),
            vmem((768, 1024), BF16),
            vmem((256, 1024), BF16),
            vmem((BLK, 1024), F32),
            vmem((2, BLK // 2, 1024), BF16),
            vmem((2, BLK // 2, 1024), BF16),
            vmem((BLK, 1024), F32),
            vmem((BLK, 1024), BF16),
            vmem((BLK, 1024), BF16),
            vmem((1024, 768), BF16),
            vmem((256, 1024), BF16),
            pltpu.SemaphoreType.DMA((13,)),
            pltpu.SemaphoreType.DMA((11,)),
            pltpu.SemaphoreType.DMA((11,)),
        ],
        compiler_params=pltpu.CompilerParams(collective_id=1, has_side_effects=True, vmem_limit_bytes=63 * 1024 * 1024),
        cost_estimate=pl.CostEstimate(flops=40_000_000_000, bytes_accessed=40_000_000, transcendentals=20_000_000),
    )(e_own, dh1, x, gain, n1, ct, nat, ot, stat, wqkvt, wo)

def solution(mesh):
    row_spec = P(('dp', 'tp'), None)
    in_specs = (row_spec, row_spec, row_spec, P(None), P(None), P(None, 'tp'), P('tp', None, None), P(None, 'tp'), P('tp', None))
    out_specs = (row_spec, P('dp', 'tp'), P(('dp', 'tp'), None, None), P('dp', 'tp'), P(('dp', 'tp'), None))

    def device_step(in_rows, mid_rows, gout_rows, ln1_gain, ln2_gain, wqkv_loc, wout_loc, wfc1_loc, wfc2_loc):
        g1 = ln1_gain.reshape(1, 1024)
        e, dh1, n1, ct, nat, ot, stat, wqkvt, grad_wfc1, grad_wfc2 = mlp_and_forward(mid_rows, gout_rows, in_rows, g1, ln2_gain.reshape(1, 1024), wqkv_loc, wfc1_loc, wfc2_loc)
        grad_in, grad_wqkv, grad_wout = attention_bwd(e, dh1, in_rows, g1, n1, ct, nat, ot, stat, wqkvt, wout_loc.reshape(256, 1024))
        return grad_in, grad_wqkv, grad_wout.reshape(4, 64, 1024), grad_wfc1, grad_wfc2

    return jax.shard_map(device_step, mesh=mesh, in_specs=in_specs, out_specs=out_specs, check_vma=False)
```

```python
import jax
import jax.numpy as jnp
from jax import lax
from jax.experimental import pallas as pl
from jax.experimental.pallas import tpu as pltpu
from jax.sharding import PartitionSpec as P

LN_EPS = 1e-5
GELU_COEF = 0.044715
GELU_SCALE = 0.7978845608028654
LOG2E = 1.4426950408889634
F32 = jnp.float32
BF16 = jnp.bfloat16
BLK = 512
HALF = 256


def ln_forward(rows):
    row_mean = jnp.mean(rows, axis=-1, keepdims=True)
    centered = rows - row_mean
    row_rstd = lax.rsqrt(jnp.mean(centered * centered, axis=-1, keepdims=True) + LN_EPS)
    return centered * row_rstd, row_rstd


def ln_backward(x_hat, row_rstd, ln_gain, grad_norm):
    grad_hat = grad_norm * ln_gain
    proj_one = jnp.mean(grad_hat, axis=-1, keepdims=True)
    proj_two = jnp.mean(grad_hat * x_hat, axis=-1, keepdims=True)
    return row_rstd * (grad_hat - proj_one - x_hat * proj_two)


def gelu_pair(pre_act):
    tanh_val = jnp.tanh(GELU_SCALE * (pre_act + GELU_COEF * pre_act * pre_act * pre_act))
    gelu_val = 0.5 * pre_act * (1.0 + tanh_val)
    gelu_der = 0.5 * (1.0 + tanh_val) + 0.5 * pre_act * (1.0 - tanh_val * tanh_val) * GELU_SCALE * (1.0 + 3.0 * GELU_COEF * pre_act * pre_act)
    return gelu_val, gelu_der


def nn(a, b):
    return lax.dot_general(a, b, (((1,), (0,)), ((), ())), preferred_element_type=F32)


def nt(a, b):
    return lax.dot_general(a, b, (((1,), (1,)), ((), ())), preferred_element_type=F32)


def qkv_block(i, n1, wqkvt, ct, nat):
    sl = pl.ds(pl.multiple_of(i * BLK, BLK), BLK)
    for n in range(4):
        c = nt(wqkvt[n * 192:(n + 1) * 192, :], n1[sl, :]).astype(BF16)
        for j in range(3):
            part = c[j * 64:(j + 1) * 64, :]
            if j == 0:
                part = part * jnp.asarray(0.125, BF16)
            ct[(3 * n + j) * 64:(3 * n + j + 1) * 64, sl] = part
            nat[3 * n + j, sl, :] = part.T


def fwd_init(ot, stat):
    ot[...] = jnp.zeros_like(ot)
    stat[0:4, :] = jnp.full((4, stat.shape[1]), -1e30, F32)
    stat[4:16, :] = jnp.zeros((12, stat.shape[1]), F32)


def fwd_tile(ki, qi, diag, ct, nat, ot, stat):
    qs = pl.ds(pl.multiple_of(qi * BLK, BLK), BLK)
    ks = pl.ds(pl.multiple_of(ki * BLK, BLK), BLK)
    for h in range(4):
        s = nn(nat[3 * h + 1, ks, :], ct[3 * h * 64:3 * h * 64 + 64, qs])
        if diag:
            key = lax.broadcasted_iota(jnp.int32, (BLK, BLK), 0)
            query = lax.broadcasted_iota(jnp.int32, (BLK, BLK), 1)
            s = jnp.where(key <= query, s, -1e30)
        m_old = stat[h:h + 1, qs]
        m_new = jnp.maximum(m_old, jnp.max(s, axis=0, keepdims=True))
        alpha = jnp.exp2((m_old - m_new) * LOG2E)
        e = jnp.exp2((s - m_new) * LOG2E)
        stat[h:h + 1, qs] = m_new
        stat[4 + h:5 + h, qs] = stat[4 + h:5 + h, qs] * alpha + jnp.sum(e, axis=0, keepdims=True)
        hs = slice(h * 64, (h + 1) * 64)
        vt = ct[(3 * h + 2) * 64:(3 * h + 3) * 64, ks]
        ot[hs, qs] = ot[hs, qs] * alpha + nn(vt, e.astype(BF16))


def fwd_finish(ot, stat):
    for h in range(4):
        inv = 1.0 / stat[4 + h:5 + h, :]
        stat[4 + h:5 + h, :] = inv
        ot[h * 64:(h + 1) * 64, :] = ot[h * 64:(h + 1) * 64, :] * inv


def do_block(i, e, wo, ot, dot_t, nat_do, stat):
    sl = pl.ds(pl.multiple_of(i * BLK, BLK), BLK)
    d = nt(wo[...], e[sl, :]).astype(BF16)
    dot_t[:, sl] = d
    for h in range(4):
        part = d[h * 64:(h + 1) * 64, :]
        nat_do[h, sl, :] = part.T
        stat[8 + h:9 + h, sl] = jnp.sum(part.astype(F32) * ot[h * 64:(h + 1) * 64, sl], axis=0, keepdims=True)


def attn_bwd_tile(ki, qi, diag, ct, nat, nat_do, dot_t, stat, dqt, dk, dv):
    ks = pl.ds(pl.multiple_of(ki * BLK, BLK), BLK)
    qs = pl.ds(pl.multiple_of(qi * BLK, BLK), BLK)
    for h in range(4):
        s = nn(nat[3 * h + 1, ks, :], ct[3 * h * 64:3 * h * 64 + 64, qs])
        r = nn(nat[3 * h + 2, ks, :], dot_t[h * 64:(h + 1) * 64, qs])
        p = jnp.exp2((s - stat[h:h + 1, qs]) * LOG2E) * stat[4 + h:5 + h, qs]
        if diag:
            key = lax.broadcasted_iota(jnp.int32, (BLK, BLK), 0)
            query = lax.broadcasted_iota(jnp.int32, (BLK, BLK), 1)
            p = jnp.where(key <= query, p, 0.0)
        ds = (p * (r - stat[8 + h:9 + h, qs])).astype(BF16)
        dv[h, ks, :] += nn(p.astype(BF16), nat_do[h, qs, :])
        dk[h, ks, :] += nn(ds, nat[3 * h, qs, :])
        hs = slice(h * 64, (h + 1) * 64)
        dqt[hs, qs] += nn(ct[(3 * h + 1) * 64:(3 * h + 2) * 64, ks], ds)


def pack_dc(i, dqt, dk, dv, dct):
    sl = pl.ds(pl.multiple_of(i * BLK, BLK), BLK)
    for h in range(4):
        dct[3 * h * 64:3 * h * 64 + 64, sl] = (dqt[h * 64:(h + 1) * 64, sl] * 0.125).astype(BF16)
        dct[(3 * h + 1) * 64:(3 * h + 2) * 64, sl] = dk[h, sl, :].astype(BF16).T
        dct[(3 * h + 2) * 64:(3 * h + 3) * 64, sl] = dv[h, sl, :].astype(BF16).T


MESH_ID = pl.DeviceIdType.MESH


def place():
    me = lax.axis_index('tp')
    chip = me // 2
    core = me - chip * 2
    return me, chip, core, chip * 2 + (1 - core), (1 - chip) * 2 + core, (1 - chip) * 2 + (1 - core)


def entry_barrier(others):
    barrier = pltpu.get_barrier_semaphore()
    for other in others:
        pl.semaphore_signal(barrier, inc=1, device_id={'tp': other}, device_id_type=MESH_ID)
    pl.semaphore_wait(barrier, 3)


def send(src, dst, ssem, rsem, to):
    return pltpu.make_async_remote_copy(src_ref=src, dst_ref=dst, send_sem=ssem, recv_sem=rsem, device_id={'tp': to}, device_id_type=MESH_ID)


def rows(start, size):
    return pl.ds(pl.multiple_of(start, size), size)


def tn(a, b):
    return lax.dot_general(a, b, (((0,), (0,)), ((), ())), preferred_element_type=F32)


def ln_rows(src, gain, dst, start):
    @pl.loop(0, 4)
    def _(i):
        hat, _ = ln_forward(src[rows(i * 128, 128), :].astype(F32))
        dst[rows(start + i * 128, 128), :] = (hat * gain[...]).astype(BF16)


def mlp_rows(start, n2, dy, w1, w2t, act, da):
    sl = rows(start, HALF)
    for c in range(4):
        cs = slice(c * 256, (c + 1) * 256)
        gelu_val, gelu_der = gelu_pair(nn(n2[sl, :], w1[:, cs]))
        act[sl, cs] = gelu_val.astype(BF16)
        da[sl, cs] = (nn(dy[sl, :], w2t[:, cs]) * gelu_der).astype(BF16)


def mlp_kernel(h1_hbm, dy_hbm, x_hbm, g1, g2, wqkv_hbm, w1_hbm, w2_hbm,
               e_hbm, dh1_hbm, n1_hbm, ct_hbm, nat_hbm, ot_hbm, stat_hbm, wqkvt_hbm, dw1_hbm, dw2_hbm,
               n2, dy, n1, w1, w1_pair, w2t, wqkv, wqkvt, act, da, da_pair, d2_send, d2_recv, h1, dh1, e, ct, nat, ot, stat, dw1, dw2,
               lsem, ssem, rsem):
    me, chip, core, pair, peer, diag = place()
    own = rows(me * BLK, BLK)
    local = []
    for n, (src, dst) in enumerate(((h1_hbm, h1), (x_hbm, e), (dy_hbm, dy.at[own, :]), (w1_hbm, w1), (w2_hbm, dw2), (wqkv_hbm, wqkv))):
        copy = pltpu.make_async_copy(src, dst, lsem.at[n])
        copy.start()
        local.append(copy)
    l_h1, l_x, l_dy, l_w1, l_w2, l_wqkv = local

    entry_barrier((pair, peer, diag))

    def chunk_copy(ref, block, n, first, to):
        sl = rows(block * BLK + n * HALF, HALF)
        return send(ref.at[sl, :], ref.at[sl, :], ssem.at[first + n], rsem.at[first + n], to)

    to_pair = [send(ref.at[own, :], ref.at[own, :], ssem.at[n], rsem.at[n], pair) for n, ref in enumerate((n2, dy, n1))]
    to_pair.append(send(w1, w1_pair, ssem.at[3], rsem.at[3], pair))
    l_dy.wait()
    chunk_copy(dy, me, 0, 6, peer).start()
    to_pair[1].start()
    l_h1.wait()
    ln_rows(h1, g2, n2, me * BLK)
    l_x.wait()
    ln_rows(e, g1, n1, me * BLK)
    chunk_copy(n2, me, 0, 4, peer).start()
    chunk_copy(dy, me, 1, 6, peer).start()
    chunk_copy(n2, me, 1, 4, peer).start()
    for n in range(2):
        chunk_copy(n1, me, n, 8, peer).start()
    to_pair[0].start()
    to_pair[2].start()
    l_w1.wait()
    to_pair[3].start()

    l_w2.wait()
    w2t[...] = dw2[...].T

    @pl.loop(0, 4)
    def _(i):
        @pl.when(i == 2)
        def _():
            to_pair[0].wait_recv()
            to_pair[1].wait_recv()

        second = i // 2
        mlp_rows((me + second * (pair - me)) * BLK + (i - 2 * second) * HALF, n2, dy, w1, w2t, act, da)

    da_swap = send(da.at[rows(pair * BLK, BLK), :], da_pair.at[0:BLK, :], ssem.at[16], rsem.at[16], pair)
    da_swap.start()
    l_wqkv.wait()
    wqkvt[...] = wqkv[...].T
    out_w = pltpu.make_async_copy(wqkvt, wqkvt_hbm, lsem.at[6])
    out_w.start()
    fwd_init(ot, stat)
    to_pair[2].wait_recv()

    @pl.loop(0, 2)
    def _(n):
        qkv_block(chip * 2 + n, n1, wqkvt, ct, nat)

    def da_far(n):
        return send(da.at[rows(diag * BLK + n * HALF, HALF), :], da_pair.at[rows(BLK + n * HALF, HALF), :], ssem.at[17 + n], rsem.at[17 + n], pair)

    def d2_far(n):
        return send(d2_send.at[n], d2_recv.at[n], ssem.at[19 + n], rsem.at[19 + n], peer)

    to_pair[3].wait_recv()

    @pl.loop(0, 2)
    def _(n):
        chunk_copy(dy, peer, n, 6, peer).wait_recv()
        chunk_copy(dy, peer, n, 12, pair).start()
        chunk_copy(n2, peer, n, 4, peer).wait_recv()
        chunk_copy(n2, peer, n, 10, pair).start()

        @pl.loop(0, 2)
        def _(j):
            @pl.when(j == 1)
            def _():
                chunk_copy(n2, diag, n, 10, pair).wait_recv()
                chunk_copy(dy, diag, n, 12, pair).wait_recv()

            mlp_rows((peer + j * (diag - peer)) * BLK + n * HALF, n2, dy, w1, w2t, act, da)

        da_far(n).start()
        first = nt(da[rows(peer * BLK + n * HALF, HALF), :], w1[...])
        da_far(n).wait_recv()
        d2_send[n] = (first + nt(da_pair[rows(BLK + n * HALF, HALF), :], w1_pair[...])).astype(BF16)
        d2_far(n).start()

    da_swap.wait_recv()

    @pl.loop(0, 2)
    def _(i):
        sl = rows(i * HALF, HALF)
        dh1[sl, :] = nt(da[rows(me * BLK + i * HALF, HALF), :], w1[...]) + nt(da_pair[sl, :], w1_pair[...])

    outs = [out_w]
    for n, (src, dst) in enumerate(((dw1, dw1_hbm), (dw2, dw2_hbm), (n1, n1_hbm), (ct, ct_hbm), (nat, nat_hbm))):
        outs.append(pltpu.make_async_copy(src, dst, lsem.at[7 + n]))

    @pl.loop(0, 6)
    def _(i):
        @pl.when(i == 2)
        def _():
            @pl.loop(0, 4)
            def _(j):
                sl = rows(j * 256, 256)
                dw2[sl, :] = tn(act[:, sl], dy[...]).astype(BF16)
                dw1[sl, :] = tn(n2[:, sl], da[...]).astype(BF16)

            outs[1].start()
            outs[2].start()
            for n in range(2):
                chunk_copy(n1, peer, n, 8, peer).wait_recv()
                chunk_copy(n1, peer, n, 14, pair).start()

            @pl.loop(0, 2)
            def _(j):
                @pl.when(j == 1)
                def _():
                    for n in range(2):
                        chunk_copy(n1, diag, n, 14, pair).wait_recv()

                qkv_block(peer + j * (diag - peer), n1, wqkvt, ct, nat)

            for n in range(3, 6):
                outs[n].start()

        group = i // 2
        far = group % 2
        qi = far * 2 + chip * 2 - 4 * far * chip + i - 2 * group
        low = (1 - far) * (1 - group // 2) * chip * 2
        high = qi + (group // 2) * (chip * 2 - qi)

        @pl.loop(low, high)
        def _(ki):
            fwd_tile(ki, qi, False, ct, nat, ot, stat)

        @pl.when(group < 2)
        def _():
            fwd_tile(qi, qi, True, ct, nat, ot, stat)

    fwd_finish(ot, stat)
    for n, (src, dst) in enumerate(((ot, ot_hbm), (stat, stat_hbm))):
        outs.append(pltpu.make_async_copy(src, dst, lsem.at[12 + n]))
        outs[-1].start()

    for n in range(2):
        d2_far(n).wait_recv()
        sl = slice(n * HALF, (n + 1) * HALF)
        hat, rstd = ln_forward(h1[sl, :].astype(F32))
        grad = dy[rows(me * BLK + n * HALF, HALF), :].astype(F32) + ln_backward(hat, rstd, g2[...], dh1[sl, :] + d2_recv[n].astype(F32))
        dh1[sl, :] = grad
        e[sl, :] = grad.astype(BF16)
    for n, (src, dst) in enumerate(((e, e_hbm), (dh1, dh1_hbm))):
        outs.append(pltpu.make_async_copy(src, dst, lsem.at[14 + n]))
        outs[-1].start()

    for copy in to_pair:
        copy.wait_send()
    da_swap.wait_send()
    for n in range(2):
        for ref, first in ((n2, 4), (dy, 6), (n1, 8)):
            chunk_copy(ref, me, n, first, peer).wait_send()
        for ref, first in ((n2, 10), (dy, 12), (n1, 14)):
            chunk_copy(ref, peer, n, first, pair).wait_send()
        da_far(n).wait_send()
        d2_far(n).wait_send()
    for copy in outs:
        copy.wait()


def mlp_and_forward(h1, dy, x, g1, g2, wqkv, w1, w2):
    tokens = 4 * BLK
    vmem = pltpu.VMEM
    shape = jax.ShapeDtypeStruct
    return pl.pallas_call(
        mlp_kernel,
        name="mlp_fwd",
        out_shape=(shape((BLK, 1024), BF16), shape((BLK, 1024), F32), shape((tokens, 1024), BF16), shape((768, tokens), BF16), shape((12, tokens, 64), BF16),
                   shape((256, tokens), F32), shape((16, tokens), F32), shape((768, 1024), BF16), shape((1024, 1024), BF16), shape((1024, 1024), BF16)),
        in_specs=[pl.BlockSpec(memory_space=pl.ANY)] * 3 + [pl.BlockSpec(memory_space=vmem)] * 2 + [pl.BlockSpec(memory_space=pl.ANY)] * 3,
        out_specs=[pl.BlockSpec(memory_space=pl.ANY)] * 10,
        scratch_shapes=[
            vmem((tokens, 1024), BF16),
            vmem((tokens, 1024), BF16),
            vmem((tokens, 1024), BF16),
            vmem((1024, 1024), BF16),
            vmem((1024, 1024), BF16),
            vmem((1024, 1024), BF16),
            vmem((1024, 768), BF16),
            vmem((768, 1024), BF16),
            vmem((tokens, 1024), BF16),
            vmem((tokens, 1024), BF16),
            vmem((2 * BLK, 1024), BF16),
            vmem((2, HALF, 1024), BF16),
            vmem((2, HALF, 1024), BF16),
            vmem((BLK, 1024), BF16),
            vmem((BLK, 1024), F32),
            vmem((BLK, 1024), BF16),
            vmem((768, tokens), BF16),
            vmem((12, tokens, 64), BF16),
            vmem((256, tokens), F32),
            vmem((16, tokens), F32),
            vmem((1024, 1024), BF16),
            vmem((1024, 1024), BF16),
            pltpu.SemaphoreType.DMA((16,)),
            pltpu.SemaphoreType.DMA((21,)),
            pltpu.SemaphoreType.DMA((21,)),
        ],
        compiler_params=pltpu.CompilerParams(collective_id=0, has_side_effects=True, vmem_limit_bytes=63 * 1024 * 1024),
        cost_estimate=pl.CostEstimate(flops=40_000_000_000, bytes_accessed=40_000_000, transcendentals=20_000_000),
    )(h1, dy, x, g1, g2, wqkv, w1, w2)


def bwd_kernel(e_own, dh1_hbm, x_hbm, gain, n1_hbm, ct_hbm, nat_hbm, ot_hbm, stat_hbm, wqkvt_hbm, wo_hbm,
               dx_hbm, dwqkv_hbm, dwo_hbm,
               e, n1, ct, nat, nat_do, ot, stat, dot_t, dqt, dk, dv, dct, dct_far, dct_own, w_own, w_pair, wo, part, d1_send, d1_recv,
               dh1, x, dx, dwqkv, dwo, lsem, ssem, rsem):
    me, chip, core, pair, peer, diag = place()
    own = rows(me * BLK, BLK)

    local = []
    for n, (src, dst) in enumerate(((e_own, e.at[own, :]), (wo_hbm, wo), (ot_hbm, ot), (stat_hbm, stat), (ct_hbm, ct), (nat_hbm, nat), (wqkvt_hbm, w_own), (n1_hbm, n1), (x_hbm, x), (dh1_hbm, dh1))):
        copy = pltpu.make_async_copy(src, dst, lsem.at[n])
        copy.start()
        local.append(copy)
    l_e, l_wo, l_ot, l_stat, l_ct, l_nat, l_w, l_n1, l_x, l_dh1 = local

    entry_barrier((pair, peer, diag))
    l_e.wait()

    def e_half(block, part_no):
        sl = rows(block * BLK + part_no * HALF, HALF)
        return e.at[sl, :]

    to_pair = [send(e_half(me, h), e_half(me, h), ssem.at[k], rsem.at[k], pair) for k, h in ((0, 1 - core), (1, core))]
    for copy in to_pair:
        copy.start()

    def to_peer(n):
        ref = e_half(chip * 2 + 1 - n, core)
        return send(ref, ref, ssem.at[2 + n], rsem.at[2 + n], peer)

    def from_peer(n):
        ref = e_half((1 - chip) * 2 + 1 - n, core)
        return send(ref, ref, ssem.at[2 + n], rsem.at[2 + n], peer)

    def relay(n, part_no):
        ref = e_half((1 - chip) * 2 + 1 - n, part_no)
        return send(ref, ref, ssem.at[4 + n], rsem.at[4 + n], pair)

    @pl.when(core == 1)
    def _():
        to_peer(0).start()

    send(e_half(pair, core), e_half(pair, core), ssem.at[0], rsem.at[0], pair).wait_recv()

    @pl.when(core == 0)
    def _():
        to_peer(0).start()

    to_peer(1).start()
    l_w.wait()
    w_swap = send(w_own, w_pair, ssem.at[8], rsem.at[8], pair)
    w_swap.start()

    dk[...] = jnp.zeros_like(dk)
    dv[...] = jnp.zeros_like(dv)
    dqt[...] = jnp.zeros_like(dqt)
    for copy in (l_wo, l_ot, l_stat, l_ct, l_nat):
        copy.wait()

    send(e_half(pair, 1 - core), e_half(pair, 1 - core), ssem.at[1], rsem.at[1], pair).wait_recv()

    @pl.loop(0, 2)
    def _(n):
        do_block(chip * 2 + n, e, wo, ot, dot_t, nat_do, stat)

    w_swap.wait_recv()

    def swap_far(n, mine_or_theirs):
        block = (1 - chip) * 2 + 1 - n
        return send(dct.at[:, rows(block * BLK + mine_or_theirs * HALF, HALF)], dct_far.at[n], ssem.at[6 + n], rsem.at[6 + n], pair)

    def d1_far(n):
        return send(d1_send.at[n], d1_recv.at[core], ssem.at[9 + n], rsem.at[9 + core], (1 - chip) * 2 + 1 - n)

    @pl.loop(0, 6)
    def _(i):
        group = i // 2
        far = group % 2
        n = i - 2 * group
        qi = (1 - far) * (chip * 2 + n) + far * ((1 - chip) * 2 + 1 - n)
        low = (group // 2) * chip * 2
        high = far * qi + (1 - far) * ((1 - group // 2) * ((1 - chip) * qi + chip * 2) + (group // 2) * chip * qi)

        @pl.when(far == 1)
        def _():
            from_peer(n).wait_recv()
            relay(n, core).start()
            relay(n, 1 - core).wait_recv()
            do_block(qi, e, wo, ot, dot_t, nat_do, stat)

        @pl.loop(low, high)
        def _(ki):
            attn_bwd_tile(ki, qi, False, ct, nat, nat_do, dot_t, stat, dqt, dk, dv)

        @pl.when(far + (1 - far) * ((1 - group // 2) * (1 - chip) + (group // 2) * chip) == 1)
        def _():
            attn_bwd_tile(qi, qi, True, ct, nat, nat_do, dot_t, stat, dqt, dk, dv)

        @pl.when(far == 1)
        def _():
            pack_dc(qi, dqt, dk, dv, dct)
            swap_far(n, 1 - core).start()
            part[0:HALF, :] = nn(dct[:, rows(qi * BLK + core * HALF, HALF)].T, w_own[...])
            swap_far(n, core).wait_recv()
            d1_send[n] = (part[0:HALF, :] + nn(dct_far[n].T, w_pair[...])).astype(BF16)
            d1_far(n).start()

    @pl.loop(0, 2)
    def _(n):
        pack_dc(chip * 2 + n, dqt, dk, dv, dct)

    swap = send(dct.at[:, rows(pair * BLK, BLK)], dct_own, ssem.at[11], rsem.at[11], pair)
    swap.start()
    part[...] = nn(dct[:, own].T, w_own[...])
    swap.wait_recv()
    part[...] += nn(dct_own[...].T, w_pair[...])
    l_n1.wait()

    @pl.loop(0, 4)
    def _(i):
        sl = rows(i * 256, 256)
        dwo[:, sl] = nn(ot[...].astype(BF16), e[:, sl]).astype(BF16)
        dwqkv[sl, :] = nn(dct[...], n1[:, sl]).astype(BF16).T

    out_wqkv = pltpu.make_async_copy(dwqkv, dwqkv_hbm, lsem.at[10])
    out_wqkv.start()
    out_wo = pltpu.make_async_copy(dwo, dwo_hbm, lsem.at[11])
    out_wo.start()
    l_x.wait()
    l_dh1.wait()
    for n in range(2):
        send(d1_send.at[n], d1_recv.at[n], ssem.at[9 + n], rsem.at[9 + n], peer).wait_recv()
        sl = slice(n * HALF, (n + 1) * HALF)
        x_hat, rstd = ln_forward(x[sl, :].astype(F32))
        grad = part[sl, :] + d1_recv[n].astype(F32)
        dx[sl, :] = (dh1[sl, :] + ln_backward(x_hat, rstd, gain[...], grad)).astype(BF16)
    out_dx = pltpu.make_async_copy(dx, dx_hbm, lsem.at[12])
    out_dx.start()

    for copy in to_pair:
        copy.wait_send()
    for n in range(2):
        to_peer(n).wait_send()
        relay(n, core).wait_send()
        swap_far(n, 1 - core).wait_send()
        d1_far(n).wait_send()
    w_swap.wait_send()
    swap.wait_send()
    out_wqkv.wait()
    out_wo.wait()
    out_dx.wait()


def attention_bwd(e_own, dh1, x, gain, n1, ct, nat, ot, stat, wqkvt, wo):
    tokens = n1.shape[0]
    vmem = pltpu.VMEM
    return pl.pallas_call(
        bwd_kernel,
        name="attn_bwd",
        out_shape=(jax.ShapeDtypeStruct((BLK, 1024), BF16), jax.ShapeDtypeStruct((1024, 768), BF16), jax.ShapeDtypeStruct((256, 1024), BF16)),
        in_specs=[pl.BlockSpec(memory_space=pl.ANY)] * 3 + [pl.BlockSpec(memory_space=vmem)] + [pl.BlockSpec(memory_space=pl.ANY)] * 7,
        out_specs=[pl.BlockSpec(memory_space=pl.ANY)] * 3,
        scratch_shapes=[
            vmem((tokens, 1024), BF16),
            vmem((tokens, 1024), BF16),
            vmem((768, tokens), BF16),
            vmem((12, tokens, 64), BF16),
            vmem((4, tokens, 64), BF16),
            vmem((256, tokens), F32),
            vmem((16, tokens), F32),
            vmem((256, tokens), BF16),
            vmem((256, tokens), F32),
            vmem((4, tokens, 64), F32),
            vmem((4, tokens, 64), F32),
            vmem((768, tokens), BF16),
            vmem((2, 768, HALF), BF16),
            vmem((768, BLK), BF16),
            vmem((768, 1024), BF16),
            vmem((768, 1024), BF16),
            vmem((256, 1024), BF16),
            vmem((BLK, 1024), F32),
            vmem((2, HALF, 1024), BF16),
            vmem((2, HALF, 1024), BF16),
            vmem((BLK, 1024), F32),
            vmem((BLK, 1024), BF16),
            vmem((BLK, 1024), BF16),
            vmem((1024, 768), BF16),
            vmem((256, 1024), BF16),
            pltpu.SemaphoreType.DMA((13,)),
            pltpu.SemaphoreType.DMA((12,)),
            pltpu.SemaphoreType.DMA((12,)),
        ],
        compiler_params=pltpu.CompilerParams(collective_id=1, has_side_effects=True, vmem_limit_bytes=63 * 1024 * 1024),
        cost_estimate=pl.CostEstimate(flops=40_000_000_000, bytes_accessed=40_000_000, transcendentals=20_000_000),
    )(e_own, dh1, x, gain, n1, ct, nat, ot, stat, wqkvt, wo)

def solution(mesh):
    row_spec = P(('dp', 'tp'), None)
    in_specs = (row_spec, row_spec, row_spec, P(None), P(None), P(None, 'tp'), P('tp', None, None), P(None, 'tp'), P('tp', None))
    out_specs = (row_spec, P('dp', 'tp'), P(('dp', 'tp'), None, None), P('dp', 'tp'), P(('dp', 'tp'), None))

    def device_step(in_rows, mid_rows, gout_rows, ln1_gain, ln2_gain, wqkv_loc, wout_loc, wfc1_loc, wfc2_loc):
        g1 = ln1_gain.reshape(1, 1024)
        e, dh1, n1, ct, nat, ot, stat, wqkvt, grad_wfc1, grad_wfc2 = mlp_and_forward(mid_rows, gout_rows, in_rows, g1, ln2_gain.reshape(1, 1024), wqkv_loc, wfc1_loc, wfc2_loc)
        grad_in, grad_wqkv, grad_wout = attention_bwd(e, dh1, in_rows, g1, n1, ct, nat, ot, stat, wqkvt, wout_loc.reshape(256, 1024))
        return grad_in, grad_wqkv, grad_wout.reshape(4, 64, 1024), grad_wfc1, grad_wfc2

    return jax.shard_map(device_step, mesh=mesh, in_specs=in_specs, out_specs=out_specs, check_vma=False)
```

```python
import jax
import jax.numpy as jnp
from jax import lax
from jax.experimental import pallas as pl
from jax.experimental.pallas import tpu as pltpu
from jax.sharding import PartitionSpec as P

LN_EPS = 1e-5
GELU_COEF = 0.044715
GELU_SCALE = 0.7978845608028654
LOG2E = 1.4426950408889634
F32 = jnp.float32
BF16 = jnp.bfloat16
BLK = 512
HALF = 256


def ln_forward(rows):
    row_mean = jnp.mean(rows, axis=-1, keepdims=True)
    centered = rows - row_mean
    row_rstd = lax.rsqrt(jnp.mean(centered * centered, axis=-1, keepdims=True) + LN_EPS)
    return centered * row_rstd, row_rstd


def ln_backward(x_hat, row_rstd, ln_gain, grad_norm):
    grad_hat = grad_norm * ln_gain
    proj_one = jnp.mean(grad_hat, axis=-1, keepdims=True)
    proj_two = jnp.mean(grad_hat * x_hat, axis=-1, keepdims=True)
    return row_rstd * (grad_hat - proj_one - x_hat * proj_two)


def gelu_pair(pre_act):
    tanh_val = jnp.tanh(GELU_SCALE * (pre_act + GELU_COEF * pre_act * pre_act * pre_act))
    gelu_val = 0.5 * pre_act * (1.0 + tanh_val)
    gelu_der = 0.5 * (1.0 + tanh_val) + 0.5 * pre_act * (1.0 - tanh_val * tanh_val) * GELU_SCALE * (1.0 + 3.0 * GELU_COEF * pre_act * pre_act)
    return gelu_val, gelu_der


def nn(a, b):
    return lax.dot_general(a, b, (((1,), (0,)), ((), ())), preferred_element_type=F32)


def nt(a, b):
    return lax.dot_general(a, b, (((1,), (1,)), ((), ())), preferred_element_type=F32)


def qkv_block(i, n1, wqkvt, ct, nat, nat_q):
    sl = pl.ds(pl.multiple_of(i * BLK, BLK), BLK)
    for n in range(4):
        c = nt(wqkvt[n * 192:(n + 1) * 192, :], n1[sl, :]).astype(BF16)
        q = c[0:64, :] * jnp.asarray(0.125, BF16)
        ct[n * 192:n * 192 + 64, sl] = q
        ct[n * 192 + 64:n * 192 + 192, sl] = c[64:192, :]
        nat_q[n, sl, :] = jnp.concatenate([q, jnp.zeros_like(q)], axis=0).T
        nat[2 * n, sl, :] = c[64:128, :].T
        nat[2 * n + 1, sl, :] = c[128:192, :].T


def fwd_init(ot, stat):
    ot[...] = jnp.zeros_like(ot)
    stat[0:4, :] = jnp.full((4, stat.shape[1]), -1e30, F32)
    stat[4:16, :] = jnp.zeros((12, stat.shape[1]), F32)


def fwd_tile(ki, qi, diag, ct, nat, ot, stat):
    qs = pl.ds(pl.multiple_of(qi * BLK, BLK), BLK)
    ks = pl.ds(pl.multiple_of(ki * BLK, BLK), BLK)
    for h in range(4):
        s = nn(nat[2 * h, ks, :], ct[3 * h * 64:3 * h * 64 + 64, qs])
        if diag:
            key = lax.broadcasted_iota(jnp.int32, (BLK, BLK), 0)
            query = lax.broadcasted_iota(jnp.int32, (BLK, BLK), 1)
            s = jnp.where(key <= query, s, -1e30)
        m_old = stat[h:h + 1, qs]
        m_new = jnp.maximum(m_old, jnp.max(s, axis=0, keepdims=True))
        alpha = jnp.exp2((m_old - m_new) * LOG2E)
        e = jnp.exp2((s - m_new) * LOG2E)
        stat[h:h + 1, qs] = m_new
        stat[4 + h:5 + h, qs] = stat[4 + h:5 + h, qs] * alpha + jnp.sum(e, axis=0, keepdims=True)
        hs = slice(h * 64, (h + 1) * 64)
        vt = ct[(3 * h + 2) * 64:(3 * h + 3) * 64, ks]
        ot[hs, qs] = ot[hs, qs] * alpha + nn(vt, e.astype(BF16))


def fwd_finish(ot, stat):
    for h in range(4):
        inv = 1.0 / stat[4 + h:5 + h, :]
        stat[4 + h:5 + h, :] = inv
        ot[h * 64:(h + 1) * 64, :] = ot[h * 64:(h + 1) * 64, :] * inv


def do_block(i, e, wo, ot, dot_t, nat_do, stat):
    sl = pl.ds(pl.multiple_of(i * BLK, BLK), BLK)
    d = nt(wo[...], e[sl, :]).astype(BF16)
    dot_t[:, sl] = d
    for h in range(4):
        part = d[h * 64:(h + 1) * 64, :]
        nat_do[h, sl, :] = jnp.concatenate([jnp.zeros_like(part), part], axis=0).T
        stat[8 + h:9 + h, sl] = jnp.sum(part.astype(F32) * ot[h * 64:(h + 1) * 64, sl], axis=0, keepdims=True)


def attn_bwd_tile(ki, qi, diag, ct, nat, nat_q, nat_do, dot_t, stat, dqt, dkv):
    ks = pl.ds(pl.multiple_of(ki * BLK, BLK), BLK)
    qs = pl.ds(pl.multiple_of(qi * BLK, BLK), BLK)
    for h in range(4):
        s = nn(nat[2 * h, ks, :], ct[3 * h * 64:3 * h * 64 + 64, qs])
        r = nn(nat[2 * h + 1, ks, :], dot_t[h * 64:(h + 1) * 64, qs])
        p = jnp.exp2((s - stat[h:h + 1, qs]) * LOG2E) * stat[4 + h:5 + h, qs]
        if diag:
            key = lax.broadcasted_iota(jnp.int32, (BLK, BLK), 0)
            query = lax.broadcasted_iota(jnp.int32, (BLK, BLK), 1)
            p = jnp.where(key <= query, p, 0.0)
        ds = (p * (r - stat[8 + h:9 + h, qs])).astype(BF16)
        dkv[h, ks, :] += nn(p.astype(BF16), nat_do[h, qs, :]) + nn(ds, nat_q[h, qs, :])
        hs = slice(h * 64, (h + 1) * 64)
        dqt[hs, qs] += nn(ct[(3 * h + 1) * 64:(3 * h + 2) * 64, ks], ds)


def pack_dc(i, dqt, dkv, dct):
    sl = pl.ds(pl.multiple_of(i * BLK, BLK), BLK)
    for h in range(4):
        dct[3 * h * 64:3 * h * 64 + 64, sl] = (dqt[h * 64:(h + 1) * 64, sl] * 0.125).astype(BF16)
        dct[(3 * h + 1) * 64:(3 * h + 3) * 64, sl] = dkv[h, sl, :].astype(BF16).T


MESH_ID = pl.DeviceIdType.MESH


def place():
    me = lax.axis_index('tp')
    chip = me // 2
    core = me - chip * 2
    return me, chip, core, chip * 2 + (1 - core), (1 - chip) * 2 + core, (1 - chip) * 2 + (1 - core)


def entry_barrier(others):
    barrier = pltpu.get_barrier_semaphore()
    for other in others:
        pl.semaphore_signal(barrier, inc=1, device_id={'tp': other}, device_id_type=MESH_ID)
    pl.semaphore_wait(barrier, 3)


def send(src, dst, ssem, rsem, to):
    return pltpu.make_async_remote_copy(src_ref=src, dst_ref=dst, send_sem=ssem, recv_sem=rsem, device_id={'tp': to}, device_id_type=MESH_ID)


def rows(start, size):
    return pl.ds(pl.multiple_of(start, size), size)


def tn(a, b):
    return lax.dot_general(a, b, (((0,), (0,)), ((), ())), preferred_element_type=F32)


def ln_rows(src, gain, dst, start):
    @pl.loop(0, 4)
    def _(i):
        hat, _ = ln_forward(src[rows(i * 128, 128), :].astype(F32))
        dst[rows(start + i * 128, 128), :] = (hat * gain[...]).astype(BF16)


def mlp_rows(start, n2, dy, w1, w2t, act, da):
    sl = rows(start, HALF)
    for c in range(4):
        cs = slice(c * 256, (c + 1) * 256)
        gelu_val, gelu_der = gelu_pair(nn(n2[sl, :], w1[:, cs]))
        act[sl, cs] = gelu_val.astype(BF16)
        da[sl, cs] = (nn(dy[sl, :], w2t[:, cs]) * gelu_der).astype(BF16)


def layer_kernel(h1_hbm, dy_hbm, x_hbm, g1, g2, wqkv_hbm, w1_hbm, w2_hbm, wo_hbm,
                 dx_hbm, dwqkv_hbm, dwo_hbm, dw1_hbm, dw2_hbm,
                 n2, dy, n1, w1_pair, da_pair, d2_send, d2_recv, d1_recv, w_pair, dct_far, dct_own, wqkvt, dh1, ct, nat, nat_q, ot, stat,
                 lsem, ssem, rsem, free_sem):
    me, chip, core, pair, peer, diag = place()
    own = rows(me * BLK, BLK)
    e = n2

    def chunk_copy(ref, block, n, first, to):
        sl = rows(block * BLK + n * HALF, HALF)
        return send(ref.at[sl, :], ref.at[sl, :], ssem.at[first + n], rsem.at[first + n], to)

    def d2_far(n):
        return send(d2_send.at[n], d2_recv.at[n], ssem.at[19 + n], rsem.at[19 + n], peer)

    def e_half(block, part_no):
        return e.at[rows(block * BLK + part_no * HALF, HALF), :]

    def e_pair(part_no):
        ref = e_half(me, part_no)
        return send(ref, ref, ssem.at[21 + part_no], rsem.at[21 + part_no], pair)

    def from_pair(part_no):
        ref = e_half(pair, part_no)
        return send(ref, ref, ssem.at[21 + part_no], rsem.at[21 + part_no], pair)

    def e_peer(n):
        ref = e_half(chip * 2 + 1 - n, core)
        return send(ref, ref, ssem.at[23 + n], rsem.at[23 + n], peer)

    def from_peer(n):
        ref = e_half((1 - chip) * 2 + 1 - n, core)
        return send(ref, ref, ssem.at[23 + n], rsem.at[23 + n], peer)

    def relay(n, part_no):
        ref = e_half((1 - chip) * 2 + 1 - n, part_no)
        return send(ref, ref, ssem.at[25 + n], rsem.at[25 + n], pair)

    w_swap = send(wqkvt, w_pair, ssem.at[29], rsem.at[29], pair)

    def phase_one(w1, w2t, wqkv, act, da, h1, x, dw1, dw2):
        local = []
        for n, (src, dst) in enumerate(((dy_hbm, dy.at[own, :]), (h1_hbm, h1), (x_hbm, x), (w1_hbm, w1), (w2_hbm, dw2), (wqkv_hbm, wqkv))):
            copy = pltpu.make_async_copy(src, dst, lsem.at[n])
            copy.start()
            local.append(copy)
        l_dy, l_h1, l_x, l_w1, l_w2, l_wqkv = local

        entry_barrier((pair, peer, diag))

        to_pair = [send(ref.at[own, :], ref.at[own, :], ssem.at[n], rsem.at[n], pair) for n, ref in enumerate((n2, dy, n1))]
        to_pair.append(send(w1, w1_pair, ssem.at[3], rsem.at[3], pair))
        l_dy.wait()
        chunk_copy(dy, me, 0, 6, peer).start()
        to_pair[1].start()
        l_h1.wait()
        ln_rows(h1, g2, n2, me * BLK)
        l_x.wait()
        ln_rows(x, g1, n1, me * BLK)
        chunk_copy(n2, me, 0, 4, peer).start()
        chunk_copy(dy, me, 1, 6, peer).start()
        chunk_copy(n2, me, 1, 4, peer).start()
        for n in range(2):
            chunk_copy(n1, me, n, 8, peer).start()
        to_pair[0].start()
        to_pair[2].start()
        l_w1.wait()
        to_pair[3].start()

        l_w2.wait()
        w2t[...] = dw2[...].T

        @pl.loop(0, 4)
        def _(i):
            @pl.when(i == 2)
            def _():
                to_pair[0].wait_recv()
                to_pair[1].wait_recv()

            second = i // 2
            mlp_rows((me + second * (pair - me)) * BLK + (i - 2 * second) * HALF, n2, dy, w1, w2t, act, da)

        da_swap = send(da.at[rows(pair * BLK, BLK), :], da_pair.at[0:BLK, :], ssem.at[16], rsem.at[16], pair)
        da_swap.start()
        l_wqkv.wait()
        wqkvt[...] = wqkv[...].T
        fwd_init(ot, stat)
        to_pair[2].wait_recv()

        @pl.loop(0, 2)
        def _(n):
            qkv_block(chip * 2 + n, n1, wqkvt, ct, nat, nat_q)

        w_swap.start()

        def da_far(n):
            return send(da.at[rows(diag * BLK + n * HALF, HALF), :], da_pair.at[rows(BLK + n * HALF, HALF), :], ssem.at[17 + n], rsem.at[17 + n], pair)

        to_pair[3].wait_recv()

        @pl.loop(0, 2)
        def _(n):
            chunk_copy(dy, peer, n, 6, peer).wait_recv()
            chunk_copy(dy, peer, n, 12, pair).start()
            chunk_copy(n2, peer, n, 4, peer).wait_recv()
            chunk_copy(n2, peer, n, 10, pair).start()

            @pl.loop(0, 2)
            def _(j):
                @pl.when(j == 1)
                def _():
                    chunk_copy(n2, diag, n, 10, pair).wait_recv()
                    chunk_copy(dy, diag, n, 12, pair).wait_recv()

                mlp_rows((peer + j * (diag - peer)) * BLK + n * HALF, n2, dy, w1, w2t, act, da)

            da_far(n).start()
            first = nt(da[rows(peer * BLK + n * HALF, HALF), :], w1[...])
            da_far(n).wait_recv()
            d2_send[n] = (first + nt(da_pair[rows(BLK + n * HALF, HALF), :], w1_pair[...])).astype(BF16)
            d2_far(n).start()

        da_swap.wait_recv()

        @pl.loop(0, 2)
        def _(i):
            sl = rows(i * HALF, HALF)
            dh1[sl, :] = nt(da[rows(me * BLK + i * HALF, HALF), :], w1[...]) + nt(da_pair[sl, :], w1_pair[...])

        outs = [pltpu.make_async_copy(src, dst, lsem.at[6 + n]) for n, (src, dst) in enumerate(((dw1, dw1_hbm), (dw2, dw2_hbm)))]

        @pl.loop(0, 6)
        def _(i):
            @pl.when(i == 2)
            def _():
                @pl.loop(0, 4)
                def _(j):
                    sl = rows(j * 256, 256)
                    dw2[sl, :] = tn(act[:, sl], dy[...]).astype(BF16)
                    dw1[sl, :] = tn(n2[:, sl], da[...]).astype(BF16)

                for copy in outs:
                    copy.start()
                to_pair[0].wait_send()
                for n in range(2):
                    chunk_copy(n2, me, n, 4, peer).wait_send()
                    chunk_copy(n2, peer, n, 10, pair).wait_send()
                for other in (pair, peer):
                    pl.semaphore_signal(free_sem, inc=1, device_id={'tp': other}, device_id_type=MESH_ID)
                for n in range(2):
                    chunk_copy(n1, peer, n, 8, peer).wait_recv()
                    chunk_copy(n1, peer, n, 14, pair).start()

                @pl.loop(0, 2)
                def _(j):
                    @pl.when(j == 1)
                    def _():
                        for n in range(2):
                            chunk_copy(n1, diag, n, 14, pair).wait_recv()

                    qkv_block(peer + j * (diag - peer), n1, wqkvt, ct, nat, nat_q)

            group = i // 2
            far = group % 2
            qi = far * 2 + chip * 2 - 4 * far * chip + i - 2 * group
            low = (1 - far) * (1 - group // 2) * chip * 2
            high = qi + (group // 2) * (chip * 2 - qi)

            @pl.loop(low, high)
            def _(ki):
                fwd_tile(ki, qi, False, ct, nat, ot, stat)

            @pl.when(group < 2)
            def _():
                fwd_tile(qi, qi, True, ct, nat, ot, stat)

        fwd_finish(ot, stat)
        for copy in outs:
            copy.wait()
        for copy in to_pair[1:] + [da_swap]:
            copy.wait_send()
        for n in range(2):
            for ref, block, first, to in ((dy, me, 6, peer), (n1, me, 8, peer), (dy, peer, 12, pair), (n1, peer, 14, pair)):
                chunk_copy(ref, block, n, first, to).wait_send()
            da_far(n).wait_send()
        pl.semaphore_wait(free_sem, 2)

        @pl.loop(0, 2)
        def _(n):
            d2_far(n).wait_recv()
            sl = rows(n * HALF, HALF)
            hat, rstd = ln_forward(h1[sl, :].astype(F32))
            rows_n = rows(me * BLK + n * HALF, HALF)
            grad = dy[rows_n, :].astype(F32) + ln_backward(hat, rstd, g2[...], dh1[sl, :] + d2_recv[n].astype(F32))
            dh1[sl, :] = grad
            e[rows_n, :] = grad.astype(BF16)
            e_pair(n).start()

            @pl.when(core == n)
            def _():
                @pl.when(core == 1)
                def _():
                    e_peer(0).start()

                from_pair(core).wait_recv()

                @pl.when(core == 0)
                def _():
                    e_peer(0).start()

                e_peer(1).start()

    pl.run_scoped(
        phase_one,
        w1=pltpu.VMEM((1024, 1024), BF16),
        w2t=pltpu.VMEM((1024, 1024), BF16),
        wqkv=pltpu.VMEM((1024, 768), BF16),
        act=pltpu.VMEM((4 * BLK, 1024), BF16),
        da=pltpu.VMEM((4 * BLK, 1024), BF16),
        h1=pltpu.VMEM((BLK, 1024), BF16),
        x=pltpu.VMEM((BLK, 1024), BF16),
        dw1=pltpu.VMEM((1024, 1024), BF16),
        dw2=pltpu.VMEM((1024, 1024), BF16),
    )

    def phase_two(nat_do, dot_t, dqt, dkv, wo, part, x, dx, dwqkv, dwo, dct):
        l_wo = pltpu.make_async_copy(wo_hbm, wo, lsem.at[8])
        l_wo.start()
        l_x = pltpu.make_async_copy(x_hbm, x, lsem.at[9])
        l_x.start()
        dkv[...] = jnp.zeros_like(dkv)
        dqt[...] = jnp.zeros_like(dqt)
        from_pair(1 - core).wait_recv()
        for n in range(2):
            d2_far(n).wait_send()
        l_wo.wait()

        @pl.loop(0, 2)
        def _(n):
            do_block(chip * 2 + n, e, wo, ot, dot_t, nat_do, stat)

        w_swap.wait_recv()

        def swap_far(n, mine_or_theirs):
            block = (1 - chip) * 2 + 1 - n
            return send(dct.at[:, rows(block * BLK + mine_or_theirs * HALF, HALF)], dct_far.at[n], ssem.at[27 + n], rsem.at[27 + n], pair)

        def d1_far(n):
            return send(d2_send.at[n], d1_recv.at[core], ssem.at[30 + n], rsem.at[30 + core], (1 - chip) * 2 + 1 - n)

        @pl.loop(0, 6)
        def _(i):
            group = i // 2
            far = group % 2
            n = i - 2 * group
            qi = (1 - far) * (chip * 2 + n) + far * ((1 - chip) * 2 + 1 - n)
            low = (group // 2) * chip * 2
            high = far * qi + (1 - far) * ((1 - group // 2) * ((1 - chip) * qi + chip * 2) + (group // 2) * chip * qi)

            @pl.when(far == 1)
            def _():
                from_peer(n).wait_recv()
                relay(n, core).start()
                relay(n, 1 - core).wait_recv()
                do_block(qi, e, wo, ot, dot_t, nat_do, stat)

            @pl.loop(low, high)
            def _(ki):
                attn_bwd_tile(ki, qi, False, ct, nat, nat_q, nat_do, dot_t, stat, dqt, dkv)

            @pl.when(far + (1 - far) * ((1 - group // 2) * (1 - chip) + (group // 2) * chip) == 1)
            def _():
                attn_bwd_tile(qi, qi, True, ct, nat, nat_q, nat_do, dot_t, stat, dqt, dkv)

            @pl.when(far == 1)
            def _():
                pack_dc(qi, dqt, dkv, dct)
                swap_far(n, 1 - core).start()
                part[0:HALF, :] = nn(dct[:, rows(qi * BLK + core * HALF, HALF)].T, wqkvt[...])
                swap_far(n, core).wait_recv()
                d2_send[n] = (part[0:HALF, :] + nn(dct_far[n].T, w_pair[...])).astype(BF16)
                d1_far(n).start()

        @pl.loop(0, 2)
        def _(n):
            pack_dc(chip * 2 + n, dqt, dkv, dct)

        swap = send(dct.at[:, rows(pair * BLK, BLK)], dct_own, ssem.at[32], rsem.at[32], pair)
        swap.start()
        part[...] = nn(dct[:, own].T, wqkvt[...])
        swap.wait_recv()
        part[...] += nn(dct_own[...].T, w_pair[...])

        @pl.loop(0, 4)
        def _(i):
            sl = rows(i * 256, 256)
            dwo[:, sl] = nn(ot[...].astype(BF16), e[:, sl]).astype(BF16)
            dwqkv[sl, :] = nn(dct[...], n1[:, sl]).astype(BF16).T

        outs = [pltpu.make_async_copy(src, dst, lsem.at[10 + n]) for n, (src, dst) in enumerate(((dwqkv, dwqkv_hbm), (dwo, dwo_hbm), (dx, dx_hbm)))]
        outs[0].start()
        outs[1].start()
        l_x.wait()

        @pl.loop(0, 2)
        def _(n):
            send(d2_send.at[n], d1_recv.at[n], ssem.at[30 + n], rsem.at[30 + n], peer).wait_recv()
            sl = rows(n * HALF, HALF)
            hat, rstd = ln_forward(x[sl, :].astype(F32))
            grad = part[sl, :] + d1_recv[n].astype(F32)
            dx[sl, :] = (dh1[sl, :] + ln_backward(hat, rstd, g1[...], grad)).astype(BF16)

        outs[2].start()
        for n in range(2):
            e_pair(n).wait_send()
            e_peer(n).wait_send()
            relay(n, core).wait_send()
            swap_far(n, 1 - core).wait_send()
            d1_far(n).wait_send()
        w_swap.wait_send()
        swap.wait_send()
        for copy in outs:
            copy.wait()

    tokens = 4 * BLK
    pl.run_scoped(
        phase_two,
        nat_do=pltpu.VMEM((4, tokens, 128), BF16),
        dot_t=pltpu.VMEM((256, tokens), BF16),
        dqt=pltpu.VMEM((256, tokens), F32),
        dkv=pltpu.VMEM((4, tokens, 128), F32),
        wo=pltpu.VMEM((256, 1024), BF16),
        part=pltpu.VMEM((BLK, 1024), F32),
        x=pltpu.VMEM((BLK, 1024), BF16),
        dx=pltpu.VMEM((BLK, 1024), BF16),
        dwqkv=pltpu.VMEM((1024, 768), BF16),
        dwo=pltpu.VMEM((256, 1024), BF16),
        dct=pltpu.VMEM((768, tokens), BF16),
    )


def layer_grads(h1, dy, x, g1, g2, wqkv, w1, w2, wo):
    tokens = 4 * BLK
    vmem = pltpu.VMEM
    shape = jax.ShapeDtypeStruct
    hbm = pl.BlockSpec(memory_space=pl.ANY)
    return pl.pallas_call(
        layer_kernel,
        name="layer_grads",
        out_shape=(shape((BLK, 1024), BF16), shape((1024, 768), BF16), shape((256, 1024), BF16), shape((1024, 1024), BF16), shape((1024, 1024), BF16)),
        in_specs=[hbm] * 3 + [pl.BlockSpec(memory_space=vmem)] * 2 + [hbm] * 4,
        out_specs=[hbm] * 5,
        scratch_shapes=[
            vmem((tokens, 1024), BF16),
            vmem((tokens, 1024), BF16),
            vmem((tokens, 1024), BF16),
            vmem((1024, 1024), BF16),
            vmem((2 * BLK, 1024), BF16),
            vmem((2, HALF, 1024), BF16),
            vmem((2, HALF, 1024), BF16),
            vmem((2, HALF, 1024), BF16),
            vmem((768, 1024), BF16),
            vmem((2, 768, HALF), BF16),
            vmem((768, BLK), BF16),
            vmem((768, 1024), BF16),
            vmem((BLK, 1024), F32),
            vmem((768, tokens), BF16),
            vmem((8, tokens, 64), BF16),
            vmem((4, tokens, 128), BF16),
            vmem((256, tokens), F32),
            vmem((16, tokens), F32),
            pltpu.SemaphoreType.DMA((13,)),
            pltpu.SemaphoreType.DMA((33,)),
            pltpu.SemaphoreType.DMA((33,)),
            pltpu.SemaphoreType.REGULAR,
        ],
        compiler_params=pltpu.CompilerParams(collective_id=0, has_side_effects=True, vmem_limit_bytes=67043328),
        cost_estimate=pl.CostEstimate(flops=80_000_000_000, bytes_accessed=40_000_000, transcendentals=40_000_000),
    )(h1, dy, x, g1, g2, wqkv, w1, w2, wo)


def solution(mesh):
    row_spec = P(('dp', 'tp'), None)
    in_specs = (row_spec, row_spec, row_spec, P(None), P(None), P(None, 'tp'), P('tp', None, None), P(None, 'tp'), P('tp', None))
    out_specs = (row_spec, P('dp', 'tp'), P(('dp', 'tp'), None, None), P('dp', 'tp'), P(('dp', 'tp'), None))

    def device_step(in_rows, mid_rows, gout_rows, ln1_gain, ln2_gain, wqkv_loc, wout_loc, wfc1_loc, wfc2_loc):
        grad_in, grad_wqkv, grad_wout, grad_wfc1, grad_wfc2 = layer_grads(mid_rows, gout_rows, in_rows, ln1_gain.reshape(1, 1024), ln2_gain.reshape(1, 1024), wqkv_loc, wfc1_loc, wfc2_loc, wout_loc.reshape(256, 1024))
        return grad_in, grad_wqkv, grad_wout.reshape(4, 64, 1024), grad_wfc1, grad_wfc2

    return jax.shard_map(device_step, mesh=mesh, in_specs=in_specs, out_specs=out_specs, check_vma=False)
```

```python
import jax
import jax.numpy as jnp
from jax import lax
from jax.experimental import pallas as pl
from jax.experimental.pallas import tpu as pltpu
from jax.sharding import PartitionSpec as P

LN_EPS = 1e-5
GELU_COEF = 0.044715
GELU_SCALE = 0.7978845608028654
LOG2E = 1.4426950408889634
F32 = jnp.float32
BF16 = jnp.bfloat16
BLK = 512
HALF = 256


def ln_forward(rows):
    row_mean = jnp.mean(rows, axis=-1, keepdims=True)
    centered = rows - row_mean
    row_rstd = lax.rsqrt(jnp.mean(centered * centered, axis=-1, keepdims=True) + LN_EPS)
    return centered * row_rstd, row_rstd


def ln_backward(x_hat, row_rstd, ln_gain, grad_norm):
    grad_hat = grad_norm * ln_gain
    proj_one = jnp.mean(grad_hat, axis=-1, keepdims=True)
    proj_two = jnp.mean(grad_hat * x_hat, axis=-1, keepdims=True)
    return row_rstd * (grad_hat - proj_one - x_hat * proj_two)


def gelu_pair(pre_act):
    tanh_val = jnp.tanh(GELU_SCALE * (pre_act + GELU_COEF * pre_act * pre_act * pre_act))
    gelu_val = 0.5 * pre_act * (1.0 + tanh_val)
    gelu_der = 0.5 * (1.0 + tanh_val) + 0.5 * pre_act * (1.0 - tanh_val * tanh_val) * GELU_SCALE * (1.0 + 3.0 * GELU_COEF * pre_act * pre_act)
    return gelu_val, gelu_der


def nn(a, b):
    return lax.dot_general(a, b, (((1,), (0,)), ((), ())), preferred_element_type=F32)


def nt(a, b):
    return lax.dot_general(a, b, (((1,), (1,)), ((), ())), preferred_element_type=F32)


def qkv_block(i, n1, wqkvt, ct, nat, nat_q):
    sl = pl.ds(pl.multiple_of(i * BLK, BLK), BLK)
    for n in range(4):
        c = nt(wqkvt[n * 192:(n + 1) * 192, :], n1[sl, :]).astype(BF16)
        q = c[0:64, :] * jnp.asarray(0.125, BF16)
        ct[n * 192:n * 192 + 64, sl] = q
        ct[n * 192 + 64:n * 192 + 192, sl] = c[64:192, :]
        nat_q[n, sl, :] = jnp.concatenate([q, jnp.zeros_like(q)], axis=0).T
        nat[2 * n, sl, :] = c[64:128, :].T
        nat[2 * n + 1, sl, :] = c[128:192, :].T


def fwd_init(ot, stat):
    ot[...] = jnp.zeros_like(ot)
    stat[0:4, :] = jnp.full((4, stat.shape[1]), -1e30, F32)
    stat[4:16, :] = jnp.zeros((12, stat.shape[1]), F32)


def fwd_tile(ki, qi, diag, ct, nat, ot, stat):
    qs = pl.ds(pl.multiple_of(qi * BLK, BLK), BLK)
    ks = pl.ds(pl.multiple_of(ki * BLK, BLK), BLK)
    for h in range(4):
        s = nn(nat[2 * h, ks, :], ct[3 * h * 64:3 * h * 64 + 64, qs])
        if diag:
            key = lax.broadcasted_iota(jnp.int32, (BLK, BLK), 0)
            query = lax.broadcasted_iota(jnp.int32, (BLK, BLK), 1)
            s = jnp.where(key <= query, s, -1e30)
        m_old = stat[h:h + 1, qs]
        m_new = jnp.maximum(m_old, jnp.max(s, axis=0, keepdims=True))
        alpha = jnp.exp2((m_old - m_new) * LOG2E)
        e = jnp.exp2((s - m_new) * LOG2E)
        stat[h:h + 1, qs] = m_new
        stat[4 + h:5 + h, qs] = stat[4 + h:5 + h, qs] * alpha + jnp.sum(e, axis=0, keepdims=True)
        hs = slice(h * 64, (h + 1) * 64)
        vt = ct[(3 * h + 2) * 64:(3 * h + 3) * 64, ks]
        ot[hs, qs] = ot[hs, qs] * alpha + nn(vt, e.astype(BF16))


def fwd_finish(ot, stat):
    for h in range(4):
        inv = 1.0 / stat[4 + h:5 + h, :]
        stat[4 + h:5 + h, :] = inv
        ot[h * 64:(h + 1) * 64, :] = ot[h * 64:(h + 1) * 64, :] * inv


def do_block(i, e, wo, ot, dot_t, nat_do, stat):
    sl = pl.ds(pl.multiple_of(i * HALF, HALF), HALF)
    d = nt(wo[...], e[sl, :]).astype(BF16)
    dot_t[:, sl] = d
    for h in range(4):
        part = d[h * 64:(h + 1) * 64, :]
        nat_do[h, sl, :] = jnp.concatenate([jnp.zeros_like(part), part], axis=0).T
        stat[8 + h:9 + h, sl] = jnp.sum(part.astype(F32) * ot[h * 64:(h + 1) * 64, sl], axis=0, keepdims=True)


def attn_bwd_tile(ki, size, qj, diag, ct, nat, nat_q, nat_do, dot_t, stat, dqt, dkv):
    ks = pl.ds(pl.multiple_of(ki * size, size), size)
    qs = pl.ds(pl.multiple_of(qj * HALF, HALF), HALF)
    for h in range(4):
        s = nn(nat[2 * h, ks, :], ct[3 * h * 64:3 * h * 64 + 64, qs])
        r = nn(nat[2 * h + 1, ks, :], dot_t[h * 64:(h + 1) * 64, qs])
        p = jnp.exp2((s - stat[h:h + 1, qs]) * LOG2E) * stat[4 + h:5 + h, qs]
        if diag:
            key = lax.broadcasted_iota(jnp.int32, (size, HALF), 0)
            query = lax.broadcasted_iota(jnp.int32, (size, HALF), 1)
            p = jnp.where(key <= query, p, 0.0)
        ds = (p * (r - stat[8 + h:9 + h, qs])).astype(BF16)
        dkv[h, ks, :] += nn(p.astype(BF16), nat_do[h, qs, :]) + nn(ds, nat_q[h, qs, :])
        hs = slice(h * 64, (h + 1) * 64)
        dqt[hs, qs] += nn(ct[(3 * h + 1) * 64:(3 * h + 2) * 64, ks], ds)


def pack_dc(i, dqt, dkv, dct):
    sl = pl.ds(pl.multiple_of(i * BLK, BLK), BLK)
    for h in range(4):
        dct[3 * h * 64:3 * h * 64 + 64, sl] = (dqt[h * 64:(h + 1) * 64, sl] * 0.125).astype(BF16)
        dct[(3 * h + 1) * 64:(3 * h + 3) * 64, sl] = dkv[h, sl, :].astype(BF16).T


MESH_ID = pl.DeviceIdType.MESH


def place():
    me = lax.axis_index('tp')
    chip = me // 2
    core = me - chip * 2
    return me, chip, core, chip * 2 + (1 - core), (1 - chip) * 2 + core, (1 - chip) * 2 + (1 - core)


def entry_barrier(others):
    barrier = pltpu.get_barrier_semaphore()
    for other in others:
        pl.semaphore_signal(barrier, inc=1, device_id={'tp': other}, device_id_type=MESH_ID)
    pl.semaphore_wait(barrier, 3)


def send(src, dst, ssem, rsem, to):
    return pltpu.make_async_remote_copy(src_ref=src, dst_ref=dst, send_sem=ssem, recv_sem=rsem, device_id={'tp': to}, device_id_type=MESH_ID)


def rows(start, size):
    return pl.ds(pl.multiple_of(start, size), size)


def tn(a, b):
    return lax.dot_general(a, b, (((0,), (0,)), ((), ())), preferred_element_type=F32)


def ln_rows(src, gain, dst, start):
    @pl.loop(0, 4)
    def _(i):
        hat, _ = ln_forward(src[rows(i * 128, 128), :].astype(F32))
        dst[rows(start + i * 128, 128), :] = (hat * gain[...]).astype(BF16)


def mlp_rows(start, n2, dy, w1, w2t, act, da):
    sl = rows(start, HALF)
    for c in range(4):
        cs = slice(c * 256, (c + 1) * 256)
        gelu_val, gelu_der = gelu_pair(nn(n2[sl, :], w1[:, cs]))
        act[sl, cs] = gelu_val.astype(BF16)
        da[sl, cs] = (nn(dy[sl, :], w2t[:, cs]) * gelu_der).astype(BF16)


def layer_kernel(h1_hbm, dy_hbm, x_hbm, g1, g2, wqkv_hbm, w1_hbm, w2_hbm, wo_hbm,
                 dx_hbm, dwqkv_hbm, dwo_hbm, dw1_hbm, dw2_hbm,
                 n2, dy, n1, w1_pair, da_pair, d2_send, d2_recv, d1_recv, w_pair, dct_far, dct_own, wqkvt, dh1, ct, nat, nat_q, ot, stat,
                 lsem, ssem, rsem, free_sem):
    me, chip, core, pair, peer, diag = place()
    own = rows(me * BLK, BLK)
    e = n2

    def chunk_copy(ref, block, n, first, to):
        sl = rows(block * BLK + n * HALF, HALF)
        return send(ref.at[sl, :], ref.at[sl, :], ssem.at[first + n], rsem.at[first + n], to)

    def d2_far(n):
        return send(d2_send.at[n], d2_recv.at[n], ssem.at[19 + n], rsem.at[19 + n], peer)

    def e_half(block, part_no):
        return e.at[rows(block * BLK + part_no * HALF, HALF), :]

    def e_pair(part_no):
        ref = e_half(me, part_no)
        return send(ref, ref, ssem.at[21 + part_no], rsem.at[21 + part_no], pair)

    def from_pair(part_no):
        ref = e_half(pair, part_no)
        return send(ref, ref, ssem.at[21 + part_no], rsem.at[21 + part_no], pair)

    def e_chunk(block, part_no, who):
        return e.at[rows(block * BLK + part_no * HALF + who * 128, 128), :]

    def e_peer(j):
        ref = e_chunk(chip * 2 + 1 - j // 2, j % 2, core)
        return send(ref, ref, ssem.at[23 + j], rsem.at[23 + j], peer)

    def from_peer(j):
        ref = e_chunk((1 - chip) * 2 + 1 - j // 2, j % 2, core)
        return send(ref, ref, ssem.at[23 + j], rsem.at[23 + j], peer)

    def relay(j, who):
        ref = e_chunk((1 - chip) * 2 + 1 - j // 2, j % 2, who)
        return send(ref, ref, ssem.at[33 + j], rsem.at[33 + j], pair)

    w_swap = send(wqkvt, w_pair, ssem.at[29], rsem.at[29], pair)

    def phase_one(w1, w2t, wqkv, act, da, h1, x, dw1, dw2):
        local = []
        for n, (src, dst) in enumerate(((dy_hbm, dy.at[own, :]), (h1_hbm, h1), (x_hbm, x), (w1_hbm, w1), (w2_hbm, dw2), (wqkv_hbm, wqkv))):
            copy = pltpu.make_async_copy(src, dst, lsem.at[n])
            copy.start()
            local.append(copy)
        l_dy, l_h1, l_x, l_w1, l_w2, l_wqkv = local

        entry_barrier((pair, peer, diag))

        to_pair = [send(ref.at[own, :], ref.at[own, :], ssem.at[n], rsem.at[n], pair) for n, ref in enumerate((n2, dy, n1))]
        to_pair.append(send(w1, w1_pair, ssem.at[3], rsem.at[3], pair))
        l_dy.wait()
        chunk_copy(dy, me, 0, 6, peer).start()
        to_pair[1].start()
        l_h1.wait()
        ln_rows(h1, g2, n2, me * BLK)
        l_x.wait()
        ln_rows(x, g1, n1, me * BLK)
        chunk_copy(n2, me, 0, 4, peer).start()
        chunk_copy(dy, me, 1, 6, peer).start()
        chunk_copy(n2, me, 1, 4, peer).start()
        for n in range(2):
            chunk_copy(n1, me, n, 8, peer).start()
        to_pair[0].start()
        to_pair[2].start()
        l_w1.wait()
        to_pair[3].start()

        l_w2.wait()
        w2t[...] = dw2[...].T

        @pl.loop(0, 4)
        def _(i):
            @pl.when(i == 2)
            def _():
                to_pair[0].wait_recv()
                to_pair[1].wait_recv()

            second = i // 2
            mlp_rows((me + second * (pair - me)) * BLK + (i - 2 * second) * HALF, n2, dy, w1, w2t, act, da)

        da_swap = send(da.at[rows(pair * BLK, BLK), :], da_pair.at[0:BLK, :], ssem.at[16], rsem.at[16], pair)
        da_swap.start()
        l_wqkv.wait()
        wqkvt[...] = wqkv[...].T
        fwd_init(ot, stat)
        to_pair[2].wait_recv()

        @pl.loop(0, 2)
        def _(n):
            qkv_block(chip * 2 + n, n1, wqkvt, ct, nat, nat_q)

        w_swap.start()

        def da_far(n):
            return send(da.at[rows(diag * BLK + n * HALF, HALF), :], da_pair.at[rows(BLK + n * HALF, HALF), :], ssem.at[17 + n], rsem.at[17 + n], pair)

        to_pair[3].wait_recv()

        @pl.loop(0, 2)
        def _(n):
            chunk_copy(dy, peer, n, 6, peer).wait_recv()
            chunk_copy(dy, peer, n, 12, pair).start()
            chunk_copy(n2, peer, n, 4, peer).wait_recv()
            chunk_copy(n2, peer, n, 10, pair).start()

            @pl.loop(0, 2)
            def _(j):
                @pl.when(j == 1)
                def _():
                    chunk_copy(n2, diag, n, 10, pair).wait_recv()
                    chunk_copy(dy, diag, n, 12, pair).wait_recv()

                mlp_rows((peer + j * (diag - peer)) * BLK + n * HALF, n2, dy, w1, w2t, act, da)

            da_far(n).start()
            first = nt(da[rows(peer * BLK + n * HALF, HALF), :], w1[...])
            da_far(n).wait_recv()
            d2_send[n] = (first + nt(da_pair[rows(BLK + n * HALF, HALF), :], w1_pair[...])).astype(BF16)
            d2_far(n).start()

        da_swap.wait_recv()

        @pl.loop(0, 2)
        def _(i):
            sl = rows(i * HALF, HALF)
            dh1[sl, :] = nt(da[rows(me * BLK + i * HALF, HALF), :], w1[...]) + nt(da_pair[sl, :], w1_pair[...])

        outs = [pltpu.make_async_copy(src, dst, lsem.at[6 + n]) for n, (src, dst) in enumerate(((dw1, dw1_hbm), (dw2, dw2_hbm)))]

        @pl.loop(0, 6)
        def _(i):
            @pl.when(i == 2)
            def _():
                @pl.loop(0, 4)
                def _(j):
                    sl = rows(j * 256, 256)
                    dw2[sl, :] = tn(act[:, sl], dy[...]).astype(BF16)
                    dw1[sl, :] = tn(n2[:, sl], da[...]).astype(BF16)

                for copy in outs:
                    copy.start()
                to_pair[0].wait_send()
                for n in range(2):
                    chunk_copy(n2, me, n, 4, peer).wait_send()
                    chunk_copy(n2, peer, n, 10, pair).wait_send()
                for other in (pair, peer):
                    pl.semaphore_signal(free_sem, inc=1, device_id={'tp': other}, device_id_type=MESH_ID)
                for n in range(2):
                    chunk_copy(n1, peer, n, 8, peer).wait_recv()
                    chunk_copy(n1, peer, n, 14, pair).start()

                @pl.loop(0, 2)
                def _(j):
                    @pl.when(j == 1)
                    def _():
                        for n in range(2):
                            chunk_copy(n1, diag, n, 14, pair).wait_recv()

                    qkv_block(peer + j * (diag - peer), n1, wqkvt, ct, nat, nat_q)

            group = i // 2
            far = group % 2
            qi = far * 2 + chip * 2 - 4 * far * chip + i - 2 * group
            low = (1 - far) * (1 - group // 2) * chip * 2
            high = qi + (group // 2) * (chip * 2 - qi)

            @pl.loop(low, high)
            def _(ki):
                fwd_tile(ki, qi, False, ct, nat, ot, stat)

            @pl.when(group < 2)
            def _():
                fwd_tile(qi, qi, True, ct, nat, ot, stat)

        fwd_finish(ot, stat)
        for copy in outs:
            copy.wait()
        for copy in to_pair[1:] + [da_swap]:
            copy.wait_send()
        for n in range(2):
            for ref, block, first, to in ((dy, me, 6, peer), (n1, me, 8, peer), (dy, peer, 12, pair), (n1, peer, 14, pair)):
                chunk_copy(ref, block, n, first, to).wait_send()
            da_far(n).wait_send()
        pl.semaphore_wait(free_sem, 2)

        @pl.loop(0, 2)
        def _(n):
            d2_far(n).wait_recv()
            sl = rows(n * HALF, HALF)
            hat, rstd = ln_forward(h1[sl, :].astype(F32))
            rows_n = rows(me * BLK + n * HALF, HALF)
            grad = dy[rows_n, :].astype(F32) + ln_backward(hat, rstd, g2[...], dh1[sl, :] + d2_recv[n].astype(F32))
            dh1[sl, :] = grad
            e[rows_n, :] = grad.astype(BF16)
            e_pair(n).start()

            @pl.when(n * core == 1)
            def _():
                e_peer(1).start()

            from_pair(n).wait_recv()

            @pl.when(n == 0)
            def _():
                e_peer(0).start()

            @pl.when(n * (1 - core) == 1)
            def _():
                e_peer(1).start()

            @pl.when(n == 1)
            def _():
                e_peer(2).start()
                e_peer(3).start()

    pl.run_scoped(
        phase_one,
        w1=pltpu.VMEM((1024, 1024), BF16),
        w2t=pltpu.VMEM((1024, 1024), BF16),
        wqkv=pltpu.VMEM((1024, 768), BF16),
        act=pltpu.VMEM((4 * BLK, 1024), BF16),
        da=pltpu.VMEM((4 * BLK, 1024), BF16),
        h1=pltpu.VMEM((BLK, 1024), BF16),
        x=pltpu.VMEM((BLK, 1024), BF16),
        dw1=pltpu.VMEM((1024, 1024), BF16),
        dw2=pltpu.VMEM((1024, 1024), BF16),
    )

    def phase_two(nat_do, dot_t, dqt, dkv, wo, part, x, dx, dwqkv, dwo, dct):
        l_wo = pltpu.make_async_copy(wo_hbm, wo, lsem.at[8])
        l_wo.start()
        l_x = pltpu.make_async_copy(x_hbm, x, lsem.at[9])
        l_x.start()
        dkv[...] = jnp.zeros_like(dkv)
        dqt[...] = jnp.zeros_like(dqt)
        for n in range(2):
            d2_far(n).wait_send()
        l_wo.wait()

        @pl.loop(0, 4)
        def _(n):
            do_block(chip * 4 + n, e, wo, ot, dot_t, nat_do, stat)

        w_swap.wait_recv()

        def swap_far(n, mine_or_theirs):
            block = (1 - chip) * 2 + 1 - n
            return send(dct.at[:, rows(block * BLK + mine_or_theirs * HALF, HALF)], dct_far.at[n], ssem.at[27 + n], rsem.at[27 + n], pair)

        def d1_far(n):
            return send(d2_send.at[n], d1_recv.at[core], ssem.at[30 + n], rsem.at[30 + core], (1 - chip) * 2 + 1 - n)

        @pl.loop(0, 12)
        def _(i):
            group = i // 4
            far = group % 2
            j = i - 4 * group
            n = j // 2
            odd = j - 2 * n
            qi = (1 - far) * (chip * 2 + n) + far * ((1 - chip) * 2 + 1 - n)
            qj = qi * 2 + odd
            low = (group // 2) * chip * 2
            high = far * qi + (1 - far) * ((1 - group // 2) * ((1 - chip) * qi + chip * 2) + (group // 2) * chip * qi)
            with_diag = far + (1 - far) * ((1 - group // 2) * (1 - chip) + (group // 2) * chip)

            @pl.when(far == 1)
            def _():
                from_peer(j).wait_recv()
                relay(j, core).start()
                relay(j, 1 - core).wait_recv()
                do_block(qj, e, wo, ot, dot_t, nat_do, stat)

            @pl.loop(low, high)
            def _(ki):
                attn_bwd_tile(ki, BLK, qj, False, ct, nat, nat_q, nat_do, dot_t, stat, dqt, dkv)

            @pl.when(with_diag * odd == 1)
            def _():
                attn_bwd_tile(qj - 1, HALF, qj, False, ct, nat, nat_q, nat_do, dot_t, stat, dqt, dkv)

            @pl.when(with_diag == 1)
            def _():
                attn_bwd_tile(qj, HALF, qj, True, ct, nat, nat_q, nat_do, dot_t, stat, dqt, dkv)

            @pl.when(far * odd == 1)
            def _():
                pack_dc(qi, dqt, dkv, dct)
                swap_far(n, 1 - core).start()
                part[0:HALF, :] = nn(dct[:, rows(qi * BLK + core * HALF, HALF)].T, wqkvt[...])
                swap_far(n, core).wait_recv()
                d2_send[n] = (part[0:HALF, :] + nn(dct_far[n].T, w_pair[...])).astype(BF16)
                d1_far(n).start()

        @pl.loop(0, 2)
        def _(n):
            pack_dc(chip * 2 + n, dqt, dkv, dct)

        swap = send(dct.at[:, rows(pair * BLK, BLK)], dct_own, ssem.at[32], rsem.at[32], pair)
        swap.start()
        part[...] = nn(dct[:, own].T, wqkvt[...])
        swap.wait_recv()
        part[...] += nn(dct_own[...].T, w_pair[...])

        @pl.loop(0, 4)
        def _(i):
            sl = rows(i * 256, 256)
            dwo[:, sl] = nn(ot[...].astype(BF16), e[:, sl]).astype(BF16)
            dwqkv[sl, :] = nn(dct[...], n1[:, sl]).astype(BF16).T

        outs = [pltpu.make_async_copy(src, dst, lsem.at[10 + n]) for n, (src, dst) in enumerate(((dwqkv, dwqkv_hbm), (dwo, dwo_hbm), (dx, dx_hbm)))]
        outs[0].start()
        outs[1].start()
        l_x.wait()

        @pl.loop(0, 2)
        def _(n):
            send(d2_send.at[n], d1_recv.at[n], ssem.at[30 + n], rsem.at[30 + n], peer).wait_recv()
            sl = rows(n * HALF, HALF)
            hat, rstd = ln_forward(x[sl, :].astype(F32))
            grad = part[sl, :] + d1_recv[n].astype(F32)
            dx[sl, :] = (dh1[sl, :] + ln_backward(hat, rstd, g1[...], grad)).astype(BF16)

        outs[2].start()
        for j in range(4):
            e_peer(j).wait_send()
            relay(j, core).wait_send()
        for n in range(2):
            e_pair(n).wait_send()
            swap_far(n, 1 - core).wait_send()
            d1_far(n).wait_send()
        w_swap.wait_send()
        swap.wait_send()
        for copy in outs:
            copy.wait()

    tokens = 4 * BLK
    pl.run_scoped(
        phase_two,
        nat_do=pltpu.VMEM((4, tokens, 128), BF16),
        dot_t=pltpu.VMEM((256, tokens), BF16),
        dqt=pltpu.VMEM((256, tokens), F32),
        dkv=pltpu.VMEM((4, tokens, 128), F32),
        wo=pltpu.VMEM((256, 1024), BF16),
        part=pltpu.VMEM((BLK, 1024), F32),
        x=pltpu.VMEM((BLK, 1024), BF16),
        dx=pltpu.VMEM((BLK, 1024), BF16),
        dwqkv=pltpu.VMEM((1024, 768), BF16),
        dwo=pltpu.VMEM((256, 1024), BF16),
        dct=pltpu.VMEM((768, tokens), BF16),
    )


def layer_grads(h1, dy, x, g1, g2, wqkv, w1, w2, wo):
    tokens = 4 * BLK
    vmem = pltpu.VMEM
    shape = jax.ShapeDtypeStruct
    hbm = pl.BlockSpec(memory_space=pl.ANY)
    return pl.pallas_call(
        layer_kernel,
        name="layer_grads",
        out_shape=(shape((BLK, 1024), BF16), shape((1024, 768), BF16), shape((256, 1024), BF16), shape((1024, 1024), BF16), shape((1024, 1024), BF16)),
        in_specs=[hbm] * 3 + [pl.BlockSpec(memory_space=vmem)] * 2 + [hbm] * 4,
        out_specs=[hbm] * 5,
        scratch_shapes=[
            vmem((tokens, 1024), BF16),
            vmem((tokens, 1024), BF16),
            vmem((tokens, 1024), BF16),
            vmem((1024, 1024), BF16),
            vmem((2 * BLK, 1024), BF16),
            vmem((2, HALF, 1024), BF16),
            vmem((2, HALF, 1024), BF16),
            vmem((2, HALF, 1024), BF16),
            vmem((768, 1024), BF16),
            vmem((2, 768, HALF), BF16),
            vmem((768, BLK), BF16),
            vmem((768, 1024), BF16),
            vmem((BLK, 1024), F32),
            vmem((768, tokens), BF16),
            vmem((8, tokens, 64), BF16),
            vmem((4, tokens, 128), BF16),
            vmem((256, tokens), F32),
            vmem((16, tokens), F32),
            pltpu.SemaphoreType.DMA((13,)),
            pltpu.SemaphoreType.DMA((37,)),
            pltpu.SemaphoreType.DMA((37,)),
            pltpu.SemaphoreType.REGULAR,
        ],
        compiler_params=pltpu.CompilerParams(collective_id=0, has_side_effects=True, vmem_limit_bytes=67043328),
        cost_estimate=pl.CostEstimate(flops=80_000_000_000, bytes_accessed=40_000_000, transcendentals=40_000_000),
    )(h1, dy, x, g1, g2, wqkv, w1, w2, wo)


def solution(mesh):
    row_spec = P(('dp', 'tp'), None)
    in_specs = (row_spec, row_spec, row_spec, P(None), P(None), P(None, 'tp'), P('tp', None, None), P(None, 'tp'), P('tp', None))
    out_specs = (row_spec, P('dp', 'tp'), P(('dp', 'tp'), None, None), P('dp', 'tp'), P(('dp', 'tp'), None))

    def device_step(in_rows, mid_rows, gout_rows, ln1_gain, ln2_gain, wqkv_loc, wout_loc, wfc1_loc, wfc2_loc):
        grad_in, grad_wqkv, grad_wout, grad_wfc1, grad_wfc2 = layer_grads(mid_rows, gout_rows, in_rows, ln1_gain.reshape(1, 1024), ln2_gain.reshape(1, 1024), wqkv_loc, wfc1_loc, wfc2_loc, wout_loc.reshape(256, 1024))
        return grad_in, grad_wqkv, grad_wout.reshape(4, 64, 1024), grad_wfc1, grad_wfc2

    return jax.shard_map(device_step, mesh=mesh, in_specs=in_specs, out_specs=out_specs, check_vma=False)
```

```python
import jax
import jax.numpy as jnp
from jax import lax
from jax.experimental import pallas as pl
from jax.experimental.pallas import tpu as pltpu
from jax.sharding import PartitionSpec as P

LN_EPS = 1e-5
GELU_COEF = 0.044715
GELU_SCALE = 0.7978845608028654
LOG2E = 1.4426950408889634
F32 = jnp.float32
BF16 = jnp.bfloat16
BLK = 512
HALF = 256


def ln_forward(rows):
    row_mean = jnp.mean(rows, axis=-1, keepdims=True)
    centered = rows - row_mean
    row_rstd = lax.rsqrt(jnp.mean(centered * centered, axis=-1, keepdims=True) + LN_EPS)
    return centered * row_rstd, row_rstd


def ln_backward(x_hat, row_rstd, ln_gain, grad_norm):
    grad_hat = grad_norm * ln_gain
    proj_one = jnp.mean(grad_hat, axis=-1, keepdims=True)
    proj_two = jnp.mean(grad_hat * x_hat, axis=-1, keepdims=True)
    return row_rstd * (grad_hat - proj_one - x_hat * proj_two)


def gelu_pair(pre_act):
    tanh_val = jnp.tanh(GELU_SCALE * (pre_act + GELU_COEF * pre_act * pre_act * pre_act))
    gelu_val = 0.5 * pre_act * (1.0 + tanh_val)
    gelu_der = 0.5 * (1.0 + tanh_val) + 0.5 * pre_act * (1.0 - tanh_val * tanh_val) * GELU_SCALE * (1.0 + 3.0 * GELU_COEF * pre_act * pre_act)
    return gelu_val, gelu_der


def nn(a, b):
    return lax.dot_general(a, b, (((1,), (0,)), ((), ())), preferred_element_type=F32)


def nt(a, b):
    return lax.dot_general(a, b, (((1,), (1,)), ((), ())), preferred_element_type=F32)


def qkv_block(i, n1, wqkvt, ct, nat, nat_q):
    sl = pl.ds(pl.multiple_of(i * BLK, BLK), BLK)
    for n in range(4):
        c = nt(wqkvt[n * 192:(n + 1) * 192, :], n1[sl, :]).astype(BF16)
        q = c[0:64, :] * jnp.asarray(0.125, BF16)
        ct[n * 192:n * 192 + 64, sl] = q
        ct[n * 192 + 64:n * 192 + 192, sl] = c[64:192, :]
        nat_q[n, sl, :] = jnp.concatenate([q, jnp.zeros_like(q)], axis=0).T
        nat[2 * n, sl, :] = c[64:128, :].T
        nat[2 * n + 1, sl, :] = c[128:192, :].T


def fwd_init(ot, stat):
    ot[...] = jnp.zeros_like(ot)
    stat[0:4, :] = jnp.full((4, stat.shape[1]), -1e30, F32)
    stat[4:16, :] = jnp.zeros((12, stat.shape[1]), F32)


def fwd_tile(ki, qi, diag, ct, nat, ot, stat):
    qs = pl.ds(pl.multiple_of(qi * BLK, BLK), BLK)
    ks = pl.ds(pl.multiple_of(ki * BLK, BLK), BLK)
    for h in range(4):
        s = nn(nat[2 * h, ks, :], ct[3 * h * 64:3 * h * 64 + 64, qs])
        if diag:
            key = lax.broadcasted_iota(jnp.int32, (BLK, BLK), 0)
            query = lax.broadcasted_iota(jnp.int32, (BLK, BLK), 1)
            s = jnp.where(key <= query, s, -1e30)
        m_old = stat[h:h + 1, qs]
        m_new = jnp.maximum(m_old, jnp.max(s, axis=0, keepdims=True))
        alpha = jnp.exp2((m_old - m_new) * LOG2E)
        e = jnp.exp2((s - m_new) * LOG2E)
        stat[h:h + 1, qs] = m_new
        stat[4 + h:5 + h, qs] = stat[4 + h:5 + h, qs] * alpha + jnp.sum(e, axis=0, keepdims=True)
        hs = slice(h * 64, (h + 1) * 64)
        vt = ct[(3 * h + 2) * 64:(3 * h + 3) * 64, ks]
        ot[hs, qs] = ot[hs, qs] * alpha + nn(vt, e.astype(BF16))


def fwd_finish(ot, stat):
    for h in range(4):
        inv = 1.0 / stat[4 + h:5 + h, :]
        stat[4 + h:5 + h, :] = inv
        ot[h * 64:(h + 1) * 64, :] = ot[h * 64:(h + 1) * 64, :] * inv


def do_block(i, e, wo, ot, dot_t, nat_do, stat):
    sl = pl.ds(pl.multiple_of(i * HALF, HALF), HALF)
    d = nt(wo[...], e[sl, :]).astype(BF16)
    dot_t[:, sl] = d
    for h in range(4):
        part = d[h * 64:(h + 1) * 64, :]
        nat_do[h, sl, :] = jnp.concatenate([jnp.zeros_like(part), part], axis=0).T
        stat[8 + h:9 + h, sl] = jnp.sum(part.astype(F32) * ot[h * 64:(h + 1) * 64, sl], axis=0, keepdims=True)


def attn_bwd_tile(k0, ksize, q0, qsize, diag, ct, nat, nat_q, nat_do, dot_t, stat, dqt, dkv):
    ks = pl.ds(pl.multiple_of(k0, HALF), ksize)
    qs = pl.ds(pl.multiple_of(q0, HALF), qsize)
    for h in range(4):
        s = nn(nat[2 * h, ks, :], ct[3 * h * 64:3 * h * 64 + 64, qs])
        r = nn(nat[2 * h + 1, ks, :], dot_t[h * 64:(h + 1) * 64, qs])
        p = jnp.exp2((s - stat[h:h + 1, qs]) * LOG2E) * stat[4 + h:5 + h, qs]
        if diag:
            key = lax.broadcasted_iota(jnp.int32, (ksize, qsize), 0)
            query = lax.broadcasted_iota(jnp.int32, (ksize, qsize), 1)
            p = jnp.where(key <= query, p, 0.0)
        ds = (p * (r - stat[8 + h:9 + h, qs])).astype(BF16)
        dkv[h, ks, :] += nn(p.astype(BF16), nat_do[h, qs, :]) + nn(ds, nat_q[h, qs, :])
        hs = slice(h * 64, (h + 1) * 64)
        dqt[hs, qs] += nn(ct[(3 * h + 1) * 64:(3 * h + 2) * 64, ks], ds)


def pack_dc(i, dqt, dkv, dct):
    sl = pl.ds(pl.multiple_of(i * BLK, BLK), BLK)
    for h in range(4):
        dct[3 * h * 64:3 * h * 64 + 64, sl] = (dqt[h * 64:(h + 1) * 64, sl] * 0.125).astype(BF16)
        dct[(3 * h + 1) * 64:(3 * h + 3) * 64, sl] = dkv[h, sl, :].astype(BF16).T


MESH_ID = pl.DeviceIdType.MESH


def place():
    me = lax.axis_index('tp')
    chip = me // 2
    core = me - chip * 2
    return me, chip, core, chip * 2 + (1 - core), (1 - chip) * 2 + core, (1 - chip) * 2 + (1 - core)


def entry_barrier(others):
    barrier = pltpu.get_barrier_semaphore()
    for other in others:
        pl.semaphore_signal(barrier, inc=1, device_id={'tp': other}, device_id_type=MESH_ID)
    pl.semaphore_wait(barrier, 3)


def send(src, dst, ssem, rsem, to):
    return pltpu.make_async_remote_copy(src_ref=src, dst_ref=dst, send_sem=ssem, recv_sem=rsem, device_id={'tp': to}, device_id_type=MESH_ID)


def rows(start, size):
    return pl.ds(pl.multiple_of(start, size), size)


def tn(a, b):
    return lax.dot_general(a, b, (((0,), (0,)), ((), ())), preferred_element_type=F32)


def ln_rows(src, gain, dst, start):
    @pl.loop(0, 4)
    def _(i):
        hat, _ = ln_forward(src[rows(i * 128, 128), :].astype(F32))
        dst[rows(start + i * 128, 128), :] = (hat * gain[...]).astype(BF16)


def mlp_rows(start, n2, dy, w1, w2t, act, da):
    sl = rows(start, HALF)
    for c in range(4):
        cs = slice(c * 256, (c + 1) * 256)
        gelu_val, gelu_der = gelu_pair(nn(n2[sl, :], w1[:, cs]))
        act[sl, cs] = gelu_val.astype(BF16)
        da[sl, cs] = (nn(dy[sl, :], w2t[:, cs]) * gelu_der).astype(BF16)


def layer_kernel(h1_hbm, dy_hbm, x_hbm, g1, g2, wqkv_hbm, w1_hbm, w2_hbm, wo_hbm,
                 dx_hbm, dwqkv_hbm, dwo_hbm, dw1_hbm, dw2_hbm,
                 n2, dy, n1, w1_pair, da_pair, d2_send, d2_recv, d1_recv, w_pair, dct_far, dct_own, wqkvt, dh1, ct, nat, nat_q, ot, stat,
                 lsem, ssem, rsem, free_sem):
    me, chip, core, pair, peer, diag = place()
    own = rows(me * BLK, BLK)
    e = n2

    def chunk_copy(ref, block, n, first, to):
        sl = rows(block * BLK + n * HALF, HALF)
        return send(ref.at[sl, :], ref.at[sl, :], ssem.at[first + n], rsem.at[first + n], to)

    def d2_far(n):
        return send(d2_send.at[n], d2_recv.at[n], ssem.at[19 + n], rsem.at[19 + n], peer)

    def e_half(block, part_no):
        return e.at[rows(block * BLK + part_no * HALF, HALF), :]

    def e_pair(part_no):
        ref = e_half(me, part_no)
        return send(ref, ref, ssem.at[21 + part_no], rsem.at[21 + part_no], pair)

    def from_pair(part_no):
        ref = e_half(pair, part_no)
        return send(ref, ref, ssem.at[21 + part_no], rsem.at[21 + part_no], pair)

    def e_chunk(block, part_no, who):
        return e.at[rows(block * BLK + part_no * HALF + who * 128, 128), :]

    def e_peer(j):
        ref = e_chunk(chip * 2 + 1 - j // 2, j % 2, core)
        return send(ref, ref, ssem.at[23 + j], rsem.at[23 + j], peer)

    def from_peer(j):
        ref = e_chunk((1 - chip) * 2 + 1 - j // 2, j % 2, core)
        return send(ref, ref, ssem.at[23 + j], rsem.at[23 + j], peer)

    def relay(j, who):
        ref = e_chunk((1 - chip) * 2 + 1 - j // 2, j % 2, who)
        return send(ref, ref, ssem.at[33 + j], rsem.at[33 + j], pair)

    w_swap = send(wqkvt, w_pair, ssem.at[29], rsem.at[29], pair)

    def phase_one(w1, w2t, wqkv, act, da, h1, x, dw1, dw2):
        local = []
        for n, (src, dst) in enumerate(((dy_hbm, dy.at[own, :]), (h1_hbm, h1), (x_hbm, x), (w1_hbm, w1), (w2_hbm, dw2), (wqkv_hbm, wqkv))):
            copy = pltpu.make_async_copy(src, dst, lsem.at[n])
            copy.start()
            local.append(copy)
        l_dy, l_h1, l_x, l_w1, l_w2, l_wqkv = local

        entry_barrier((pair, peer, diag))

        to_pair = [send(ref.at[own, :], ref.at[own, :], ssem.at[n], rsem.at[n], pair) for n, ref in enumerate((n2, dy, n1))]
        to_pair.append(send(w1, w1_pair, ssem.at[3], rsem.at[3], pair))
        l_dy.wait()
        chunk_copy(dy, me, 0, 6, peer).start()
        to_pair[1].start()
        l_h1.wait()
        ln_rows(h1, g2, n2, me * BLK)
        l_x.wait()
        ln_rows(x, g1, n1, me * BLK)
        chunk_copy(n2, me, 0, 4, peer).start()
        chunk_copy(dy, me, 1, 6, peer).start()
        chunk_copy(n2, me, 1, 4, peer).start()
        for n in range(2):
            chunk_copy(n1, me, n, 8, peer).start()
        to_pair[0].start()
        to_pair[2].start()
        l_w1.wait()
        to_pair[3].start()

        l_w2.wait()
        w2t[...] = dw2[...].T

        @pl.loop(0, 4)
        def _(i):
            @pl.when(i == 2)
            def _():
                to_pair[0].wait_recv()
                to_pair[1].wait_recv()

            second = i // 2
            mlp_rows((me + second * (pair - me)) * BLK + (i - 2 * second) * HALF, n2, dy, w1, w2t, act, da)

        da_swap = send(da.at[rows(pair * BLK, BLK), :], da_pair.at[0:BLK, :], ssem.at[16], rsem.at[16], pair)
        da_swap.start()
        l_wqkv.wait()
        wqkvt[...] = wqkv[...].T
        fwd_init(ot, stat)
        to_pair[2].wait_recv()

        @pl.loop(0, 2)
        def _(n):
            qkv_block(chip * 2 + n, n1, wqkvt, ct, nat, nat_q)

        w_swap.start()

        def da_far(n):
            return send(da.at[rows(diag * BLK + n * HALF, HALF), :], da_pair.at[rows(BLK + n * HALF, HALF), :], ssem.at[17 + n], rsem.at[17 + n], pair)

        to_pair[3].wait_recv()

        @pl.loop(0, 2)
        def _(n):
            chunk_copy(dy, peer, n, 6, peer).wait_recv()
            chunk_copy(dy, peer, n, 12, pair).start()
            chunk_copy(n2, peer, n, 4, peer).wait_recv()
            chunk_copy(n2, peer, n, 10, pair).start()

            @pl.loop(0, 2)
            def _(j):
                @pl.when(j == 1)
                def _():
                    chunk_copy(n2, diag, n, 10, pair).wait_recv()
                    chunk_copy(dy, diag, n, 12, pair).wait_recv()

                mlp_rows((peer + j * (diag - peer)) * BLK + n * HALF, n2, dy, w1, w2t, act, da)

            da_far(n).start()
            first = nt(da[rows(peer * BLK + n * HALF, HALF), :], w1[...])
            da_far(n).wait_recv()
            d2_send[n] = (first + nt(da_pair[rows(BLK + n * HALF, HALF), :], w1_pair[...])).astype(BF16)
            d2_far(n).start()

        da_swap.wait_recv()

        @pl.loop(0, 2)
        def _(i):
            sl = rows(i * HALF, HALF)
            dh1[sl, :] = nt(da[rows(me * BLK + i * HALF, HALF), :], w1[...]) + nt(da_pair[sl, :], w1_pair[...])

        outs = [pltpu.make_async_copy(src, dst, lsem.at[6 + n]) for n, (src, dst) in enumerate(((dw1, dw1_hbm), (dw2, dw2_hbm)))]

        @pl.loop(0, 6)
        def _(i):
            @pl.when(i == 2)
            def _():
                @pl.loop(0, 4)
                def _(j):
                    sl = rows(j * 256, 256)
                    dw2[sl, :] = tn(act[:, sl], dy[...]).astype(BF16)
                    dw1[sl, :] = tn(n2[:, sl], da[...]).astype(BF16)

                for copy in outs:
                    copy.start()
                to_pair[0].wait_send()
                for n in range(2):
                    chunk_copy(n2, me, n, 4, peer).wait_send()
                    chunk_copy(n2, peer, n, 10, pair).wait_send()
                for other in (pair, peer):
                    pl.semaphore_signal(free_sem, inc=1, device_id={'tp': other}, device_id_type=MESH_ID)
                for n in range(2):
                    chunk_copy(n1, peer, n, 8, peer).wait_recv()
                    chunk_copy(n1, peer, n, 14, pair).start()

                @pl.loop(0, 2)
                def _(j):
                    @pl.when(j == 1)
                    def _():
                        for n in range(2):
                            chunk_copy(n1, diag, n, 14, pair).wait_recv()

                    qkv_block(peer + j * (diag - peer), n1, wqkvt, ct, nat, nat_q)

            group = i // 2
            far = group % 2
            qi = far * 2 + chip * 2 - 4 * far * chip + i - 2 * group
            low = (1 - far) * (1 - group // 2) * chip * 2
            high = qi + (group // 2) * (chip * 2 - qi)

            @pl.loop(low, high)
            def _(ki):
                fwd_tile(ki, qi, False, ct, nat, ot, stat)

            @pl.when(group < 2)
            def _():
                fwd_tile(qi, qi, True, ct, nat, ot, stat)

        fwd_finish(ot, stat)
        for copy in outs:
            copy.wait()
        for copy in to_pair[1:] + [da_swap]:
            copy.wait_send()
        for n in range(2):
            for ref, block, first, to in ((dy, me, 6, peer), (n1, me, 8, peer), (dy, peer, 12, pair), (n1, peer, 14, pair)):
                chunk_copy(ref, block, n, first, to).wait_send()
            da_far(n).wait_send()
        pl.semaphore_wait(free_sem, 2)

        @pl.loop(0, 2)
        def _(n):
            d2_far(n).wait_recv()
            sl = rows(n * HALF, HALF)
            hat, rstd = ln_forward(h1[sl, :].astype(F32))
            rows_n = rows(me * BLK + n * HALF, HALF)
            grad = dy[rows_n, :].astype(F32) + ln_backward(hat, rstd, g2[...], dh1[sl, :] + d2_recv[n].astype(F32))
            dh1[sl, :] = grad
            e[rows_n, :] = grad.astype(BF16)
            e_pair(n).start()

            @pl.when(n * core == 1)
            def _():
                e_peer(1).start()

            from_pair(n).wait_recv()

            @pl.when(n == 0)
            def _():
                e_peer(0).start()

            @pl.when(n * (1 - core) == 1)
            def _():
                e_peer(1).start()

            @pl.when(n == 1)
            def _():
                e_peer(2).start()
                e_peer(3).start()

    pl.run_scoped(
        phase_one,
        w1=pltpu.VMEM((1024, 1024), BF16),
        w2t=pltpu.VMEM((1024, 1024), BF16),
        wqkv=pltpu.VMEM((1024, 768), BF16),
        act=pltpu.VMEM((4 * BLK, 1024), BF16),
        da=pltpu.VMEM((4 * BLK, 1024), BF16),
        h1=pltpu.VMEM((BLK, 1024), BF16),
        x=pltpu.VMEM((BLK, 1024), BF16),
        dw1=pltpu.VMEM((1024, 1024), BF16),
        dw2=pltpu.VMEM((1024, 1024), BF16),
    )

    def phase_two(nat_do, dot_t, dqt, dkv, wo, part, x, dx, dwqkv, dwo, dct):
        l_wo = pltpu.make_async_copy(wo_hbm, wo, lsem.at[8])
        l_wo.start()
        l_x = pltpu.make_async_copy(x_hbm, x, lsem.at[9])
        l_x.start()
        dkv[...] = jnp.zeros_like(dkv)
        dqt[...] = jnp.zeros_like(dqt)
        for n in range(2):
            d2_far(n).wait_send()
        l_wo.wait()

        @pl.loop(0, 4)
        def _(n):
            do_block(chip * 4 + n, e, wo, ot, dot_t, nat_do, stat)

        w_swap.wait_recv()

        def swap_far(n, mine_or_theirs):
            block = (1 - chip) * 2 + 1 - n
            return send(dct.at[:, rows(block * BLK + mine_or_theirs * HALF, HALF)], dct_far.at[n], ssem.at[27 + n], rsem.at[27 + n], pair)

        def d1_far(n):
            return send(d2_send.at[n], d1_recv.at[core], ssem.at[30 + n], rsem.at[30 + core], (1 - chip) * 2 + 1 - n)

        def take_far(n):
            for half in range(2):
                from_peer(2 * n + half).wait_recv()
                relay(2 * n + half, core).start()

        def far_do(n):
            for half in range(2):
                relay(2 * n + half, 1 - core).wait_recv()

            @pl.loop(0, 2)
            def _(half):
                do_block(((1 - chip) * 2 + 1 - n) * 2 + half, e, wo, ot, dot_t, nat_do, stat)

        @pl.loop(0, 6)
        def _(i):
            group = i // 2
            far = group % 2
            n = i - 2 * group
            qi = (1 - far) * (chip * 2 + n) + far * ((1 - chip) * 2 + 1 - n)
            low = (group // 2) * chip * 2
            high = far * qi + (1 - far) * ((1 - group // 2) * ((1 - chip) * qi + chip * 2) + (group // 2) * chip * qi)

            @pl.when(i == 2)
            def _():
                take_far(0)

            @pl.when(far == 1)
            def _():
                far_do(n)

            @pl.loop(low, high)
            def _(ki):
                attn_bwd_tile(ki * BLK, BLK, qi * BLK, BLK, False, ct, nat, nat_q, nat_do, dot_t, stat, dqt, dkv)

            @pl.when(far + (1 - far) * ((1 - group // 2) * (1 - chip) + (group // 2) * chip) == 1)
            def _():
                attn_bwd_tile(qi * BLK, HALF, qi * BLK, BLK, True, ct, nat, nat_q, nat_do, dot_t, stat, dqt, dkv)
                attn_bwd_tile(qi * BLK + HALF, HALF, qi * BLK + HALF, HALF, True, ct, nat, nat_q, nat_do, dot_t, stat, dqt, dkv)

            @pl.when(far == 1)
            def _():
                pack_dc(qi, dqt, dkv, dct)
                swap_far(n, 1 - core).start()
                part[0:HALF, :] = nn(dct[:, rows(qi * BLK + core * HALF, HALF)].T, wqkvt[...])
                swap_far(n, core).wait_recv()
                d2_send[n] = (part[0:HALF, :] + nn(dct_far[n].T, w_pair[...])).astype(BF16)
                d1_far(n).start()

                @pl.when(n == 0)
                def _():
                    take_far(1)

        @pl.loop(0, 2)
        def _(n):
            pack_dc(chip * 2 + n, dqt, dkv, dct)

        swap = send(dct.at[:, rows(pair * BLK, BLK)], dct_own, ssem.at[32], rsem.at[32], pair)
        swap.start()
        part[...] = nn(dct[:, own].T, wqkvt[...])
        swap.wait_recv()
        part[...] += nn(dct_own[...].T, w_pair[...])

        @pl.loop(0, 4)
        def _(i):
            sl = rows(i * 256, 256)
            dwo[:, sl] = nn(ot[...].astype(BF16), e[:, sl]).astype(BF16)
            dwqkv[sl, :] = nn(dct[...], n1[:, sl]).astype(BF16).T

        outs = [pltpu.make_async_copy(src, dst, lsem.at[10 + n]) for n, (src, dst) in enumerate(((dwqkv, dwqkv_hbm), (dwo, dwo_hbm), (dx, dx_hbm)))]
        outs[0].start()
        outs[1].start()
        l_x.wait()

        @pl.loop(0, 2)
        def _(n):
            send(d2_send.at[n], d1_recv.at[n], ssem.at[30 + n], rsem.at[30 + n], peer).wait_recv()
            sl = rows(n * HALF, HALF)
            hat, rstd = ln_forward(x[sl, :].astype(F32))
            grad = part[sl, :] + d1_recv[n].astype(F32)
            dx[sl, :] = (dh1[sl, :] + ln_backward(hat, rstd, g1[...], grad)).astype(BF16)

        outs[2].start()
        for j in range(4):
            e_peer(j).wait_send()
            relay(j, core).wait_send()
        for n in range(2):
            e_pair(n).wait_send()
            swap_far(n, 1 - core).wait_send()
            d1_far(n).wait_send()
        w_swap.wait_send()
        swap.wait_send()
        for copy in outs:
            copy.wait()

    tokens = 4 * BLK
    pl.run_scoped(
        phase_two,
        nat_do=pltpu.VMEM((4, tokens, 128), BF16),
        dot_t=pltpu.VMEM((256, tokens), BF16),
        dqt=pltpu.VMEM((256, tokens), F32),
        dkv=pltpu.VMEM((4, tokens, 128), F32),
        wo=pltpu.VMEM((256, 1024), BF16),
        part=pltpu.VMEM((BLK, 1024), F32),
        x=pltpu.VMEM((BLK, 1024), BF16),
        dx=pltpu.VMEM((BLK, 1024), BF16),
        dwqkv=pltpu.VMEM((1024, 768), BF16),
        dwo=pltpu.VMEM((256, 1024), BF16),
        dct=pltpu.VMEM((768, tokens), BF16),
    )


def layer_grads(h1, dy, x, g1, g2, wqkv, w1, w2, wo):
    tokens = 4 * BLK
    vmem = pltpu.VMEM
    shape = jax.ShapeDtypeStruct
    hbm = pl.BlockSpec(memory_space=pl.ANY)
    return pl.pallas_call(
        layer_kernel,
        name="layer_grads",
        out_shape=(shape((BLK, 1024), BF16), shape((1024, 768), BF16), shape((256, 1024), BF16), shape((1024, 1024), BF16), shape((1024, 1024), BF16)),
        in_specs=[hbm] * 3 + [pl.BlockSpec(memory_space=vmem)] * 2 + [hbm] * 4,
        out_specs=[hbm] * 5,
        scratch_shapes=[
            vmem((tokens, 1024), BF16),
            vmem((tokens, 1024), BF16),
            vmem((tokens, 1024), BF16),
            vmem((1024, 1024), BF16),
            vmem((2 * BLK, 1024), BF16),
            vmem((2, HALF, 1024), BF16),
            vmem((2, HALF, 1024), BF16),
            vmem((2, HALF, 1024), BF16),
            vmem((768, 1024), BF16),
            vmem((2, 768, HALF), BF16),
            vmem((768, BLK), BF16),
            vmem((768, 1024), BF16),
            vmem((BLK, 1024), F32),
            vmem((768, tokens), BF16),
            vmem((8, tokens, 64), BF16),
            vmem((4, tokens, 128), BF16),
            vmem((256, tokens), F32),
            vmem((16, tokens), F32),
            pltpu.SemaphoreType.DMA((13,)),
            pltpu.SemaphoreType.DMA((37,)),
            pltpu.SemaphoreType.DMA((37,)),
            pltpu.SemaphoreType.REGULAR,
        ],
        compiler_params=pltpu.CompilerParams(collective_id=0, has_side_effects=True, vmem_limit_bytes=67043328),
        cost_estimate=pl.CostEstimate(flops=80_000_000_000, bytes_accessed=40_000_000, transcendentals=40_000_000),
    )(h1, dy, x, g1, g2, wqkv, w1, w2, wo)


def copy_kernel(*refs):
    count = (len(refs) - 2) // 3
    srcs, dsts, bufs, in_sem, out_sem = refs[:count], refs[count:2 * count], refs[2 * count:3 * count], refs[-2], refs[-1]
    reads = [pltpu.make_async_copy(src, buf, in_sem.at[n]) for n, (src, buf) in enumerate(zip(srcs, bufs))]
    writes = [pltpu.make_async_copy(buf, dst, out_sem.at[n]) for n, (dst, buf) in enumerate(zip(dsts, bufs))]
    for copy in reads:
        copy.start()
    for read, write in zip(reads, writes):
        read.wait()
        write.start()
    for copy in writes:
        copy.wait()


def copy_out(*arrays):
    hbm = pl.BlockSpec(memory_space=pl.ANY)
    return pl.pallas_call(
        copy_kernel,
        name="copy_out",
        out_shape=[jax.ShapeDtypeStruct(a.shape, a.dtype) for a in arrays],
        in_specs=[hbm] * len(arrays),
        out_specs=[hbm] * len(arrays),
        scratch_shapes=[pltpu.VMEM(a.shape, a.dtype) for a in arrays] + [pltpu.SemaphoreType.DMA((len(arrays),))] * 2,
        compiler_params=pltpu.CompilerParams(vmem_limit_bytes=67043328),
    )(*arrays)


def solution(mesh):
    row_spec = P(('dp', 'tp'), None)
    in_specs = (row_spec, row_spec, row_spec, P(None), P(None), P(None, 'tp'), P('tp', None, None), P(None, 'tp'), P('tp', None))
    out_specs = (row_spec, P('dp', 'tp'), P(('dp', 'tp'), None, None), P('dp', 'tp'), P(('dp', 'tp'), None))

    def device_step(in_rows, mid_rows, gout_rows, ln1_gain, ln2_gain, wqkv_loc, wout_loc, wfc1_loc, wfc2_loc):
        grad_in, grad_wqkv, grad_wout, grad_wfc1, grad_wfc2 = copy_out(*layer_grads(mid_rows, gout_rows, in_rows, ln1_gain.reshape(1, 1024), ln2_gain.reshape(1, 1024), wqkv_loc, wfc1_loc, wfc2_loc, wout_loc.reshape(256, 1024)))
        return grad_in, grad_wqkv, grad_wout.reshape(4, 64, 1024), grad_wfc1, grad_wfc2

    return jax.shard_map(device_step, mesh=mesh, in_specs=in_specs, out_specs=out_specs, check_vma=False)
```

```python
import jax
import jax.numpy as jnp
from jax import lax
from jax.experimental import pallas as pl
from jax.experimental.pallas import tpu as pltpu
from jax.sharding import PartitionSpec as P

LN_EPS = 1e-5
GELU_COEF = 0.044715
GELU_SCALE = 0.7978845608028654
LOG2E = 1.4426950408889634
F32 = jnp.float32
BF16 = jnp.bfloat16
BLK = 512
HALF = 256


def ln_forward(rows):
    row_mean = jnp.mean(rows, axis=-1, keepdims=True)
    centered = rows - row_mean
    row_rstd = lax.rsqrt(jnp.mean(centered * centered, axis=-1, keepdims=True) + LN_EPS)
    return centered * row_rstd, row_rstd


def ln_backward(x_hat, row_rstd, ln_gain, grad_norm):
    grad_hat = grad_norm * ln_gain
    proj_one = jnp.mean(grad_hat, axis=-1, keepdims=True)
    proj_two = jnp.mean(grad_hat * x_hat, axis=-1, keepdims=True)
    return row_rstd * (grad_hat - proj_one - x_hat * proj_two)


def gelu_pair(pre_act):
    tanh_val = jnp.tanh(GELU_SCALE * (pre_act + GELU_COEF * pre_act * pre_act * pre_act))
    gelu_val = 0.5 * pre_act * (1.0 + tanh_val)
    gelu_der = 0.5 * (1.0 + tanh_val) + 0.5 * pre_act * (1.0 - tanh_val * tanh_val) * GELU_SCALE * (1.0 + 3.0 * GELU_COEF * pre_act * pre_act)
    return gelu_val, gelu_der


def nn(a, b):
    return lax.dot_general(a, b, (((1,), (0,)), ((), ())), preferred_element_type=F32)


def nt(a, b):
    return lax.dot_general(a, b, (((1,), (1,)), ((), ())), preferred_element_type=F32)


def qkv_block(i, n1, wqkvt, ct, nat):
    sl = pl.ds(pl.multiple_of(i * BLK, BLK), BLK)
    for n in range(4):
        c = nt(wqkvt[n * 192:(n + 1) * 192, :], n1[sl, :]).astype(BF16)
        q = c[0:64, :] * jnp.asarray(0.125, BF16)
        ct[n * 192:n * 192 + 64, sl] = q
        ct[n * 192 + 64:n * 192 + 192, sl] = c[64:192, :]
        nat[2 * n, sl, :] = c[64:128, :].T
        nat[2 * n + 1, sl, :] = c[128:192, :].T


def fwd_init(ot, stat):
    ot[...] = jnp.zeros_like(ot)
    stat[0:4, :] = jnp.full((4, stat.shape[1]), -1e30, F32)
    stat[4:16, :] = jnp.zeros((12, stat.shape[1]), F32)


def fwd_tile(ki, qi, diag, ct, nat, ot, stat):
    qs = pl.ds(pl.multiple_of(qi * BLK, BLK), BLK)
    ks = pl.ds(pl.multiple_of(ki * BLK, BLK), BLK)
    for h in range(4):
        s = nn(nat[2 * h, ks, :], ct[3 * h * 64:3 * h * 64 + 64, qs])
        if diag:
            key = lax.broadcasted_iota(jnp.int32, (BLK, BLK), 0)
            query = lax.broadcasted_iota(jnp.int32, (BLK, BLK), 1)
            s = jnp.where(key <= query, s, -1e30)
        m_old = stat[h:h + 1, qs]
        m_new = jnp.maximum(m_old, jnp.max(s, axis=0, keepdims=True))
        alpha = jnp.exp2((m_old - m_new) * LOG2E)
        e = jnp.exp2((s - m_new) * LOG2E)
        stat[h:h + 1, qs] = m_new
        stat[4 + h:5 + h, qs] = stat[4 + h:5 + h, qs] * alpha + jnp.sum(e, axis=0, keepdims=True)
        hs = slice(h * 64, (h + 1) * 64)
        vt = ct[(3 * h + 2) * 64:(3 * h + 3) * 64, ks]
        ot[hs, qs] = ot[hs, qs] * alpha + nn(vt, e.astype(BF16))


def fwd_finish(ot, stat):
    for h in range(4):
        inv = 1.0 / stat[4 + h:5 + h, :]
        stat[4 + h:5 + h, :] = inv
        ot[h * 64:(h + 1) * 64, :] = ot[h * 64:(h + 1) * 64, :] * inv


def do_block(i, e, wo, ot, dot_t, stat):
    sl = pl.ds(pl.multiple_of(i * HALF, HALF), HALF)
    d = nt(wo[...], e[sl, :]).astype(BF16)
    dot_t[:, sl] = d
    for h in range(4):
        part = d[h * 64:(h + 1) * 64, :]
        stat[8 + h:9 + h, sl] = jnp.sum(part.astype(F32) * ot[h * 64:(h + 1) * 64, sl], axis=0, keepdims=True)


def attn_bwd_tile(k0, ksize, q0, qsize, diag, ct, nat, dot_t, stat, dqt, dkt, dvt):
    ks = pl.ds(pl.multiple_of(k0, HALF), ksize)
    qs = pl.ds(pl.multiple_of(q0, HALF), qsize)
    for h in range(4):
        s = nn(nat[2 * h, ks, :], ct[3 * h * 64:3 * h * 64 + 64, qs])
        r = nn(nat[2 * h + 1, ks, :], dot_t[h * 64:(h + 1) * 64, qs])
        p = jnp.exp2((s - stat[h:h + 1, qs]) * LOG2E) * stat[4 + h:5 + h, qs]
        if diag:
            key = lax.broadcasted_iota(jnp.int32, (ksize, qsize), 0)
            query = lax.broadcasted_iota(jnp.int32, (ksize, qsize), 1)
            p = jnp.where(key <= query, p, 0.0)
        ds = (p * (r - stat[8 + h:9 + h, qs])).astype(BF16)
        hs = slice(h * 64, (h + 1) * 64)
        dvt[hs, ks] += nt(dot_t[hs, qs], p.astype(BF16))
        dkt[hs, ks] += nt(ct[3 * h * 64:3 * h * 64 + 64, qs], ds)
        dqt[hs, qs] += nn(ct[(3 * h + 1) * 64:(3 * h + 2) * 64, ks], ds)


def pack_dc(i, dqt, dkt, dvt, dct):
    sl = pl.ds(pl.multiple_of(i * BLK, BLK), BLK)
    for h in range(4):
        dct[3 * h * 64:3 * h * 64 + 64, sl] = (dqt[h * 64:(h + 1) * 64, sl] * 0.125).astype(BF16)
        dct[(3 * h + 1) * 64:(3 * h + 2) * 64, sl] = dkt[h * 64:(h + 1) * 64, sl].astype(BF16)
        dct[(3 * h + 2) * 64:(3 * h + 3) * 64, sl] = dvt[h * 64:(h + 1) * 64, sl].astype(BF16)


MESH_ID = pl.DeviceIdType.MESH


def place():
    me = lax.axis_index('tp')
    chip = me // 2
    core = me - chip * 2
    return me, chip, core, chip * 2 + (1 - core), (1 - chip) * 2 + core, (1 - chip) * 2 + (1 - core)


def entry_barrier(others):
    barrier = pltpu.get_barrier_semaphore()
    for other in others:
        pl.semaphore_signal(barrier, inc=1, device_id={'tp': other}, device_id_type=MESH_ID)
    pl.semaphore_wait(barrier, 3)


def send(src, dst, ssem, rsem, to):
    return pltpu.make_async_remote_copy(src_ref=src, dst_ref=dst, send_sem=ssem, recv_sem=rsem, device_id={'tp': to}, device_id_type=MESH_ID)


def rows(start, size):
    return pl.ds(pl.multiple_of(start, size), size)


def tn(a, b):
    return lax.dot_general(a, b, (((0,), (0,)), ((), ())), preferred_element_type=F32)


def ln_rows(src, gain, dst, start):
    @pl.loop(0, 4)
    def _(i):
        hat, _ = ln_forward(src[rows(i * 128, 128), :].astype(F32))
        dst[rows(start + i * 128, 128), :] = (hat * gain[...]).astype(BF16)


def mlp_rows(start, n2, dy, w1, w2t, act, da):
    sl = rows(start, HALF)
    for c in range(4):
        cs = slice(c * 256, (c + 1) * 256)
        gelu_val, gelu_der = gelu_pair(nn(n2[sl, :], w1[:, cs]))
        act[sl, cs] = gelu_val.astype(BF16)
        da[sl, cs] = (nn(dy[sl, :], w2t[:, cs]) * gelu_der).astype(BF16)


def layer_kernel(h1_hbm, dy_hbm, x_hbm, g1, g2, wqkv_hbm, w1_hbm, w2_hbm, wo_hbm,
                 dx_hbm, dwqkv_hbm, dwo_hbm, dw1_hbm, dw2_hbm,
                 n2, dy, n1, w1_pair, da_pair, d2_send, d2_recv, d1_recv, w_pair, dct_far, dct_own, wqkvt, dh1, ct, nat, ot, stat,
                 lsem, ssem, rsem, free_sem):
    me, chip, core, pair, peer, diag = place()
    own = rows(me * BLK, BLK)
    e = n2

    def chunk_copy(ref, block, n, first, to):
        sl = rows(block * BLK + n * HALF, HALF)
        return send(ref.at[sl, :], ref.at[sl, :], ssem.at[first + n], rsem.at[first + n], to)

    def d2_far(n):
        return send(d2_send.at[n], d2_recv.at[n], ssem.at[19 + n], rsem.at[19 + n], peer)

    def e_half(block, part_no):
        return e.at[rows(block * BLK + part_no * HALF, HALF), :]

    def e_pair(part_no):
        ref = e_half(me, part_no)
        return send(ref, ref, ssem.at[21 + part_no], rsem.at[21 + part_no], pair)

    def from_pair(part_no):
        ref = e_half(pair, part_no)
        return send(ref, ref, ssem.at[21 + part_no], rsem.at[21 + part_no], pair)

    def e_chunk(block, part_no, who):
        return e.at[rows(block * BLK + part_no * HALF + who * 128, 128), :]

    def e_peer(j):
        ref = e_chunk(chip * 2 + 1 - j // 2, j % 2, core)
        return send(ref, ref, ssem.at[23 + j], rsem.at[23 + j], peer)

    def from_peer(j):
        ref = e_chunk((1 - chip) * 2 + 1 - j // 2, j % 2, core)
        return send(ref, ref, ssem.at[23 + j], rsem.at[23 + j], peer)

    def relay(j, who):
        ref = e_chunk((1 - chip) * 2 + 1 - j // 2, j % 2, who)
        return send(ref, ref, ssem.at[33 + j], rsem.at[33 + j], pair)

    w_swap = send(wqkvt, w_pair, ssem.at[29], rsem.at[29], pair)

    def phase_one(w1, w2t, wqkv, act, da, h1, x, dw1, dw2):
        local = []
        for n, (src, dst) in enumerate(((dy_hbm, dy.at[own, :]), (h1_hbm, h1), (x_hbm, x), (w1_hbm, w1), (w2_hbm, dw2), (wqkv_hbm, wqkv))):
            copy = pltpu.make_async_copy(src, dst, lsem.at[n])
            copy.start()
            local.append(copy)
        l_dy, l_h1, l_x, l_w1, l_w2, l_wqkv = local

        entry_barrier((pair, peer, diag))

        to_pair = [send(ref.at[own, :], ref.at[own, :], ssem.at[n], rsem.at[n], pair) for n, ref in enumerate((n2, dy, n1))]
        to_pair.append(send(w1, w1_pair, ssem.at[3], rsem.at[3], pair))
        l_dy.wait()
        chunk_copy(dy, me, 0, 6, peer).start()
        to_pair[1].start()
        l_h1.wait()
        ln_rows(h1, g2, n2, me * BLK)
        l_x.wait()
        ln_rows(x, g1, n1, me * BLK)
        chunk_copy(n2, me, 0, 4, peer).start()
        chunk_copy(dy, me, 1, 6, peer).start()
        chunk_copy(n2, me, 1, 4, peer).start()
        for n in range(2):
            chunk_copy(n1, me, n, 8, peer).start()
        to_pair[0].start()
        to_pair[2].start()
        l_w1.wait()
        to_pair[3].start()

        l_w2.wait()
        w2t[...] = dw2[...].T

        @pl.loop(0, 4)
        def _(i):
            @pl.when(i == 2)
            def _():
                to_pair[0].wait_recv()
                to_pair[1].wait_recv()

            second = i // 2
            mlp_rows((me + second * (pair - me)) * BLK + (i - 2 * second) * HALF, n2, dy, w1, w2t, act, da)

        da_swap = send(da.at[rows(pair * BLK, BLK), :], da_pair.at[0:BLK, :], ssem.at[16], rsem.at[16], pair)
        da_swap.start()
        l_wqkv.wait()
        wqkvt[...] = wqkv[...].T
        fwd_init(ot, stat)
        to_pair[2].wait_recv()

        @pl.loop(0, 2)
        def _(n):
            qkv_block(chip * 2 + n, n1, wqkvt, ct, nat)

        w_swap.start()

        def da_far(n):
            return send(da.at[rows(diag * BLK + n * HALF, HALF), :], da_pair.at[rows(BLK + n * HALF, HALF), :], ssem.at[17 + n], rsem.at[17 + n], pair)

        to_pair[3].wait_recv()

        @pl.loop(0, 2)
        def _(n):
            chunk_copy(dy, peer, n, 6, peer).wait_recv()
            chunk_copy(dy, peer, n, 12, pair).start()
            chunk_copy(n2, peer, n, 4, peer).wait_recv()
            chunk_copy(n2, peer, n, 10, pair).start()

            @pl.loop(0, 2)
            def _(j):
                @pl.when(j == 1)
                def _():
                    chunk_copy(n2, diag, n, 10, pair).wait_recv()
                    chunk_copy(dy, diag, n, 12, pair).wait_recv()

                mlp_rows((peer + j * (diag - peer)) * BLK + n * HALF, n2, dy, w1, w2t, act, da)

            da_far(n).start()
            first = nt(da[rows(peer * BLK + n * HALF, HALF), :], w1[...])
            da_far(n).wait_recv()
            d2_send[n] = (first + nt(da_pair[rows(BLK + n * HALF, HALF), :], w1_pair[...])).astype(BF16)
            d2_far(n).start()

        da_swap.wait_recv()

        @pl.loop(0, 2)
        def _(i):
            sl = rows(i * HALF, HALF)
            dh1[sl, :] = nt(da[rows(me * BLK + i * HALF, HALF), :], w1[...]) + nt(da_pair[sl, :], w1_pair[...])

        outs = [pltpu.make_async_copy(src, dst, lsem.at[6 + n]) for n, (src, dst) in enumerate(((dw1, dw1_hbm), (dw2, dw2_hbm)))]

        @pl.loop(0, 6)
        def _(i):
            @pl.when(i == 2)
            def _():
                @pl.loop(0, 4)
                def _(j):
                    sl = rows(j * 256, 256)
                    dw2[sl, :] = tn(act[:, sl], dy[...]).astype(BF16)
                    dw1[sl, :] = tn(n2[:, sl], da[...]).astype(BF16)

                for copy in outs:
                    copy.start()
                to_pair[0].wait_send()
                for n in range(2):
                    chunk_copy(n2, me, n, 4, peer).wait_send()
                    chunk_copy(n2, peer, n, 10, pair).wait_send()
                for other in (pair, peer):
                    pl.semaphore_signal(free_sem, inc=1, device_id={'tp': other}, device_id_type=MESH_ID)
                for n in range(2):
                    chunk_copy(n1, peer, n, 8, peer).wait_recv()
                    chunk_copy(n1, peer, n, 14, pair).start()

                @pl.loop(0, 2)
                def _(j):
                    @pl.when(j == 1)
                    def _():
                        for n in range(2):
                            chunk_copy(n1, diag, n, 14, pair).wait_recv()

                    qkv_block(peer + j * (diag - peer), n1, wqkvt, ct, nat)

            group = i // 2
            far = group % 2
            qi = far * 2 + chip * 2 - 4 * far * chip + i - 2 * group
            low = (1 - far) * (1 - group // 2) * chip * 2
            high = qi + (group // 2) * (chip * 2 - qi)

            @pl.loop(low, high)
            def _(ki):
                fwd_tile(ki, qi, False, ct, nat, ot, stat)

            @pl.when(group < 2)
            def _():
                fwd_tile(qi, qi, True, ct, nat, ot, stat)

        fwd_finish(ot, stat)
        for copy in outs:
            copy.wait()
        for copy in to_pair[1:] + [da_swap]:
            copy.wait_send()
        for n in range(2):
            for ref, block, first, to in ((dy, me, 6, peer), (n1, me, 8, peer), (dy, peer, 12, pair), (n1, peer, 14, pair)):
                chunk_copy(ref, block, n, first, to).wait_send()
            da_far(n).wait_send()
        pl.semaphore_wait(free_sem, 2)

        @pl.loop(0, 2)
        def _(n):
            d2_far(n).wait_recv()
            sl = rows(n * HALF, HALF)
            hat, rstd = ln_forward(h1[sl, :].astype(F32))
            rows_n = rows(me * BLK + n * HALF, HALF)
            grad = dy[rows_n, :].astype(F32) + ln_backward(hat, rstd, g2[...], dh1[sl, :] + d2_recv[n].astype(F32))
            dh1[sl, :] = grad
            e[rows_n, :] = grad.astype(BF16)
            e_pair(n).start()

            @pl.when(n * core == 1)
            def _():
                e_peer(1).start()

            from_pair(n).wait_recv()

            @pl.when(n == 0)
            def _():
                e_peer(0).start()

            @pl.when(n * (1 - core) == 1)
            def _():
                e_peer(1).start()

            @pl.when(n == 1)
            def _():
                e_peer(2).start()
                e_peer(3).start()

    pl.run_scoped(
        phase_one,
        w1=pltpu.VMEM((1024, 1024), BF16),
        w2t=pltpu.VMEM((1024, 1024), BF16),
        wqkv=pltpu.VMEM((1024, 768), BF16),
        act=pltpu.VMEM((4 * BLK, 1024), BF16),
        da=pltpu.VMEM((4 * BLK, 1024), BF16),
        h1=pltpu.VMEM((BLK, 1024), BF16),
        x=pltpu.VMEM((BLK, 1024), BF16),
        dw1=pltpu.VMEM((1024, 1024), BF16),
        dw2=pltpu.VMEM((1024, 1024), BF16),
    )

    def phase_two(dot_t, dqt, dkt, dvt, wo, part, x, dx, dwqkv, dwo, dct):
        l_wo = pltpu.make_async_copy(wo_hbm, wo, lsem.at[8])
        l_wo.start()
        l_x = pltpu.make_async_copy(x_hbm, x, lsem.at[9])
        l_x.start()
        dkt[...] = jnp.zeros_like(dkt)
        dvt[...] = jnp.zeros_like(dvt)
        dqt[...] = jnp.zeros_like(dqt)
        for n in range(2):
            d2_far(n).wait_send()
        l_wo.wait()

        @pl.loop(0, 4)
        def _(n):
            do_block(chip * 4 + n, e, wo, ot, dot_t, stat)

        w_swap.wait_recv()

        def swap_far(n, mine_or_theirs):
            block = (1 - chip) * 2 + 1 - n
            return send(dct.at[:, rows(block * BLK + mine_or_theirs * HALF, HALF)], dct_far.at[n], ssem.at[27 + n], rsem.at[27 + n], pair)

        def d1_far(n, piece):
            sl = rows(piece * 128, 128)
            return send(d2_send.at[n, sl, :], d1_recv.at[core, sl, :], ssem.at[30 + n + 7 * piece], rsem.at[30 + core + 7 * piece], (1 - chip) * 2 + 1 - n)

        def take_far(n):
            for half in range(2):
                from_peer(2 * n + half).wait_recv()
                relay(2 * n + half, core).start()

        def far_do(n):
            for half in range(2):
                relay(2 * n + half, 1 - core).wait_recv()

            @pl.loop(0, 2)
            def _(half):
                do_block(((1 - chip) * 2 + 1 - n) * 2 + half, e, wo, ot, dot_t, stat)

        @pl.loop(0, 6)
        def _(i):
            group = i // 2
            far = group % 2
            n = i - 2 * group
            qi = (1 - far) * (chip * 2 + n) + far * ((1 - chip) * 2 + 1 - n)
            low = (group // 2) * chip * 2
            high = far * qi + (1 - far) * ((1 - group // 2) * ((1 - chip) * qi + chip * 2) + (group // 2) * chip * qi)

            @pl.when(i == 2)
            def _():
                take_far(0)
                far_do(0)

            @pl.loop(low, high)
            def _(ki):
                attn_bwd_tile(ki * BLK, BLK, qi * BLK, BLK, False, ct, nat, dot_t, stat, dqt, dkt, dvt)

            @pl.when(far + (1 - far) * ((1 - group // 2) * (1 - chip) + (group // 2) * chip) == 1)
            def _():
                attn_bwd_tile(qi * BLK, HALF, qi * BLK, BLK, True, ct, nat, dot_t, stat, dqt, dkt, dvt)
                attn_bwd_tile(qi * BLK + HALF, HALF, qi * BLK + HALF, HALF, True, ct, nat, dot_t, stat, dqt, dkt, dvt)

            @pl.when(far == 1)
            def _():
                pack_dc(qi, dqt, dkt, dvt, dct)
                swap_far(n, 1 - core).start()
                part[0:HALF, :] = nn(dct[:, rows(qi * BLK + core * HALF, HALF)].T, wqkvt[...])

                @pl.when(n == 0)
                def _():
                    take_far(1)
                    far_do(1)

                swap_far(n, core).wait_recv()

                @pl.loop(0, 2)
                def _(piece):
                    sl = rows(piece * 128, 128)
                    d2_send[n, sl, :] = (part[sl, :] + nn(dct_far[n, :, sl].T, w_pair[...])).astype(BF16)
                    d1_far(n, piece).start()

        @pl.loop(0, 2)
        def _(n):
            pack_dc(chip * 2 + n, dqt, dkt, dvt, dct)

        swap = send(dct.at[:, rows(pair * BLK, BLK)], dct_own, ssem.at[32], rsem.at[32], pair)
        swap.start()
        part[...] = nn(dct[:, own].T, wqkvt[...])
        swap.wait_recv()
        part[...] += nn(dct_own[...].T, w_pair[...])

        @pl.loop(0, 4)
        def _(i):
            sl = rows(i * 256, 256)
            dwo[:, sl] = nn(ot[...].astype(BF16), e[:, sl]).astype(BF16)
            dwqkv[sl, :] = nn(dct[...], n1[:, sl]).astype(BF16).T

        outs = [pltpu.make_async_copy(src, dst, lsem.at[10 + n]) for n, (src, dst) in enumerate(((dwqkv, dwqkv_hbm), (dwo, dwo_hbm)))]
        outs[0].start()
        outs[1].start()
        l_x.wait()

        def dx_out(k):
            sl = rows(k * 128, 128)
            return pltpu.make_async_copy(dx.at[sl, :], dx_hbm.at[sl, :], lsem.at[12 + k])

        @pl.loop(0, 4)
        def _(i):
            piece = i // 2
            n = i - 2 * piece
            arrived = rows(piece * 128, 128)
            send(d2_send.at[n, arrived, :], d1_recv.at[n, arrived, :], ssem.at[30 + n + 7 * piece], rsem.at[30 + n + 7 * piece], peer).wait_recv()
            sl = rows(n * HALF + piece * 128, 128)
            hat, rstd = ln_forward(x[sl, :].astype(F32))
            grad = part[sl, :] + d1_recv[n, arrived, :].astype(F32)
            dx[sl, :] = (dh1[sl, :] + ln_backward(hat, rstd, g1[...], grad)).astype(BF16)
            dx_out(n * 2 + piece).start()

        for j in range(4):
            e_peer(j).wait_send()
            relay(j, core).wait_send()
        for n in range(2):
            e_pair(n).wait_send()
            swap_far(n, 1 - core).wait_send()
            for piece in range(2):
                d1_far(n, piece).wait_send()
        w_swap.wait_send()
        swap.wait_send()
        for copy in outs + [dx_out(k) for k in range(4)]:
            copy.wait()

    tokens = 4 * BLK
    pl.run_scoped(
        phase_two,
        dot_t=pltpu.VMEM((256, tokens), BF16),
        dqt=pltpu.VMEM((256, tokens), F32),
        dkt=pltpu.VMEM((256, tokens), F32),
        dvt=pltpu.VMEM((256, tokens), F32),
        wo=pltpu.VMEM((256, 1024), BF16),
        part=pltpu.VMEM((BLK, 1024), F32),
        x=pltpu.VMEM((BLK, 1024), BF16),
        dx=pltpu.VMEM((BLK, 1024), BF16),
        dwqkv=pltpu.VMEM((1024, 768), BF16),
        dwo=pltpu.VMEM((256, 1024), BF16),
        dct=pltpu.VMEM((768, tokens), BF16),
    )


def layer_grads(h1, dy, x, g1, g2, wqkv, w1, w2, wo):
    tokens = 4 * BLK
    vmem = pltpu.VMEM
    shape = jax.ShapeDtypeStruct
    hbm = pl.BlockSpec(memory_space=pl.ANY)
    return pl.pallas_call(
        layer_kernel,
        name="layer_grads",
        out_shape=(shape((BLK, 1024), BF16), shape((1024, 768), BF16), shape((256, 1024), BF16), shape((1024, 1024), BF16), shape((1024, 1024), BF16)),
        in_specs=[hbm] * 3 + [pl.BlockSpec(memory_space=vmem)] * 2 + [hbm] * 4,
        out_specs=[hbm] * 5,
        scratch_shapes=[
            vmem((tokens, 1024), BF16),
            vmem((tokens, 1024), BF16),
            vmem((tokens, 1024), BF16),
            vmem((1024, 1024), BF16),
            vmem((2 * BLK, 1024), BF16),
            vmem((2, HALF, 1024), BF16),
            vmem((2, HALF, 1024), BF16),
            vmem((2, HALF, 1024), BF16),
            vmem((768, 1024), BF16),
            vmem((2, 768, HALF), BF16),
            vmem((768, BLK), BF16),
            vmem((768, 1024), BF16),
            vmem((BLK, 1024), F32),
            vmem((768, tokens), BF16),
            vmem((8, tokens, 64), BF16),
            vmem((256, tokens), F32),
            vmem((16, tokens), F32),
            pltpu.SemaphoreType.DMA((16,)),
            pltpu.SemaphoreType.DMA((39,)),
            pltpu.SemaphoreType.DMA((39,)),
            pltpu.SemaphoreType.REGULAR,
        ],
        compiler_params=pltpu.CompilerParams(collective_id=0, has_side_effects=True, vmem_limit_bytes=67043328),
        cost_estimate=pl.CostEstimate(flops=80_000_000_000, bytes_accessed=40_000_000, transcendentals=40_000_000),
    )(h1, dy, x, g1, g2, wqkv, w1, w2, wo)


def copy_kernel(*refs):
    count = (len(refs) - 2) // 3
    srcs, dsts, bufs, in_sem, out_sem = refs[:count], refs[count:2 * count], refs[2 * count:3 * count], refs[-2], refs[-1]
    reads = [pltpu.make_async_copy(src, buf, in_sem.at[n]) for n, (src, buf) in enumerate(zip(srcs, bufs))]
    writes = [pltpu.make_async_copy(buf, dst, out_sem.at[n]) for n, (dst, buf) in enumerate(zip(dsts, bufs))]
    for copy in reads:
        copy.start()
    for read, write in zip(reads, writes):
        read.wait()
        write.start()
    for copy in writes:
        copy.wait()


def copy_out(*arrays):
    hbm = pl.BlockSpec(memory_space=pl.ANY)
    return pl.pallas_call(
        copy_kernel,
        name="copy_out",
        out_shape=[jax.ShapeDtypeStruct(a.shape, a.dtype) for a in arrays],
        in_specs=[hbm] * len(arrays),
        out_specs=[hbm] * len(arrays),
        scratch_shapes=[pltpu.VMEM(a.shape, a.dtype) for a in arrays] + [pltpu.SemaphoreType.DMA((len(arrays),))] * 2,
        compiler_params=pltpu.CompilerParams(vmem_limit_bytes=67043328),
    )(*arrays)


def solution(mesh):
    row_spec = P(('dp', 'tp'), None)
    in_specs = (row_spec, row_spec, row_spec, P(None), P(None), P(None, 'tp'), P('tp', None, None), P(None, 'tp'), P('tp', None))
    out_specs = (row_spec, P('dp', 'tp'), P(('dp', 'tp'), None, None), P('dp', 'tp'), P(('dp', 'tp'), None))

    def device_step(in_rows, mid_rows, gout_rows, ln1_gain, ln2_gain, wqkv_loc, wout_loc, wfc1_loc, wfc2_loc):
        grad_in, grad_wqkv, grad_wout, grad_wfc1, grad_wfc2 = copy_out(*layer_grads(mid_rows, gout_rows, in_rows, ln1_gain.reshape(1, 1024), ln2_gain.reshape(1, 1024), wqkv_loc, wfc1_loc, wfc2_loc, wout_loc.reshape(256, 1024)))
        return grad_in, grad_wqkv, grad_wout.reshape(4, 64, 1024), grad_wfc1, grad_wfc2

    return jax.shard_map(device_step, mesh=mesh, in_specs=in_specs, out_specs=out_specs, check_vma=False)
```

```python
import jax
import jax.numpy as jnp
from jax import lax
from jax.experimental import pallas as pl
from jax.experimental.pallas import tpu as pltpu
from jax.sharding import PartitionSpec as P

LN_EPS = 1e-5
GELU_COEF = 0.044715
GELU_SCALE = 0.7978845608028654
LOG2E = 1.4426950408889634
F32 = jnp.float32
BF16 = jnp.bfloat16
BLK = 512
HALF = 256


def ln_forward(rows):
    row_mean = jnp.mean(rows, axis=-1, keepdims=True)
    centered = rows - row_mean
    row_rstd = lax.rsqrt(jnp.mean(centered * centered, axis=-1, keepdims=True) + LN_EPS)
    return centered * row_rstd, row_rstd


def ln_backward(x_hat, row_rstd, ln_gain, grad_norm):
    grad_hat = grad_norm * ln_gain
    proj_one = jnp.mean(grad_hat, axis=-1, keepdims=True)
    proj_two = jnp.mean(grad_hat * x_hat, axis=-1, keepdims=True)
    return row_rstd * (grad_hat - proj_one - x_hat * proj_two)


def gelu_pair(pre_act):
    tanh_val = jnp.tanh(GELU_SCALE * (pre_act + GELU_COEF * pre_act * pre_act * pre_act))
    gelu_val = 0.5 * pre_act * (1.0 + tanh_val)
    gelu_der = 0.5 * (1.0 + tanh_val) + 0.5 * pre_act * (1.0 - tanh_val * tanh_val) * GELU_SCALE * (1.0 + 3.0 * GELU_COEF * pre_act * pre_act)
    return gelu_val, gelu_der


def nn(a, b):
    return lax.dot_general(a, b, (((1,), (0,)), ((), ())), preferred_element_type=F32)


def nt(a, b):
    return lax.dot_general(a, b, (((1,), (1,)), ((), ())), preferred_element_type=F32)


def qkv_block(i, n1, wqkvt, ct, nat):
    sl = pl.ds(pl.multiple_of(i * BLK, BLK), BLK)
    for n in range(4):
        c = nt(wqkvt[n * 192:(n + 1) * 192, :], n1[sl, :]).astype(BF16)
        q = c[0:64, :] * jnp.asarray(0.125, BF16)
        ct[n * 192:n * 192 + 64, sl] = q
        ct[n * 192 + 64:n * 192 + 192, sl] = c[64:192, :]
        nat[2 * n, sl, :] = c[64:128, :].T
        nat[2 * n + 1, sl, :] = c[128:192, :].T


def fwd_init(ot, stat):
    ot[...] = jnp.zeros_like(ot)
    stat[0:4, :] = jnp.full((4, stat.shape[1]), -1e30, F32)
    stat[4:16, :] = jnp.zeros((12, stat.shape[1]), F32)


def fwd_tile(ki, qi, diag, ct, nat, ot, stat):
    qs = pl.ds(pl.multiple_of(qi * BLK, BLK), BLK)
    ks = pl.ds(pl.multiple_of(ki * BLK, BLK), BLK)
    for h in range(4):
        s = nn(nat[2 * h, ks, :], ct[3 * h * 64:3 * h * 64 + 64, qs])
        if diag:
            key = lax.broadcasted_iota(jnp.int32, (BLK, BLK), 0)
            query = lax.broadcasted_iota(jnp.int32, (BLK, BLK), 1)
            s = jnp.where(key <= query, s, -1e30)
        m_old = stat[h:h + 1, qs]
        m_new = jnp.maximum(m_old, jnp.max(s, axis=0, keepdims=True))
        alpha = jnp.exp2((m_old - m_new) * LOG2E)
        e = jnp.exp2((s - m_new) * LOG2E)
        stat[h:h + 1, qs] = m_new
        stat[4 + h:5 + h, qs] = stat[4 + h:5 + h, qs] * alpha + jnp.sum(e, axis=0, keepdims=True)
        hs = slice(h * 64, (h + 1) * 64)
        vt = ct[(3 * h + 2) * 64:(3 * h + 3) * 64, ks]
        ot[hs, qs] = ot[hs, qs] * alpha + nn(vt, e.astype(BF16))


def fwd_finish(ot, stat):
    for h in range(4):
        inv = 1.0 / stat[4 + h:5 + h, :]
        stat[4 + h:5 + h, :] = inv
        ot[h * 64:(h + 1) * 64, :] = ot[h * 64:(h + 1) * 64, :] * inv


def do_block(i, e, wo, ot, dot_t, stat):
    sl = pl.ds(pl.multiple_of(i * HALF, HALF), HALF)
    d = nt(wo[...], e[sl, :]).astype(BF16)
    dot_t[:, sl] = d
    for h in range(4):
        part = d[h * 64:(h + 1) * 64, :]
        stat[8 + h:9 + h, sl] = jnp.sum(part.astype(F32) * ot[h * 64:(h + 1) * 64, sl], axis=0, keepdims=True)


def attn_bwd_tile(k0, ksize, q0, qsize, diag, ct, nat, dot_t, stat, dqt, dkt, dvt):
    ks = pl.ds(pl.multiple_of(k0, HALF), ksize)
    qs = pl.ds(pl.multiple_of(q0, HALF), qsize)
    for h in range(4):
        s = nn(nat[2 * h, ks, :], ct[3 * h * 64:3 * h * 64 + 64, qs])
        r = nn(nat[2 * h + 1, ks, :], dot_t[h * 64:(h + 1) * 64, qs])
        p = jnp.exp2((s - stat[h:h + 1, qs]) * LOG2E) * stat[4 + h:5 + h, qs]
        if diag:
            key = lax.broadcasted_iota(jnp.int32, (ksize, qsize), 0)
            query = lax.broadcasted_iota(jnp.int32, (ksize, qsize), 1)
            p = jnp.where(key <= query, p, 0.0)
        ds = (p * (r - stat[8 + h:9 + h, qs])).astype(BF16)
        hs = slice(h * 64, (h + 1) * 64)
        dvt[hs, ks] += nt(dot_t[hs, qs], p.astype(BF16))
        dkt[hs, ks] += nt(ct[3 * h * 64:3 * h * 64 + 64, qs], ds)
        dqt[hs, qs] += nn(ct[(3 * h + 1) * 64:(3 * h + 2) * 64, ks], ds)


def pack_dc(i, dqt, dkt, dvt, dct):
    sl = pl.ds(pl.multiple_of(i * BLK, BLK), BLK)
    for h in range(4):
        dct[3 * h * 64:3 * h * 64 + 64, sl] = (dqt[h * 64:(h + 1) * 64, sl] * 0.125).astype(BF16)
        dct[(3 * h + 1) * 64:(3 * h + 2) * 64, sl] = dkt[h * 64:(h + 1) * 64, sl].astype(BF16)
        dct[(3 * h + 2) * 64:(3 * h + 3) * 64, sl] = dvt[h * 64:(h + 1) * 64, sl].astype(BF16)


MESH_ID = pl.DeviceIdType.MESH


def place():
    me = lax.axis_index('tp')
    chip = me // 2
    core = me - chip * 2
    return me, chip, core, chip * 2 + (1 - core), (1 - chip) * 2 + core, (1 - chip) * 2 + (1 - core)


def entry_barrier(others):
    barrier = pltpu.get_barrier_semaphore()
    for other in others:
        pl.semaphore_signal(barrier, inc=1, device_id={'tp': other}, device_id_type=MESH_ID)
    pl.semaphore_wait(barrier, 3)


def send(src, dst, ssem, rsem, to):
    return pltpu.make_async_remote_copy(src_ref=src, dst_ref=dst, send_sem=ssem, recv_sem=rsem, device_id={'tp': to}, device_id_type=MESH_ID)


def rows(start, size):
    return pl.ds(pl.multiple_of(start, size), size)


def tn(a, b):
    return lax.dot_general(a, b, (((0,), (0,)), ((), ())), preferred_element_type=F32)


def ln_rows(src, gain, dst, start):
    @pl.loop(0, 4)
    def _(i):
        hat, _ = ln_forward(src[rows(i * 128, 128), :].astype(F32))
        dst[rows(start + i * 128, 128), :] = (hat * gain[...]).astype(BF16)


def mlp_rows(start, n2, dy, w1, w2t, act, da):
    sl = rows(start, HALF)
    for c in range(4):
        cs = slice(c * 256, (c + 1) * 256)
        gelu_val, gelu_der = gelu_pair(nn(n2[sl, :], w1[:, cs]))
        act[sl, cs] = gelu_val.astype(BF16)
        da[sl, cs] = (nn(dy[sl, :], w2t[:, cs]) * gelu_der).astype(BF16)


def layer_kernel(h1_hbm, dy_hbm, x_hbm, g1, g2, wqkv_hbm, w1_hbm, w2_hbm, wo_hbm,
                 dx_hbm, dwqkv_hbm, dwo_hbm, dw1_hbm, dw2_hbm,
                 n2, dy, n1, w1_pair, da_pair, d2_send, d2_recv, d1_recv, w_pair, dct_far, dct_own, wqkvt, dh1, ct, nat, ot, stat,
                 lsem, ssem, rsem, free_sem):
    me, chip, core, pair, peer, diag = place()
    own = rows(me * BLK, BLK)
    e = n2

    def chunk_copy(ref, block, n, first, to):
        sl = rows(block * BLK + n * HALF, HALF)
        return send(ref.at[sl, :], ref.at[sl, :], ssem.at[first + n], rsem.at[first + n], to)

    def d2_far(n):
        return send(d2_send.at[n], d2_recv.at[n], ssem.at[19 + n], rsem.at[19 + n], peer)

    def e_half(block, part_no):
        return e.at[rows(block * BLK + part_no * HALF, HALF), :]

    def e_pair(part_no):
        ref = e_half(me, part_no)
        return send(ref, ref, ssem.at[21 + part_no], rsem.at[21 + part_no], pair)

    def from_pair(part_no):
        ref = e_half(pair, part_no)
        return send(ref, ref, ssem.at[21 + part_no], rsem.at[21 + part_no], pair)

    def e_chunk(block, part_no, who):
        return e.at[rows(block * BLK + part_no * HALF + who * 128, 128), :]

    def e_peer(j):
        ref = e_chunk(chip * 2 + 1 - j // 2, j % 2, core)
        return send(ref, ref, ssem.at[23 + j], rsem.at[23 + j], peer)

    def from_peer(j):
        ref = e_chunk((1 - chip) * 2 + 1 - j // 2, j % 2, core)
        return send(ref, ref, ssem.at[23 + j], rsem.at[23 + j], peer)

    def relay(j, who):
        ref = e_chunk((1 - chip) * 2 + 1 - j // 2, j % 2, who)
        return send(ref, ref, ssem.at[33 + j], rsem.at[33 + j], pair)

    w_swap = send(wqkvt, w_pair, ssem.at[29], rsem.at[29], pair)

    def phase_one(w1, w2t, wqkv, act, da, h1, x, dw1, dw2):
        local = []
        for n, (src, dst) in enumerate(((dy_hbm, dy.at[own, :]), (h1_hbm, h1), (x_hbm, x), (w1_hbm, w1), (w2_hbm, dw2), (wqkv_hbm, wqkv))):
            copy = pltpu.make_async_copy(src, dst, lsem.at[n])
            local.append(copy)
        l_dy, l_h1, l_x, l_w1, l_w2, l_wqkv = local
        for copy in (l_dy, l_h1, l_x):
            copy.start()

        entry_barrier((pair, peer, diag))

        first_rows = rows(me * BLK, HALF)
        send(dy_hbm.at[0:HALF, :], dy.at[first_rows, :], ssem.at[6], rsem.at[6], peer).start()
        for copy in (l_w1, l_w2, l_wqkv):
            copy.start()
        to_pair = [send(ref.at[own, :], ref.at[own, :], ssem.at[n], rsem.at[n], pair) for n, ref in enumerate((n2, dy, n1))]
        to_pair.append(send(w1, w1_pair, ssem.at[3], rsem.at[3], pair))
        l_dy.wait()
        to_pair[1].start()
        l_h1.wait()
        ln_rows(h1, g2, n2, me * BLK)
        l_x.wait()
        ln_rows(x, g1, n1, me * BLK)
        chunk_copy(n2, me, 0, 4, peer).start()
        chunk_copy(dy, me, 1, 6, peer).start()
        chunk_copy(n2, me, 1, 4, peer).start()
        for n in range(2):
            chunk_copy(n1, me, n, 8, peer).start()
        to_pair[0].start()
        to_pair[2].start()
        l_w1.wait()
        to_pair[3].start()

        l_w2.wait()
        w2t[...] = dw2[...].T

        @pl.loop(0, 4)
        def _(i):
            @pl.when(i == 2)
            def _():
                to_pair[0].wait_recv()
                to_pair[1].wait_recv()

            second = i // 2
            mlp_rows((me + second * (pair - me)) * BLK + (i - 2 * second) * HALF, n2, dy, w1, w2t, act, da)

        da_swap = send(da.at[rows(pair * BLK, BLK), :], da_pair.at[0:BLK, :], ssem.at[16], rsem.at[16], pair)
        da_swap.start()
        l_wqkv.wait()
        wqkvt[...] = wqkv[...].T
        fwd_init(ot, stat)
        to_pair[2].wait_recv()

        @pl.loop(0, 2)
        def _(n):
            qkv_block(chip * 2 + n, n1, wqkvt, ct, nat)

        w_swap.start()

        def da_far(n):
            return send(da.at[rows(diag * BLK + n * HALF, HALF), :], da_pair.at[rows(BLK + n * HALF, HALF), :], ssem.at[17 + n], rsem.at[17 + n], pair)

        to_pair[3].wait_recv()

        @pl.loop(0, 2)
        def _(n):
            chunk_copy(dy, peer, n, 6, peer).wait_recv()
            chunk_copy(dy, peer, n, 12, pair).start()
            chunk_copy(n2, peer, n, 4, peer).wait_recv()
            chunk_copy(n2, peer, n, 10, pair).start()

            @pl.loop(0, 2)
            def _(j):
                @pl.when(j == 1)
                def _():
                    chunk_copy(n2, diag, n, 10, pair).wait_recv()
                    chunk_copy(dy, diag, n, 12, pair).wait_recv()

                mlp_rows((peer + j * (diag - peer)) * BLK + n * HALF, n2, dy, w1, w2t, act, da)

            da_far(n).start()
            first = nt(da[rows(peer * BLK + n * HALF, HALF), :], w1[...])
            da_far(n).wait_recv()
            d2_send[n] = (first + nt(da_pair[rows(BLK + n * HALF, HALF), :], w1_pair[...])).astype(BF16)
            d2_far(n).start()

        da_swap.wait_recv()

        @pl.loop(0, 2)
        def _(i):
            sl = rows(i * HALF, HALF)
            dh1[sl, :] = nt(da[rows(me * BLK + i * HALF, HALF), :], w1[...]) + nt(da_pair[sl, :], w1_pair[...])

        outs = [pltpu.make_async_copy(src, dst, lsem.at[6 + n]) for n, (src, dst) in enumerate(((dw1, dw1_hbm), (dw2, dw2_hbm)))]

        @pl.loop(0, 6)
        def _(i):
            @pl.when(i == 2)
            def _():
                @pl.loop(0, 4)
                def _(j):
                    sl = rows(j * 256, 256)
                    dw2[sl, :] = tn(act[:, sl], dy[...]).astype(BF16)
                    dw1[sl, :] = tn(n2[:, sl], da[...]).astype(BF16)

                for copy in outs:
                    copy.start()
                to_pair[0].wait_send()
                for n in range(2):
                    chunk_copy(n2, me, n, 4, peer).wait_send()
                    chunk_copy(n2, peer, n, 10, pair).wait_send()
                for other in (pair, peer):
                    pl.semaphore_signal(free_sem, inc=1, device_id={'tp': other}, device_id_type=MESH_ID)
                for n in range(2):
                    chunk_copy(n1, peer, n, 8, peer).wait_recv()
                    chunk_copy(n1, peer, n, 14, pair).start()

                @pl.loop(0, 2)
                def _(j):
                    @pl.when(j == 1)
                    def _():
                        for n in range(2):
                            chunk_copy(n1, diag, n, 14, pair).wait_recv()

                    qkv_block(peer + j * (diag - peer), n1, wqkvt, ct, nat)

            group = i // 2
            far = group % 2
            qi = far * 2 + chip * 2 - 4 * far * chip + i - 2 * group
            low = (1 - far) * (1 - group // 2) * chip * 2
            high = qi + (group // 2) * (chip * 2 - qi)

            @pl.loop(low, high)
            def _(ki):
                fwd_tile(ki, qi, False, ct, nat, ot, stat)

            @pl.when(group < 2)
            def _():
                fwd_tile(qi, qi, True, ct, nat, ot, stat)

        fwd_finish(ot, stat)
        for copy in outs:
            copy.wait()
        for copy in to_pair[1:] + [da_swap]:
            copy.wait_send()
        for n in range(2):
            for ref, block, first, to in ((dy, me, 6, peer), (n1, me, 8, peer), (dy, peer, 12, pair), (n1, peer, 14, pair)):
                chunk_copy(ref, block, n, first, to).wait_send()
            da_far(n).wait_send()
        pl.semaphore_wait(free_sem, 2)

        @pl.loop(0, 2)
        def _(n):
            d2_far(n).wait_recv()
            sl = rows(n * HALF, HALF)
            hat, rstd = ln_forward(h1[sl, :].astype(F32))
            rows_n = rows(me * BLK + n * HALF, HALF)
            grad = dy[rows_n, :].astype(F32) + ln_backward(hat, rstd, g2[...], dh1[sl, :] + d2_recv[n].astype(F32))
            dh1[sl, :] = grad
            e[rows_n, :] = grad.astype(BF16)
            e_pair(n).start()

            @pl.when(n * core == 1)
            def _():
                e_peer(1).start()

            from_pair(n).wait_recv()

            @pl.when(n == 0)
            def _():
                e_peer(0).start()

            @pl.when(n * (1 - core) == 1)
            def _():
                e_peer(1).start()

            @pl.when(n == 1)
            def _():
                e_peer(2).start()
                e_peer(3).start()

    pl.run_scoped(
        phase_one,
        w1=pltpu.VMEM((1024, 1024), BF16),
        w2t=pltpu.VMEM((1024, 1024), BF16),
        wqkv=pltpu.VMEM((1024, 768), BF16),
        act=pltpu.VMEM((4 * BLK, 1024), BF16),
        da=pltpu.VMEM((4 * BLK, 1024), BF16),
        h1=pltpu.VMEM((BLK, 1024), BF16),
        x=pltpu.VMEM((BLK, 1024), BF16),
        dw1=pltpu.VMEM((1024, 1024), BF16),
        dw2=pltpu.VMEM((1024, 1024), BF16),
    )

    def phase_two(dot_t, dqt, dkt, dvt, wo, part, x, dx, dwqkv, dwo, dct):
        l_wo = pltpu.make_async_copy(wo_hbm, wo, lsem.at[8])
        l_wo.start()
        l_x = pltpu.make_async_copy(x_hbm, x, lsem.at[9])
        l_x.start()
        dkt[...] = jnp.zeros_like(dkt)
        dvt[...] = jnp.zeros_like(dvt)
        dqt[...] = jnp.zeros_like(dqt)
        for n in range(2):
            d2_far(n).wait_send()
        l_wo.wait()

        @pl.loop(0, 4)
        def _(n):
            do_block(chip * 4 + n, e, wo, ot, dot_t, stat)

        w_swap.wait_recv()

        def swap_far(n, mine_or_theirs):
            block = (1 - chip) * 2 + 1 - n
            return send(dct.at[:, rows(block * BLK + mine_or_theirs * HALF, HALF)], dct_far.at[n], ssem.at[27 + n], rsem.at[27 + n], pair)

        def d1_far(n, piece):
            sl = rows(piece * 128, 128)
            return send(d2_send.at[n, sl, :], d1_recv.at[core, sl, :], ssem.at[30 + n + 7 * piece], rsem.at[30 + core + 7 * piece], (1 - chip) * 2 + 1 - n)

        def take_far(n):
            for half in range(2):
                from_peer(2 * n + half).wait_recv()
                relay(2 * n + half, core).start()

        def far_do(n):
            for half in range(2):
                relay(2 * n + half, 1 - core).wait_recv()

            @pl.loop(0, 2)
            def _(half):
                do_block(((1 - chip) * 2 + 1 - n) * 2 + half, e, wo, ot, dot_t, stat)

        @pl.loop(0, 6)
        def _(i):
            group = i // 2
            far = group % 2
            n = i - 2 * group
            qi = (1 - far) * (chip * 2 + n) + far * ((1 - chip) * 2 + 1 - n)
            low = (group // 2) * chip * 2
            high = far * qi + (1 - far) * ((1 - group // 2) * ((1 - chip) * qi + chip * 2) + (group // 2) * chip * qi)

            @pl.when(i == 2)
            def _():
                take_far(0)
                far_do(0)

            @pl.loop(low, high)
            def _(ki):
                attn_bwd_tile(ki * BLK, BLK, qi * BLK, BLK, False, ct, nat, dot_t, stat, dqt, dkt, dvt)

            @pl.when(far + (1 - far) * ((1 - group // 2) * (1 - chip) + (group // 2) * chip) == 1)
            def _():
                attn_bwd_tile(qi * BLK, HALF, qi * BLK, BLK, True, ct, nat, dot_t, stat, dqt, dkt, dvt)
                attn_bwd_tile(qi * BLK + HALF, HALF, qi * BLK + HALF, HALF, True, ct, nat, dot_t, stat, dqt, dkt, dvt)

            @pl.when(far == 1)
            def _():
                pack_dc(qi, dqt, dkt, dvt, dct)
                swap_far(n, 1 - core).start()
                part[0:HALF, :] = nn(dct[:, rows(qi * BLK + core * HALF, HALF)].T, wqkvt[...])

                swap_far(n, core).wait_recv()

                @pl.loop(0, 2)
                def _(piece):
                    sl = rows(piece * 128, 128)
                    d2_send[n, sl, :] = (part[sl, :] + nn(dct_far[n, :, sl].T, w_pair[...])).astype(BF16)
                    d1_far(n, piece).start()

                @pl.when(n == 0)
                def _():
                    take_far(1)
                    far_do(1)

        @pl.loop(0, 2)
        def _(n):
            pack_dc(chip * 2 + n, dqt, dkt, dvt, dct)

        swap = send(dct.at[:, rows(pair * BLK, BLK)], dct_own, ssem.at[32], rsem.at[32], pair)
        swap.start()
        part[...] = nn(dct[:, own].T, wqkvt[...])
        swap.wait_recv()
        part[...] += nn(dct_own[...].T, w_pair[...])

        @pl.loop(0, 4)
        def _(i):
            sl = rows(i * 256, 256)
            dwo[:, sl] = nn(ot[...].astype(BF16), e[:, sl]).astype(BF16)
            dwqkv[sl, :] = nn(dct[...], n1[:, sl]).astype(BF16).T

        outs = [pltpu.make_async_copy(src, dst, lsem.at[10 + n]) for n, (src, dst) in enumerate(((dwqkv, dwqkv_hbm), (dwo, dwo_hbm)))]
        outs[0].start()
        outs[1].start()
        l_x.wait()

        def dx_out(k):
            sl = rows(k * 128, 128)
            return pltpu.make_async_copy(dx.at[sl, :], dx_hbm.at[sl, :], lsem.at[12 + k])

        @pl.loop(0, 4)
        def _(i):
            piece = i // 2
            n = i - 2 * piece
            arrived = rows(piece * 128, 128)
            send(d2_send.at[n, arrived, :], d1_recv.at[n, arrived, :], ssem.at[30 + n + 7 * piece], rsem.at[30 + n + 7 * piece], peer).wait_recv()
            sl = rows(n * HALF + piece * 128, 128)
            hat, rstd = ln_forward(x[sl, :].astype(F32))
            grad = part[sl, :] + d1_recv[n, arrived, :].astype(F32)
            dx[sl, :] = (dh1[sl, :] + ln_backward(hat, rstd, g1[...], grad)).astype(BF16)
            dx_out(n * 2 + piece).start()

        for j in range(4):
            e_peer(j).wait_send()
            relay(j, core).wait_send()
        for n in range(2):
            e_pair(n).wait_send()
            swap_far(n, 1 - core).wait_send()
            for piece in range(2):
                d1_far(n, piece).wait_send()
        w_swap.wait_send()
        swap.wait_send()
        for copy in outs + [dx_out(k) for k in range(4)]:
            copy.wait()

    tokens = 4 * BLK
    pl.run_scoped(
        phase_two,
        dot_t=pltpu.VMEM((256, tokens), BF16),
        dqt=pltpu.VMEM((256, tokens), F32),
        dkt=pltpu.VMEM((256, tokens), F32),
        dvt=pltpu.VMEM((256, tokens), F32),
        wo=pltpu.VMEM((256, 1024), BF16),
        part=pltpu.VMEM((BLK, 1024), F32),
        x=pltpu.VMEM((BLK, 1024), BF16),
        dx=pltpu.VMEM((BLK, 1024), BF16),
        dwqkv=pltpu.VMEM((1024, 768), BF16),
        dwo=pltpu.VMEM((256, 1024), BF16),
        dct=pltpu.VMEM((768, tokens), BF16),
    )


def layer_grads(h1, dy, x, g1, g2, wqkv, w1, w2, wo):
    tokens = 4 * BLK
    vmem = pltpu.VMEM
    shape = jax.ShapeDtypeStruct
    hbm = pl.BlockSpec(memory_space=pl.ANY)
    return pl.pallas_call(
        layer_kernel,
        name="layer_grads",
        out_shape=(shape((BLK, 1024), BF16), shape((1024, 768), BF16), shape((256, 1024), BF16), shape((1024, 1024), BF16), shape((1024, 1024), BF16)),
        in_specs=[hbm] * 3 + [pl.BlockSpec(memory_space=vmem)] * 2 + [hbm] * 4,
        out_specs=[hbm] * 5,
        scratch_shapes=[
            vmem((tokens, 1024), BF16),
            vmem((tokens, 1024), BF16),
            vmem((tokens, 1024), BF16),
            vmem((1024, 1024), BF16),
            vmem((2 * BLK, 1024), BF16),
            vmem((2, HALF, 1024), BF16),
            vmem((2, HALF, 1024), BF16),
            vmem((2, HALF, 1024), BF16),
            vmem((768, 1024), BF16),
            vmem((2, 768, HALF), BF16),
            vmem((768, BLK), BF16),
            vmem((768, 1024), BF16),
            vmem((BLK, 1024), F32),
            vmem((768, tokens), BF16),
            vmem((8, tokens, 64), BF16),
            vmem((256, tokens), F32),
            vmem((16, tokens), F32),
            pltpu.SemaphoreType.DMA((16,)),
            pltpu.SemaphoreType.DMA((39,)),
            pltpu.SemaphoreType.DMA((39,)),
            pltpu.SemaphoreType.REGULAR,
        ],
        compiler_params=pltpu.CompilerParams(collective_id=0, has_side_effects=True, vmem_limit_bytes=67043328),
        cost_estimate=pl.CostEstimate(flops=80_000_000_000, bytes_accessed=40_000_000, transcendentals=40_000_000),
    )(h1, dy, x, g1, g2, wqkv, w1, w2, wo)


def copy_kernel(*refs):
    count = (len(refs) - 2) // 3
    srcs, dsts, bufs, in_sem, out_sem = refs[:count], refs[count:2 * count], refs[2 * count:3 * count], refs[-2], refs[-1]
    reads = [pltpu.make_async_copy(src, buf, in_sem.at[n]) for n, (src, buf) in enumerate(zip(srcs, bufs))]
    writes = [pltpu.make_async_copy(buf, dst, out_sem.at[n]) for n, (dst, buf) in enumerate(zip(dsts, bufs))]
    for copy in reads:
        copy.start()
    for read, write in zip(reads, writes):
        read.wait()
        write.start()
    for copy in writes:
        copy.wait()


def copy_out(*arrays):
    hbm = pl.BlockSpec(memory_space=pl.ANY)
    return pl.pallas_call(
        copy_kernel,
        name="copy_out",
        out_shape=[jax.ShapeDtypeStruct(a.shape, a.dtype) for a in arrays],
        in_specs=[hbm] * len(arrays),
        out_specs=[hbm] * len(arrays),
        scratch_shapes=[pltpu.VMEM(a.shape, a.dtype) for a in arrays] + [pltpu.SemaphoreType.DMA((len(arrays),))] * 2,
        compiler_params=pltpu.CompilerParams(vmem_limit_bytes=67043328),
    )(*arrays)


def solution(mesh):
    row_spec = P(('dp', 'tp'), None)
    in_specs = (row_spec, row_spec, row_spec, P(None), P(None), P(None, 'tp'), P('tp', None, None), P(None, 'tp'), P('tp', None))
    out_specs = (row_spec, P('dp', 'tp'), P(('dp', 'tp'), None, None), P('dp', 'tp'), P(('dp', 'tp'), None))

    def device_step(in_rows, mid_rows, gout_rows, ln1_gain, ln2_gain, wqkv_loc, wout_loc, wfc1_loc, wfc2_loc):
        grad_in, grad_wqkv, grad_wout, grad_wfc1, grad_wfc2 = copy_out(*layer_grads(mid_rows, gout_rows, in_rows, ln1_gain.reshape(1, 1024), ln2_gain.reshape(1, 1024), wqkv_loc, wfc1_loc, wfc2_loc, wout_loc.reshape(256, 1024)))
        return grad_in, grad_wqkv, grad_wout.reshape(4, 64, 1024), grad_wfc1, grad_wfc2

    return jax.shard_map(device_step, mesh=mesh, in_specs=in_specs, out_specs=out_specs, check_vma=False)
```

```python
import jax
import jax.numpy as jnp
from jax import lax
from jax.experimental import pallas as pl
from jax.experimental.pallas import tpu as pltpu
from jax.sharding import PartitionSpec as P

LN_EPS = 1e-5
GELU_COEF = 0.044715
GELU_SCALE = 0.7978845608028654
LOG2E = 1.4426950408889634
F32 = jnp.float32
BF16 = jnp.bfloat16
BLK = 512
HALF = 256


def ln_forward(rows):
    row_mean = jnp.mean(rows, axis=-1, keepdims=True)
    centered = rows - row_mean
    row_rstd = lax.rsqrt(jnp.mean(centered * centered, axis=-1, keepdims=True) + LN_EPS)
    return centered * row_rstd, row_rstd


def ln_backward(x_hat, row_rstd, ln_gain, grad_norm):
    grad_hat = grad_norm * ln_gain
    proj_one = jnp.mean(grad_hat, axis=-1, keepdims=True)
    proj_two = jnp.mean(grad_hat * x_hat, axis=-1, keepdims=True)
    return row_rstd * (grad_hat - proj_one - x_hat * proj_two)


def gelu_pair(pre_act):
    tanh_val = jnp.tanh(GELU_SCALE * (pre_act + GELU_COEF * pre_act * pre_act * pre_act))
    gelu_val = 0.5 * pre_act * (1.0 + tanh_val)
    gelu_der = 0.5 * (1.0 + tanh_val) + 0.5 * pre_act * (1.0 - tanh_val * tanh_val) * GELU_SCALE * (1.0 + 3.0 * GELU_COEF * pre_act * pre_act)
    return gelu_val, gelu_der


def nn(a, b):
    return lax.dot_general(a, b, (((1,), (0,)), ((), ())), preferred_element_type=F32)


def nt(a, b):
    return lax.dot_general(a, b, (((1,), (1,)), ((), ())), preferred_element_type=F32)


def qkv_block(i, n1, wqkvt, ct, nat):
    sl = pl.ds(pl.multiple_of(i * BLK, BLK), BLK)
    for n in range(4):
        c = nt(wqkvt[n * 192:(n + 1) * 192, :], n1[sl, :]).astype(BF16)
        q = c[0:64, :] * jnp.asarray(0.125, BF16)
        ct[n * 192:n * 192 + 64, sl] = q
        ct[n * 192 + 64:n * 192 + 192, sl] = c[64:192, :]
        nat[2 * n, sl, :] = c[64:128, :].T
        nat[2 * n + 1, sl, :] = c[128:192, :].T


def fwd_init(ot, stat):
    ot[...] = jnp.zeros_like(ot)
    stat[0:4, :] = jnp.full((4, stat.shape[1]), -1e30, F32)
    stat[4:16, :] = jnp.zeros((12, stat.shape[1]), F32)


def fwd_tile(ki, qi, diag, ct, nat, ot, stat):
    qs = pl.ds(pl.multiple_of(qi * BLK, BLK), BLK)
    ks = pl.ds(pl.multiple_of(ki * BLK, BLK), BLK)
    for h in range(4):
        s = nn(nat[2 * h, ks, :], ct[3 * h * 64:3 * h * 64 + 64, qs])
        if diag:
            key = lax.broadcasted_iota(jnp.int32, (BLK, BLK), 0)
            query = lax.broadcasted_iota(jnp.int32, (BLK, BLK), 1)
            s = jnp.where(key <= query, s, -1e30)
        m_old = stat[h:h + 1, qs]
        m_new = jnp.maximum(m_old, jnp.max(s, axis=0, keepdims=True))
        alpha = jnp.exp2((m_old - m_new) * LOG2E)
        e = jnp.exp2((s - m_new) * LOG2E)
        stat[h:h + 1, qs] = m_new
        stat[4 + h:5 + h, qs] = stat[4 + h:5 + h, qs] * alpha + jnp.sum(e, axis=0, keepdims=True)
        hs = slice(h * 64, (h + 1) * 64)
        vt = ct[(3 * h + 2) * 64:(3 * h + 3) * 64, ks]
        ot[hs, qs] = ot[hs, qs] * alpha + nn(vt, e.astype(BF16))


def fwd_finish(ot, stat):
    for h in range(4):
        inv = 1.0 / stat[4 + h:5 + h, :]
        stat[4 + h:5 + h, :] = inv
        ot[h * 64:(h + 1) * 64, :] = ot[h * 64:(h + 1) * 64, :] * inv


def do_block(i, e, wo, ot, dot_t, stat):
    sl = pl.ds(pl.multiple_of(i * HALF, HALF), HALF)
    d = nt(wo[...], e[sl, :]).astype(BF16)
    dot_t[:, sl] = d
    for h in range(4):
        part = d[h * 64:(h + 1) * 64, :]
        stat[8 + h:9 + h, sl] = jnp.sum(part.astype(F32) * ot[h * 64:(h + 1) * 64, sl], axis=0, keepdims=True)


def attn_bwd_tile(k0, ksize, q0, qsize, diag, ct, nat, dot_t, stat, dqt, dkt, dvt):
    ks = pl.ds(pl.multiple_of(k0, HALF), ksize)
    qs = pl.ds(pl.multiple_of(q0, HALF), qsize)
    for h in range(4):
        s = nn(nat[2 * h, ks, :], ct[3 * h * 64:3 * h * 64 + 64, qs])
        r = nn(nat[2 * h + 1, ks, :], dot_t[h * 64:(h + 1) * 64, qs])
        p = jnp.exp2((s - stat[h:h + 1, qs]) * LOG2E) * stat[4 + h:5 + h, qs]
        if diag:
            key = lax.broadcasted_iota(jnp.int32, (ksize, qsize), 0)
            query = lax.broadcasted_iota(jnp.int32, (ksize, qsize), 1)
            p = jnp.where(key <= query, p, 0.0)
        ds = (p * (r - stat[8 + h:9 + h, qs])).astype(BF16)
        hs = slice(h * 64, (h + 1) * 64)
        dvt[hs, ks] += nt(dot_t[hs, qs], p.astype(BF16))
        dkt[hs, ks] += nt(ct[3 * h * 64:3 * h * 64 + 64, qs], ds)
        dqt[hs, qs] += nn(ct[(3 * h + 1) * 64:(3 * h + 2) * 64, ks], ds)


def pack_dc(i, dqt, dkt, dvt, dct):
    sl = pl.ds(pl.multiple_of(i * BLK, BLK), BLK)
    for h in range(4):
        dct[3 * h * 64:3 * h * 64 + 64, sl] = (dqt[h * 64:(h + 1) * 64, sl] * 0.125).astype(BF16)
        dct[(3 * h + 1) * 64:(3 * h + 2) * 64, sl] = dkt[h * 64:(h + 1) * 64, sl].astype(BF16)
        dct[(3 * h + 2) * 64:(3 * h + 3) * 64, sl] = dvt[h * 64:(h + 1) * 64, sl].astype(BF16)


MESH_ID = pl.DeviceIdType.MESH


def place():
    me = lax.axis_index('tp')
    chip = me // 2
    core = me - chip * 2
    return me, chip, core, chip * 2 + (1 - core), (1 - chip) * 2 + core, (1 - chip) * 2 + (1 - core)


def entry_barrier(others):
    barrier = pltpu.get_barrier_semaphore()
    for other in others:
        pl.semaphore_signal(barrier, inc=1, device_id={'tp': other}, device_id_type=MESH_ID)
    pl.semaphore_wait(barrier, 3)


def send(src, dst, ssem, rsem, to):
    return pltpu.make_async_remote_copy(src_ref=src, dst_ref=dst, send_sem=ssem, recv_sem=rsem, device_id={'tp': to}, device_id_type=MESH_ID)


def rows(start, size):
    return pl.ds(pl.multiple_of(start, size), size)


def tn(a, b):
    return lax.dot_general(a, b, (((0,), (0,)), ((), ())), preferred_element_type=F32)


def ln_rows(src, gain, dst, start):
    @pl.loop(0, 4)
    def _(i):
        hat, _ = ln_forward(src[rows(i * 128, 128), :].astype(F32))
        dst[rows(start + i * 128, 128), :] = (hat * gain[...]).astype(BF16)


def mlp_rows(start, n2, dy, w1, w2t, act, da):
    sl = rows(start, HALF)
    for c in range(4):
        cs = slice(c * 256, (c + 1) * 256)
        gelu_val, gelu_der = gelu_pair(nn(n2[sl, :], w1[:, cs]))
        act[sl, cs] = gelu_val.astype(BF16)
        da[sl, cs] = (nn(dy[sl, :], w2t[:, cs]) * gelu_der).astype(BF16)


def layer_kernel(h1_hbm, dy_hbm, x_hbm, g1, g2, wqkv_hbm, w1_hbm, w2_hbm, wo_hbm,
                 dx_hbm, dwqkv_hbm, dwo_hbm, dw1_hbm, dw2_hbm,
                 n2, dy, n1, w1_pair, da_pair, d2_send, d2_recv, d1_recv, w_pair, dct_far, dct_own, wqkvt, dh1, ct, nat, ot, stat,
                 lsem, ssem, rsem, free_sem):
    me, chip, core, pair, peer, diag = place()
    own = rows(me * BLK, BLK)
    e = n2

    def chunk_copy(ref, block, n, first, to):
        sl = rows(block * BLK + n * HALF, HALF)
        return send(ref.at[sl, :], ref.at[sl, :], ssem.at[first + n], rsem.at[first + n], to)

    def d2_far(n):
        return send(d2_send.at[n], d2_recv.at[n], ssem.at[19 + n], rsem.at[19 + n], peer)

    def e_half(block, part_no):
        return e.at[rows(block * BLK + part_no * HALF, HALF), :]

    def e_pair(part_no):
        ref = e_half(me, part_no)
        return send(ref, ref, ssem.at[21 + part_no], rsem.at[21 + part_no], pair)

    def from_pair(part_no):
        ref = e_half(pair, part_no)
        return send(ref, ref, ssem.at[21 + part_no], rsem.at[21 + part_no], pair)

    def e_chunk(block, part_no, who):
        return e.at[rows(block * BLK + part_no * HALF + who * 128, 128), :]

    def e_peer(j):
        ref = e_chunk(chip * 2 + 1 - j // 2, j % 2, core)
        return send(ref, ref, ssem.at[23 + j], rsem.at[23 + j], peer)

    def from_peer(j):
        ref = e_chunk((1 - chip) * 2 + 1 - j // 2, j % 2, core)
        return send(ref, ref, ssem.at[23 + j], rsem.at[23 + j], peer)

    def relay(j, who):
        ref = e_chunk((1 - chip) * 2 + 1 - j // 2, j % 2, who)
        return send(ref, ref, ssem.at[33 + j], rsem.at[33 + j], pair)

    w_swap = send(wqkvt, w_pair, ssem.at[29], rsem.at[29], pair)

    def phase_one(w1, w2t, wqkv, act, da, h1, x, dw1, dw2):
        local = []
        for n, (src, dst) in enumerate(((dy_hbm, dy.at[own, :]), (h1_hbm, h1), (x_hbm, x), (w1_hbm, w1), (w2_hbm, dw2), (wqkv_hbm, wqkv))):
            copy = pltpu.make_async_copy(src, dst, lsem.at[n])
            local.append(copy)
        l_dy, l_h1, l_x, l_w1, l_w2, l_wqkv = local
        for copy in (l_dy, l_h1, l_x):
            copy.start()

        entry_barrier((pair, peer, diag))

        first_rows = rows(me * BLK, HALF)
        send(dy_hbm.at[0:HALF, :], dy.at[first_rows, :], ssem.at[6], rsem.at[6], peer).start()
        for copy in (l_w1, l_w2, l_wqkv):
            copy.start()
        to_pair = [send(ref.at[own, :], ref.at[own, :], ssem.at[n], rsem.at[n], pair) for n, ref in enumerate((n2, dy, n1))]
        to_pair.append(send(w1, w1_pair, ssem.at[3], rsem.at[3], pair))
        l_dy.wait()
        to_pair[1].start()
        l_h1.wait()
        ln_rows(h1, g2, n2, me * BLK)
        l_x.wait()
        ln_rows(x, g1, n1, me * BLK)
        chunk_copy(n2, me, 0, 4, peer).start()
        chunk_copy(dy, me, 1, 6, peer).start()
        chunk_copy(n2, me, 1, 4, peer).start()
        for n in range(2):
            chunk_copy(n1, me, n, 8, peer).start()
        to_pair[0].start()
        to_pair[2].start()
        l_w1.wait()
        to_pair[3].start()

        l_w2.wait()
        w2t[...] = dw2[...].T

        @pl.loop(0, 4)
        def _(i):
            @pl.when(i == 2)
            def _():
                to_pair[0].wait_recv()
                to_pair[1].wait_recv()

            second = i // 2
            mlp_rows((me + second * (pair - me)) * BLK + (i - 2 * second) * HALF, n2, dy, w1, w2t, act, da)

        da_swap = send(da.at[rows(pair * BLK, BLK), :], da_pair.at[0:BLK, :], ssem.at[16], rsem.at[16], pair)
        da_swap.start()
        l_wqkv.wait()
        wqkvt[...] = wqkv[...].T
        fwd_init(ot, stat)
        to_pair[2].wait_recv()

        @pl.loop(0, 2)
        def _(n):
            qkv_block(chip * 2 + n, n1, wqkvt, ct, nat)

        w_swap.start()

        def da_far(n):
            return send(da.at[rows(diag * BLK + n * HALF, HALF), :], da_pair.at[rows(BLK + n * HALF, HALF), :], ssem.at[17 + n], rsem.at[17 + n], pair)

        to_pair[3].wait_recv()

        @pl.loop(0, 2)
        def _(n):
            chunk_copy(dy, peer, n, 6, peer).wait_recv()
            chunk_copy(dy, peer, n, 12, pair).start()
            chunk_copy(n2, peer, n, 4, peer).wait_recv()
            chunk_copy(n2, peer, n, 10, pair).start()

            @pl.loop(0, 2)
            def _(j):
                @pl.when(j == 1)
                def _():
                    chunk_copy(n2, diag, n, 10, pair).wait_recv()
                    chunk_copy(dy, diag, n, 12, pair).wait_recv()

                mlp_rows((peer + j * (diag - peer)) * BLK + n * HALF, n2, dy, w1, w2t, act, da)

            da_far(n).start()
            first = nt(da[rows(peer * BLK + n * HALF, HALF), :], w1[...])
            da_far(n).wait_recv()
            d2_send[n] = (first + nt(da_pair[rows(BLK + n * HALF, HALF), :], w1_pair[...])).astype(BF16)
            d2_far(n).start()

        da_swap.wait_recv()

        @pl.loop(0, 2)
        def _(i):
            sl = rows(i * HALF, HALF)
            dh1[sl, :] = nt(da[rows(me * BLK + i * HALF, HALF), :], w1[...]) + nt(da_pair[sl, :], w1_pair[...])

        outs = [pltpu.make_async_copy(src, dst, lsem.at[6 + n]) for n, (src, dst) in enumerate(((dw1, dw1_hbm), (dw2, dw2_hbm)))]

        def mid_grad(n):
            d2_far(n).wait_recv()
            sl = rows(n * HALF, HALF)
            hat, rstd = ln_forward(h1[sl, :].astype(F32))
            rows_n = rows(me * BLK + n * HALF, HALF)
            grad = dy[rows_n, :].astype(F32) + ln_backward(hat, rstd, g2[...], dh1[sl, :] + d2_recv[n].astype(F32))
            dh1[sl, :] = grad
            e[rows_n, :] = grad.astype(BF16)
            e_pair(n).start()
            if n == 0:
                from_pair(0).wait_recv()
                e_peer(0).start()
            else:
                @pl.when(core == 1)
                def _():
                    e_peer(1).start()

                from_pair(1).wait_recv()

                @pl.when(core == 0)
                def _():
                    e_peer(1).start()

                e_peer(2).start()
                e_peer(3).start()

        @pl.loop(0, 6)
        def _(i):
            @pl.when(i == 4)
            def _():
                pl.semaphore_wait(free_sem, 2)
                mid_grad(0)

            @pl.when(i == 2)
            def _():
                @pl.loop(0, 4)
                def _(j):
                    sl = rows(j * 256, 256)
                    dw2[sl, :] = tn(act[:, sl], dy[...]).astype(BF16)
                    dw1[sl, :] = tn(n2[:, sl], da[...]).astype(BF16)

                for copy in outs:
                    copy.start()
                to_pair[0].wait_send()
                for n in range(2):
                    chunk_copy(n2, me, n, 4, peer).wait_send()
                    chunk_copy(n2, peer, n, 10, pair).wait_send()
                for other in (pair, peer):
                    pl.semaphore_signal(free_sem, inc=1, device_id={'tp': other}, device_id_type=MESH_ID)
                for n in range(2):
                    chunk_copy(n1, peer, n, 8, peer).wait_recv()
                    chunk_copy(n1, peer, n, 14, pair).start()

                @pl.loop(0, 2)
                def _(j):
                    @pl.when(j == 1)
                    def _():
                        for n in range(2):
                            chunk_copy(n1, diag, n, 14, pair).wait_recv()

                    qkv_block(peer + j * (diag - peer), n1, wqkvt, ct, nat)

            group = i // 2
            far = group % 2
            qi = far * 2 + chip * 2 - 4 * far * chip + i - 2 * group
            low = (1 - far) * (1 - group // 2) * chip * 2
            high = qi + (group // 2) * (chip * 2 - qi)

            @pl.loop(low, high)
            def _(ki):
                fwd_tile(ki, qi, False, ct, nat, ot, stat)

            @pl.when(group < 2)
            def _():
                fwd_tile(qi, qi, True, ct, nat, ot, stat)

        fwd_finish(ot, stat)
        for copy in outs:
            copy.wait()
        for copy in to_pair[1:] + [da_swap]:
            copy.wait_send()
        for n in range(2):
            for ref, block, first, to in ((dy, me, 6, peer), (n1, me, 8, peer), (dy, peer, 12, pair), (n1, peer, 14, pair)):
                chunk_copy(ref, block, n, first, to).wait_send()
            da_far(n).wait_send()
        mid_grad(1)

    pl.run_scoped(
        phase_one,
        w1=pltpu.VMEM((1024, 1024), BF16),
        w2t=pltpu.VMEM((1024, 1024), BF16),
        wqkv=pltpu.VMEM((1024, 768), BF16),
        act=pltpu.VMEM((4 * BLK, 1024), BF16),
        da=pltpu.VMEM((4 * BLK, 1024), BF16),
        h1=pltpu.VMEM((BLK, 1024), BF16),
        x=pltpu.VMEM((BLK, 1024), BF16),
        dw1=pltpu.VMEM((1024, 1024), BF16),
        dw2=pltpu.VMEM((1024, 1024), BF16),
    )

    def phase_two(dot_t, dqt, dkt, dvt, wo, part, x, dx, dwqkv, dwo, dct):
        l_wo = pltpu.make_async_copy(wo_hbm, wo, lsem.at[8])
        l_wo.start()
        l_x = pltpu.make_async_copy(x_hbm, x, lsem.at[9])
        l_x.start()
        dkt[...] = jnp.zeros_like(dkt)
        dvt[...] = jnp.zeros_like(dvt)
        dqt[...] = jnp.zeros_like(dqt)
        for n in range(2):
            d2_far(n).wait_send()
        l_wo.wait()

        @pl.loop(0, 4)
        def _(n):
            do_block(chip * 4 + n, e, wo, ot, dot_t, stat)

        w_swap.wait_recv()

        def swap_far(n, mine_or_theirs):
            block = (1 - chip) * 2 + 1 - n
            return send(dct.at[:, rows(block * BLK + mine_or_theirs * HALF, HALF)], dct_far.at[n], ssem.at[27 + n], rsem.at[27 + n], pair)

        def d1_far(n, piece):
            sl = rows(piece * 128, 128)
            return send(d2_send.at[n, sl, :], d1_recv.at[core, sl, :], ssem.at[30 + n + 7 * piece], rsem.at[30 + core + 7 * piece], (1 - chip) * 2 + 1 - n)

        def take_far(n):
            for half in range(2):
                from_peer(2 * n + half).wait_recv()
                relay(2 * n + half, core).start()

        def far_do(n):
            for half in range(2):
                relay(2 * n + half, 1 - core).wait_recv()

            @pl.loop(0, 2)
            def _(half):
                do_block(((1 - chip) * 2 + 1 - n) * 2 + half, e, wo, ot, dot_t, stat)

        @pl.loop(0, 6)
        def _(i):
            group = i // 2
            far = group % 2
            n = i - 2 * group
            qi = (1 - far) * (chip * 2 + n) + far * ((1 - chip) * 2 + 1 - n)
            low = (group // 2) * chip * 2
            high = far * qi + (1 - far) * ((1 - group // 2) * ((1 - chip) * qi + chip * 2) + (group // 2) * chip * qi)

            @pl.when(i == 2)
            def _():
                take_far(0)
                far_do(0)

            @pl.loop(low, high)
            def _(ki):
                attn_bwd_tile(ki * BLK, BLK, qi * BLK, BLK, False, ct, nat, dot_t, stat, dqt, dkt, dvt)

            @pl.when(far + (1 - far) * ((1 - group // 2) * (1 - chip) + (group // 2) * chip) == 1)
            def _():
                attn_bwd_tile(qi * BLK, HALF, qi * BLK, BLK, True, ct, nat, dot_t, stat, dqt, dkt, dvt)
                attn_bwd_tile(qi * BLK + HALF, HALF, qi * BLK + HALF, HALF, True, ct, nat, dot_t, stat, dqt, dkt, dvt)

            @pl.when(i == 2)
            def _():
                take_far(1)

            @pl.when(far == 1)
            def _():
                pack_dc(qi, dqt, dkt, dvt, dct)
                swap_far(n, 1 - core).start()
                part[0:HALF, :] = nn(dct[:, rows(qi * BLK + core * HALF, HALF)].T, wqkvt[...])

                swap_far(n, core).wait_recv()

                @pl.loop(0, 2)
                def _(piece):
                    sl = rows(piece * 128, 128)
                    d2_send[n, sl, :] = (part[sl, :] + nn(dct_far[n, :, sl].T, w_pair[...])).astype(BF16)
                    d1_far(n, piece).start()

                @pl.when(n == 0)
                def _():
                    far_do(1)

        @pl.loop(0, 2)
        def _(n):
            pack_dc(chip * 2 + n, dqt, dkt, dvt, dct)

        swap = send(dct.at[:, rows(pair * BLK, BLK)], dct_own, ssem.at[32], rsem.at[32], pair)
        swap.start()
        part[...] = nn(dct[:, own].T, wqkvt[...])
        swap.wait_recv()
        part[...] += nn(dct_own[...].T, w_pair[...])

        @pl.loop(0, 4)
        def _(i):
            sl = rows(i * 256, 256)
            dwo[:, sl] = nn(ot[...].astype(BF16), e[:, sl]).astype(BF16)
            dwqkv[sl, :] = nn(dct[...], n1[:, sl]).astype(BF16).T

        outs = [pltpu.make_async_copy(src, dst, lsem.at[10 + n]) for n, (src, dst) in enumerate(((dwqkv, dwqkv_hbm), (dwo, dwo_hbm)))]
        outs[0].start()
        outs[1].start()
        l_x.wait()

        def dx_out(k):
            sl = rows(k * 128, 128)
            return pltpu.make_async_copy(dx.at[sl, :], dx_hbm.at[sl, :], lsem.at[12 + k])

        @pl.loop(0, 4)
        def _(i):
            piece = i // 2
            n = i - 2 * piece
            arrived = rows(piece * 128, 128)
            send(d2_send.at[n, arrived, :], d1_recv.at[n, arrived, :], ssem.at[30 + n + 7 * piece], rsem.at[30 + n + 7 * piece], peer).wait_recv()
            sl = rows(n * HALF + piece * 128, 128)
            hat, rstd = ln_forward(x[sl, :].astype(F32))
            grad = part[sl, :] + d1_recv[n, arrived, :].astype(F32)
            dx[sl, :] = (dh1[sl, :] + ln_backward(hat, rstd, g1[...], grad)).astype(BF16)
            dx_out(n * 2 + piece).start()

        for j in range(4):
            e_peer(j).wait_send()
            relay(j, core).wait_send()
        for n in range(2):
            e_pair(n).wait_send()
            swap_far(n, 1 - core).wait_send()
            for piece in range(2):
                d1_far(n, piece).wait_send()
        w_swap.wait_send()
        swap.wait_send()
        for copy in outs + [dx_out(k) for k in range(4)]:
            copy.wait()

    tokens = 4 * BLK
    pl.run_scoped(
        phase_two,
        dot_t=pltpu.VMEM((256, tokens), BF16),
        dqt=pltpu.VMEM((256, tokens), F32),
        dkt=pltpu.VMEM((256, tokens), F32),
        dvt=pltpu.VMEM((256, tokens), F32),
        wo=pltpu.VMEM((256, 1024), BF16),
        part=pltpu.VMEM((BLK, 1024), F32),
        x=pltpu.VMEM((BLK, 1024), BF16),
        dx=pltpu.VMEM((BLK, 1024), BF16),
        dwqkv=pltpu.VMEM((1024, 768), BF16),
        dwo=pltpu.VMEM((256, 1024), BF16),
        dct=pltpu.VMEM((768, tokens), BF16),
    )


def layer_grads(h1, dy, x, g1, g2, wqkv, w1, w2, wo):
    tokens = 4 * BLK
    vmem = pltpu.VMEM
    shape = jax.ShapeDtypeStruct
    hbm = pl.BlockSpec(memory_space=pl.ANY)
    return pl.pallas_call(
        layer_kernel,
        name="layer_grads",
        out_shape=(shape((BLK, 1024), BF16), shape((1024, 768), BF16), shape((256, 1024), BF16), shape((1024, 1024), BF16), shape((1024, 1024), BF16)),
        in_specs=[hbm] * 3 + [pl.BlockSpec(memory_space=vmem)] * 2 + [hbm] * 4,
        out_specs=[hbm] * 5,
        scratch_shapes=[
            vmem((tokens, 1024), BF16),
            vmem((tokens, 1024), BF16),
            vmem((tokens, 1024), BF16),
            vmem((1024, 1024), BF16),
            vmem((2 * BLK, 1024), BF16),
            vmem((2, HALF, 1024), BF16),
            vmem((2, HALF, 1024), BF16),
            vmem((2, HALF, 1024), BF16),
            vmem((768, 1024), BF16),
            vmem((2, 768, HALF), BF16),
            vmem((768, BLK), BF16),
            vmem((768, 1024), BF16),
            vmem((BLK, 1024), F32),
            vmem((768, tokens), BF16),
            vmem((8, tokens, 64), BF16),
            vmem((256, tokens), F32),
            vmem((16, tokens), F32),
            pltpu.SemaphoreType.DMA((16,)),
            pltpu.SemaphoreType.DMA((39,)),
            pltpu.SemaphoreType.DMA((39,)),
            pltpu.SemaphoreType.REGULAR,
        ],
        compiler_params=pltpu.CompilerParams(collective_id=0, has_side_effects=True, vmem_limit_bytes=67043328),
        cost_estimate=pl.CostEstimate(flops=80_000_000_000, bytes_accessed=40_000_000, transcendentals=40_000_000),
    )(h1, dy, x, g1, g2, wqkv, w1, w2, wo)


def copy_kernel(*refs):
    count = (len(refs) - 2) // 3
    srcs, dsts, bufs, in_sem, out_sem = refs[:count], refs[count:2 * count], refs[2 * count:3 * count], refs[-2], refs[-1]
    reads = [pltpu.make_async_copy(src, buf, in_sem.at[n]) for n, (src, buf) in enumerate(zip(srcs, bufs))]
    writes = [pltpu.make_async_copy(buf, dst, out_sem.at[n]) for n, (dst, buf) in enumerate(zip(dsts, bufs))]
    for copy in reads:
        copy.start()
    for read, write in zip(reads, writes):
        read.wait()
        write.start()
    for copy in writes:
        copy.wait()


def copy_out(*arrays):
    hbm = pl.BlockSpec(memory_space=pl.ANY)
    return pl.pallas_call(
        copy_kernel,
        name="copy_out",
        out_shape=[jax.ShapeDtypeStruct(a.shape, a.dtype) for a in arrays],
        in_specs=[hbm] * len(arrays),
        out_specs=[hbm] * len(arrays),
        scratch_shapes=[pltpu.VMEM(a.shape, a.dtype) for a in arrays] + [pltpu.SemaphoreType.DMA((len(arrays),))] * 2,
        compiler_params=pltpu.CompilerParams(vmem_limit_bytes=67043328),
    )(*arrays)


def solution(mesh):
    row_spec = P(('dp', 'tp'), None)
    in_specs = (row_spec, row_spec, row_spec, P(None), P(None), P(None, 'tp'), P('tp', None, None), P(None, 'tp'), P('tp', None))
    out_specs = (row_spec, P('dp', 'tp'), P(('dp', 'tp'), None, None), P('dp', 'tp'), P(('dp', 'tp'), None))

    def device_step(in_rows, mid_rows, gout_rows, ln1_gain, ln2_gain, wqkv_loc, wout_loc, wfc1_loc, wfc2_loc):
        grad_in, grad_wqkv, grad_wout, grad_wfc1, grad_wfc2 = copy_out(*layer_grads(mid_rows, gout_rows, in_rows, ln1_gain.reshape(1, 1024), ln2_gain.reshape(1, 1024), wqkv_loc, wfc1_loc, wfc2_loc, wout_loc.reshape(256, 1024)))
        return grad_in, grad_wqkv, grad_wout.reshape(4, 64, 1024), grad_wfc1, grad_wfc2

    return jax.shard_map(device_step, mesh=mesh, in_specs=in_specs, out_specs=out_specs, check_vma=False)
```

```python
import jax
import jax.numpy as jnp
from jax import lax
from jax.experimental import pallas as pl
from jax.experimental.pallas import tpu as pltpu
from jax.sharding import PartitionSpec as P

LN_EPS = 1e-5
GELU_COEF = 0.044715
GELU_SCALE = 0.7978845608028654
LOG2E = 1.4426950408889634
F32 = jnp.float32
BF16 = jnp.bfloat16
BLK = 512
HALF = 256


def ln_forward(rows):
    row_mean = jnp.mean(rows, axis=-1, keepdims=True)
    centered = rows - row_mean
    row_rstd = lax.rsqrt(jnp.mean(centered * centered, axis=-1, keepdims=True) + LN_EPS)
    return centered * row_rstd, row_rstd


def ln_backward(x_hat, row_rstd, ln_gain, grad_norm):
    grad_hat = grad_norm * ln_gain
    proj_one = jnp.mean(grad_hat, axis=-1, keepdims=True)
    proj_two = jnp.mean(grad_hat * x_hat, axis=-1, keepdims=True)
    return row_rstd * (grad_hat - proj_one - x_hat * proj_two)


def gelu_pair(pre_act):
    tanh_val = jnp.tanh(GELU_SCALE * (pre_act + GELU_COEF * pre_act * pre_act * pre_act))
    gelu_val = 0.5 * pre_act * (1.0 + tanh_val)
    gelu_der = 0.5 * (1.0 + tanh_val) + 0.5 * pre_act * (1.0 - tanh_val * tanh_val) * GELU_SCALE * (1.0 + 3.0 * GELU_COEF * pre_act * pre_act)
    return gelu_val, gelu_der


def nn(a, b):
    return lax.dot_general(a, b, (((1,), (0,)), ((), ())), preferred_element_type=F32)


def nt(a, b):
    return lax.dot_general(a, b, (((1,), (1,)), ((), ())), preferred_element_type=F32)


def qkv_block(i, n1, wqkvt, ct, nat):
    sl = pl.ds(pl.multiple_of(i * BLK, BLK), BLK)
    for n in range(4):
        c = nt(wqkvt[n * 192:(n + 1) * 192, :], n1[sl, :]).astype(BF16)
        q = c[0:64, :] * jnp.asarray(0.125, BF16)
        ct[n * 192:n * 192 + 64, sl] = q
        ct[n * 192 + 64:n * 192 + 192, sl] = c[64:192, :]
        nat[2 * n, sl, :] = c[64:128, :].T
        nat[2 * n + 1, sl, :] = c[128:192, :].T


def fwd_init(ot, stat):
    ot[...] = jnp.zeros_like(ot)
    stat[0:4, :] = jnp.full((4, stat.shape[1]), -1e30, F32)
    stat[4:16, :] = jnp.zeros((12, stat.shape[1]), F32)


def fwd_tile(ki, qi, diag, ct, nat, ot, stat):
    qs = pl.ds(pl.multiple_of(qi * BLK, BLK), BLK)
    ks = pl.ds(pl.multiple_of(ki * BLK, BLK), BLK)
    for h in range(4):
        s = nn(nat[2 * h, ks, :], ct[3 * h * 64:3 * h * 64 + 64, qs])
        if diag:
            key = lax.broadcasted_iota(jnp.int32, (BLK, BLK), 0)
            query = lax.broadcasted_iota(jnp.int32, (BLK, BLK), 1)
            s = jnp.where(key <= query, s, -1e30)
        m_old = stat[h:h + 1, qs]
        m_new = jnp.maximum(m_old, jnp.max(s, axis=0, keepdims=True))
        alpha = jnp.exp2((m_old - m_new) * LOG2E)
        e = jnp.exp2((s - m_new) * LOG2E)
        stat[h:h + 1, qs] = m_new
        stat[4 + h:5 + h, qs] = stat[4 + h:5 + h, qs] * alpha + jnp.sum(e, axis=0, keepdims=True)
        hs = slice(h * 64, (h + 1) * 64)
        vt = ct[(3 * h + 2) * 64:(3 * h + 3) * 64, ks]
        ot[hs, qs] = ot[hs, qs] * alpha + nn(vt, e.astype(BF16))


def fwd_finish(ot, stat):
    for h in range(4):
        inv = 1.0 / stat[4 + h:5 + h, :]
        stat[4 + h:5 + h, :] = inv
        ot[h * 64:(h + 1) * 64, :] = ot[h * 64:(h + 1) * 64, :] * inv


def do_block(i, e, wo, ot, dot_t, stat):
    sl = pl.ds(pl.multiple_of(i * HALF, HALF), HALF)
    d = nt(wo[...], e[sl, :]).astype(BF16)
    dot_t[:, sl] = d
    for h in range(4):
        part = d[h * 64:(h + 1) * 64, :]
        stat[8 + h:9 + h, sl] = jnp.sum(part.astype(F32) * ot[h * 64:(h + 1) * 64, sl], axis=0, keepdims=True)


def attn_bwd_tile(k0, ksize, q0, qsize, diag, ct, nat, dot_t, stat, dqt, dkt, dvt):
    ks = pl.ds(pl.multiple_of(k0, HALF), ksize)
    qs = pl.ds(pl.multiple_of(q0, HALF), qsize)
    for h in range(4):
        s = nn(nat[2 * h, ks, :], ct[3 * h * 64:3 * h * 64 + 64, qs])
        r = nn(nat[2 * h + 1, ks, :], dot_t[h * 64:(h + 1) * 64, qs])
        p = jnp.exp2((s - stat[h:h + 1, qs]) * LOG2E) * stat[4 + h:5 + h, qs]
        if diag:
            key = lax.broadcasted_iota(jnp.int32, (ksize, qsize), 0)
            query = lax.broadcasted_iota(jnp.int32, (ksize, qsize), 1)
            p = jnp.where(key <= query, p, 0.0)
        ds = (p * (r - stat[8 + h:9 + h, qs])).astype(BF16)
        hs = slice(h * 64, (h + 1) * 64)
        dvt[hs, ks] += nt(dot_t[hs, qs], p.astype(BF16))
        dkt[hs, ks] += nt(ct[3 * h * 64:3 * h * 64 + 64, qs], ds)
        dqt[hs, qs] += nn(ct[(3 * h + 1) * 64:(3 * h + 2) * 64, ks], ds)


def pack_dc(i, dqt, dkt, dvt, dct):
    sl = pl.ds(pl.multiple_of(i * BLK, BLK), BLK)
    for h in range(4):
        dct[3 * h * 64:3 * h * 64 + 64, sl] = (dqt[h * 64:(h + 1) * 64, sl] * 0.125).astype(BF16)
        dct[(3 * h + 1) * 64:(3 * h + 2) * 64, sl] = dkt[h * 64:(h + 1) * 64, sl].astype(BF16)
        dct[(3 * h + 2) * 64:(3 * h + 3) * 64, sl] = dvt[h * 64:(h + 1) * 64, sl].astype(BF16)


MESH_ID = pl.DeviceIdType.MESH


def place():
    me = lax.axis_index('tp')
    chip = me // 2
    core = me - chip * 2
    return me, chip, core, chip * 2 + (1 - core), (1 - chip) * 2 + core, (1 - chip) * 2 + (1 - core)


def entry_barrier(others):
    barrier = pltpu.get_barrier_semaphore()
    for other in others:
        pl.semaphore_signal(barrier, inc=1, device_id={'tp': other}, device_id_type=MESH_ID)
    pl.semaphore_wait(barrier, 3)


def send(src, dst, ssem, rsem, to):
    return pltpu.make_async_remote_copy(src_ref=src, dst_ref=dst, send_sem=ssem, recv_sem=rsem, device_id={'tp': to}, device_id_type=MESH_ID)


def rows(start, size):
    return pl.ds(pl.multiple_of(start, size), size)


def tn(a, b):
    return lax.dot_general(a, b, (((0,), (0,)), ((), ())), preferred_element_type=F32)


def ln_rows(src, gain, dst, start):
    @pl.loop(0, 4)
    def _(i):
        hat, _ = ln_forward(src[rows(i * 128, 128), :].astype(F32))
        dst[rows(start + i * 128, 128), :] = (hat * gain[...]).astype(BF16)


def mlp_rows(start, n2, dy, w1, w2t, act, da):
    sl = rows(start, HALF)
    for c in range(4):
        cs = slice(c * 256, (c + 1) * 256)
        gelu_val, gelu_der = gelu_pair(nn(n2[sl, :], w1[:, cs]))
        act[sl, cs] = gelu_val.astype(BF16)
        da[sl, cs] = (nn(dy[sl, :], w2t[:, cs]) * gelu_der).astype(BF16)


def layer_kernel(h1_hbm, dy_hbm, x_hbm, g1, g2, wqkv_hbm, w1_hbm, w2_hbm, wo_hbm,
                 dx_hbm, dwqkv_hbm, dwo_hbm, dw1_hbm, dw2_hbm,
                 n2, dy, n1, w1_pair, da_pair, d2_send, d2_recv, d1_recv, w_pair, dct_far, dct_own, wqkvt, dh1, ct, nat, ot, stat,
                 lsem, ssem, rsem, free_sem):
    me, chip, core, pair, peer, diag = place()
    own = rows(me * BLK, BLK)
    e = n2

    def chunk_copy(ref, block, n, first, to):
        sl = rows(block * BLK + n * HALF, HALF)
        return send(ref.at[sl, :], ref.at[sl, :], ssem.at[first + n], rsem.at[first + n], to)

    def d2_far(n):
        return send(d2_send.at[n], d2_recv.at[n], ssem.at[19 + n], rsem.at[19 + n], peer)

    def e_half(block, part_no):
        return e.at[rows(block * BLK + part_no * HALF, HALF), :]

    def e_pair(part_no):
        ref = e_half(me, part_no)
        return send(ref, ref, ssem.at[21 + part_no], rsem.at[21 + part_no], pair)

    def from_pair(part_no):
        ref = e_half(pair, part_no)
        return send(ref, ref, ssem.at[21 + part_no], rsem.at[21 + part_no], pair)

    def e_chunk(block, part_no, who):
        return e.at[rows(block * BLK + part_no * HALF + who * 128, 128), :]

    def e_peer(j):
        ref = e_chunk(chip * 2 + 1 - j // 2, j % 2, core)
        return send(ref, ref, ssem.at[23 + j], rsem.at[23 + j], peer)

    def from_peer(j):
        ref = e_chunk((1 - chip) * 2 + 1 - j // 2, j % 2, core)
        return send(ref, ref, ssem.at[23 + j], rsem.at[23 + j], peer)

    def relay(j, who):
        ref = e_chunk((1 - chip) * 2 + 1 - j // 2, j % 2, who)
        return send(ref, ref, ssem.at[33 + j], rsem.at[33 + j], pair)

    w_swap = send(wqkvt, w_pair, ssem.at[29], rsem.at[29], pair)

    def phase_one(w1, w2t, wqkv, act, da, h1, x, dw1, dw2):
        local = []
        for n, (src, dst) in enumerate(((dy_hbm, dy.at[own, :]), (h1_hbm, h1), (x_hbm, x), (w1_hbm, w1), (w2_hbm, dw2), (wqkv_hbm, wqkv))):
            copy = pltpu.make_async_copy(src, dst, lsem.at[n])
            local.append(copy)
        l_dy, l_h1, l_x, l_w1, l_w2, l_wqkv = local
        for copy in (l_dy, l_h1, l_x):
            copy.start()

        entry_barrier((pair, peer, diag))

        first_rows = rows(me * BLK, HALF)
        send(dy_hbm.at[0:HALF, :], dy.at[first_rows, :], ssem.at[6], rsem.at[6], peer).start()
        for copy in (l_w1, l_w2, l_wqkv):
            copy.start()
        to_pair = [send(ref.at[own, :], ref.at[own, :], ssem.at[n], rsem.at[n], pair) for n, ref in enumerate((n2, dy, n1))]
        to_pair.append(send(w1, w1_pair, ssem.at[3], rsem.at[3], pair))
        l_dy.wait()
        to_pair[1].start()
        l_h1.wait()
        ln_rows(h1, g2, n2, me * BLK)
        l_x.wait()
        ln_rows(x, g1, n1, me * BLK)
        chunk_copy(n2, me, 0, 4, peer).start()
        chunk_copy(dy, me, 1, 6, peer).start()
        chunk_copy(n2, me, 1, 4, peer).start()
        for n in range(2):
            chunk_copy(n1, me, n, 8, peer).start()
        to_pair[0].start()
        to_pair[2].start()
        l_w1.wait()
        to_pair[3].start()

        l_w2.wait()
        w2t[...] = dw2[...].T

        @pl.loop(0, 4)
        def _(i):
            @pl.when(i == 2)
            def _():
                to_pair[0].wait_recv()
                to_pair[1].wait_recv()

            second = i // 2
            mlp_rows((me + second * (pair - me)) * BLK + (i - 2 * second) * HALF, n2, dy, w1, w2t, act, da)

        da_swap = send(da.at[rows(pair * BLK, BLK), :], da_pair.at[0:BLK, :], ssem.at[16], rsem.at[16], pair)
        da_swap.start()
        l_wqkv.wait()
        wqkvt[...] = wqkv[...].T
        fwd_init(ot, stat)
        to_pair[2].wait_recv()

        @pl.loop(0, 2)
        def _(n):
            qkv_block(chip * 2 + n, n1, wqkvt, ct, nat)

        w_swap.start()

        def da_far(n):
            return send(da.at[rows(diag * BLK + n * HALF, HALF), :], da_pair.at[rows(BLK + n * HALF, HALF), :], ssem.at[17 + n], rsem.at[17 + n], pair)

        to_pair[3].wait_recv()

        @pl.loop(0, 2)
        def _(n):
            chunk_copy(dy, peer, n, 6, peer).wait_recv()
            chunk_copy(dy, peer, n, 12, pair).start()
            chunk_copy(n2, peer, n, 4, peer).wait_recv()
            chunk_copy(n2, peer, n, 10, pair).start()

            @pl.loop(0, 2)
            def _(j):
                @pl.when(j == 1)
                def _():
                    chunk_copy(n2, diag, n, 10, pair).wait_recv()
                    chunk_copy(dy, diag, n, 12, pair).wait_recv()

                mlp_rows((peer + j * (diag - peer)) * BLK + n * HALF, n2, dy, w1, w2t, act, da)

            da_far(n).start()
            first = nt(da[rows(peer * BLK + n * HALF, HALF), :], w1[...])
            da_far(n).wait_recv()
            d2_send[n] = (first + nt(da_pair[rows(BLK + n * HALF, HALF), :], w1_pair[...])).astype(BF16)
            d2_far(n).start()

        da_swap.wait_recv()

        @pl.loop(0, 2)
        def _(i):
            sl = rows(i * HALF, HALF)
            dh1[sl, :] = nt(da[rows(me * BLK + i * HALF, HALF), :], w1[...]) + nt(da_pair[sl, :], w1_pair[...])

        outs = [pltpu.make_async_copy(src, dst, lsem.at[6 + n]) for n, (src, dst) in enumerate(((dw1, dw1_hbm), (dw2, dw2_hbm)))]

        def mid_grad(n):
            d2_far(n).wait_recv()
            sl = rows(n * HALF, HALF)
            hat, rstd = ln_forward(h1[sl, :].astype(F32))
            rows_n = rows(me * BLK + n * HALF, HALF)
            grad = dy[rows_n, :].astype(F32) + ln_backward(hat, rstd, g2[...], dh1[sl, :] + d2_recv[n].astype(F32))
            dh1[sl, :] = grad
            e[rows_n, :] = grad.astype(BF16)
            e_pair(n).start()
            if n == 0:
                from_pair(0).wait_recv()
                e_peer(0).start()
            else:
                @pl.when(core == 1)
                def _():
                    e_peer(1).start()

                from_pair(1).wait_recv()

                @pl.when(core == 0)
                def _():
                    e_peer(1).start()

                e_peer(2).start()
                e_peer(3).start()

        @pl.loop(0, 6)
        def _(i):
            @pl.when(i == 4)
            def _():
                pl.semaphore_wait(free_sem, 2)
                mid_grad(0)

            @pl.when(i == 2)
            def _():
                @pl.loop(0, 4)
                def _(j):
                    sl = rows(j * 256, 256)
                    dw2[sl, :] = tn(act[:, sl], dy[...]).astype(BF16)
                    dw1[sl, :] = tn(n2[:, sl], da[...]).astype(BF16)

                for copy in outs:
                    copy.start()
                to_pair[0].wait_send()
                for n in range(2):
                    chunk_copy(n2, me, n, 4, peer).wait_send()
                    chunk_copy(n2, peer, n, 10, pair).wait_send()
                for other in (pair, peer):
                    pl.semaphore_signal(free_sem, inc=1, device_id={'tp': other}, device_id_type=MESH_ID)
                for n in range(2):
                    chunk_copy(n1, peer, n, 8, peer).wait_recv()
                    chunk_copy(n1, peer, n, 14, pair).start()

                @pl.loop(0, 2)
                def _(j):
                    @pl.when(j == 1)
                    def _():
                        for n in range(2):
                            chunk_copy(n1, diag, n, 14, pair).wait_recv()

                    qkv_block(peer + j * (diag - peer), n1, wqkvt, ct, nat)

            group = i // 2
            far = group % 2
            qi = far * 2 + chip * 2 - 4 * far * chip + i - 2 * group
            low = (1 - far) * (1 - group // 2) * chip * 2
            high = qi + (group // 2) * (chip * 2 - qi)

            @pl.loop(low, high)
            def _(ki):
                fwd_tile(ki, qi, False, ct, nat, ot, stat)

            @pl.when(group < 2)
            def _():
                fwd_tile(qi, qi, True, ct, nat, ot, stat)

        fwd_finish(ot, stat)
        for copy in outs:
            copy.wait()
        for copy in to_pair[1:] + [da_swap]:
            copy.wait_send()
        for n in range(2):
            for ref, block, first, to in ((dy, me, 6, peer), (n1, me, 8, peer), (dy, peer, 12, pair), (n1, peer, 14, pair)):
                chunk_copy(ref, block, n, first, to).wait_send()
            da_far(n).wait_send()
        mid_grad(1)

    pl.run_scoped(
        phase_one,
        w1=pltpu.VMEM((1024, 1024), BF16),
        w2t=pltpu.VMEM((1024, 1024), BF16),
        wqkv=pltpu.VMEM((1024, 768), BF16),
        act=pltpu.VMEM((4 * BLK, 1024), BF16),
        da=pltpu.VMEM((4 * BLK, 1024), BF16),
        h1=pltpu.VMEM((BLK, 1024), BF16),
        x=pltpu.VMEM((BLK, 1024), BF16),
        dw1=pltpu.VMEM((1024, 1024), BF16),
        dw2=pltpu.VMEM((1024, 1024), BF16),
    )

    def phase_two(dot_t, dqt, dkt, dvt, wo, part, x, dx, dwqkv, dwo, dct):
        l_wo = pltpu.make_async_copy(wo_hbm, wo, lsem.at[8])
        l_wo.start()
        l_x = pltpu.make_async_copy(x_hbm, x, lsem.at[9])
        l_x.start()
        dkt[...] = jnp.zeros_like(dkt)
        dvt[...] = jnp.zeros_like(dvt)
        dqt[...] = jnp.zeros_like(dqt)
        for n in range(2):
            d2_far(n).wait_send()
        l_wo.wait()

        @pl.loop(0, 4)
        def _(n):
            do_block(chip * 4 + n, e, wo, ot, dot_t, stat)

        w_swap.wait_recv()

        def swap_far(n, mine_or_theirs):
            block = (1 - chip) * 2 + 1 - n
            return send(dct.at[:, rows(block * BLK + mine_or_theirs * HALF, HALF)], dct_far.at[n], ssem.at[27 + n], rsem.at[27 + n], pair)

        def d1_far(n, piece):
            sl = rows(piece * 128, 128)
            return send(d2_send.at[n, sl, :], d1_recv.at[core, sl, :], ssem.at[30 + n + 7 * piece], rsem.at[30 + core + 7 * piece], (1 - chip) * 2 + 1 - n)

        def take_far(n):
            for half in range(2):
                from_peer(2 * n + half).wait_recv()
                relay(2 * n + half, core).start()

        def far_do(n):
            @pl.loop(0, 2)
            def _(half):
                relay(2 * n + half, 1 - core).wait_recv()
                do_block(((1 - chip) * 2 + 1 - n) * 2 + half, e, wo, ot, dot_t, stat)

        @pl.loop(0, 6)
        def _(i):
            group = i // 2
            far = group % 2
            n = i - 2 * group
            qi = (1 - far) * (chip * 2 + n) + far * ((1 - chip) * 2 + 1 - n)
            low = (group // 2) * chip * 2
            high = far * qi + (1 - far) * ((1 - group // 2) * ((1 - chip) * qi + chip * 2) + (group // 2) * chip * qi)

            @pl.when(i == 2)
            def _():
                take_far(0)
                far_do(0)

            @pl.loop(low, high)
            def _(ki):
                attn_bwd_tile(ki * BLK, BLK, qi * BLK, BLK, False, ct, nat, dot_t, stat, dqt, dkt, dvt)

            @pl.when(far + (1 - far) * ((1 - group // 2) * (1 - chip) + (group // 2) * chip) == 1)
            def _():
                attn_bwd_tile(qi * BLK, HALF, qi * BLK, BLK, True, ct, nat, dot_t, stat, dqt, dkt, dvt)
                attn_bwd_tile(qi * BLK + HALF, HALF, qi * BLK + HALF, HALF, True, ct, nat, dot_t, stat, dqt, dkt, dvt)

            @pl.when(i == 2)
            def _():
                take_far(1)

            @pl.when(far == 1)
            def _():
                pack_dc(qi, dqt, dkt, dvt, dct)
                swap_far(n, 1 - core).start()
                part[0:HALF, :] = nn(dct[:, rows(qi * BLK + core * HALF, HALF)].T, wqkvt[...])

                swap_far(n, core).wait_recv()

                @pl.loop(0, 2)
                def _(piece):
                    sl = rows(piece * 128, 128)
                    d2_send[n, sl, :] = (part[sl, :] + nn(dct_far[n, :, sl].T, w_pair[...])).astype(BF16)
                    d1_far(n, piece).start()

                @pl.when(n == 0)
                def _():
                    far_do(1)

        @pl.loop(0, 2)
        def _(n):
            pack_dc(chip * 2 + n, dqt, dkt, dvt, dct)

        swap = send(dct.at[:, rows(pair * BLK, BLK)], dct_own, ssem.at[32], rsem.at[32], pair)
        swap.start()
        part[...] = nn(dct[:, own].T, wqkvt[...])
        swap.wait_recv()
        part[...] += nn(dct_own[...].T, w_pair[...])

        @pl.loop(0, 4)
        def _(i):
            sl = rows(i * 256, 256)
            dwo[:, sl] = nn(ot[...].astype(BF16), e[:, sl]).astype(BF16)
            dwqkv[sl, :] = nn(dct[...], n1[:, sl]).astype(BF16).T

        outs = [pltpu.make_async_copy(src, dst, lsem.at[10 + n]) for n, (src, dst) in enumerate(((dwqkv, dwqkv_hbm), (dwo, dwo_hbm)))]
        outs[0].start()
        outs[1].start()
        l_x.wait()

        def dx_out(k):
            sl = rows(k * 128, 128)
            return pltpu.make_async_copy(dx.at[sl, :], dx_hbm.at[sl, :], lsem.at[12 + k])

        @pl.loop(0, 4)
        def _(i):
            piece = i // 2
            n = i - 2 * piece
            arrived = rows(piece * 128, 128)
            send(d2_send.at[n, arrived, :], d1_recv.at[n, arrived, :], ssem.at[30 + n + 7 * piece], rsem.at[30 + n + 7 * piece], peer).wait_recv()
            sl = rows(n * HALF + piece * 128, 128)
            hat, rstd = ln_forward(x[sl, :].astype(F32))
            grad = part[sl, :] + d1_recv[n, arrived, :].astype(F32)
            dx[sl, :] = (dh1[sl, :] + ln_backward(hat, rstd, g1[...], grad)).astype(BF16)
            dx_out(n * 2 + piece).start()

        for j in range(4):
            e_peer(j).wait_send()
            relay(j, core).wait_send()
        for n in range(2):
            e_pair(n).wait_send()
            swap_far(n, 1 - core).wait_send()
            for piece in range(2):
                d1_far(n, piece).wait_send()
        w_swap.wait_send()
        swap.wait_send()
        for copy in outs + [dx_out(k) for k in range(4)]:
            copy.wait()

    tokens = 4 * BLK
    pl.run_scoped(
        phase_two,
        dot_t=pltpu.VMEM((256, tokens), BF16),
        dqt=pltpu.VMEM((256, tokens), F32),
        dkt=pltpu.VMEM((256, tokens), F32),
        dvt=pltpu.VMEM((256, tokens), F32),
        wo=pltpu.VMEM((256, 1024), BF16),
        part=pltpu.VMEM((BLK, 1024), F32),
        x=pltpu.VMEM((BLK, 1024), BF16),
        dx=pltpu.VMEM((BLK, 1024), BF16),
        dwqkv=pltpu.VMEM((1024, 768), BF16),
        dwo=pltpu.VMEM((256, 1024), BF16),
        dct=pltpu.VMEM((768, tokens), BF16),
    )


def layer_grads(h1, dy, x, g1, g2, wqkv, w1, w2, wo):
    tokens = 4 * BLK
    vmem = pltpu.VMEM
    shape = jax.ShapeDtypeStruct
    hbm = pl.BlockSpec(memory_space=pl.ANY)
    return pl.pallas_call(
        layer_kernel,
        name="layer_grads",
        out_shape=(shape((BLK, 1024), BF16), shape((1024, 768), BF16), shape((256, 1024), BF16), shape((1024, 1024), BF16), shape((1024, 1024), BF16)),
        in_specs=[hbm] * 3 + [pl.BlockSpec(memory_space=vmem)] * 2 + [hbm] * 4,
        out_specs=[hbm] * 5,
        scratch_shapes=[
            vmem((tokens, 1024), BF16),
            vmem((tokens, 1024), BF16),
            vmem((tokens, 1024), BF16),
            vmem((1024, 1024), BF16),
            vmem((2 * BLK, 1024), BF16),
            vmem((2, HALF, 1024), BF16),
            vmem((2, HALF, 1024), BF16),
            vmem((2, HALF, 1024), BF16),
            vmem((768, 1024), BF16),
            vmem((2, 768, HALF), BF16),
            vmem((768, BLK), BF16),
            vmem((768, 1024), BF16),
            vmem((BLK, 1024), F32),
            vmem((768, tokens), BF16),
            vmem((8, tokens, 64), BF16),
            vmem((256, tokens), F32),
            vmem((16, tokens), F32),
            pltpu.SemaphoreType.DMA((16,)),
            pltpu.SemaphoreType.DMA((39,)),
            pltpu.SemaphoreType.DMA((39,)),
            pltpu.SemaphoreType.REGULAR,
        ],
        compiler_params=pltpu.CompilerParams(collective_id=0, has_side_effects=True, vmem_limit_bytes=67043328),
        cost_estimate=pl.CostEstimate(flops=80_000_000_000, bytes_accessed=40_000_000, transcendentals=40_000_000),
    )(h1, dy, x, g1, g2, wqkv, w1, w2, wo)


def copy_kernel(*refs):
    count = (len(refs) - 2) // 3
    srcs, dsts, bufs, in_sem, out_sem = refs[:count], refs[count:2 * count], refs[2 * count:3 * count], refs[-2], refs[-1]
    reads = [pltpu.make_async_copy(src, buf, in_sem.at[n]) for n, (src, buf) in enumerate(zip(srcs, bufs))]
    writes = [pltpu.make_async_copy(buf, dst, out_sem.at[n]) for n, (dst, buf) in enumerate(zip(dsts, bufs))]
    for copy in reads:
        copy.start()
    for read, write in zip(reads, writes):
        read.wait()
        write.start()
    for copy in writes:
        copy.wait()


def copy_out(*arrays):
    hbm = pl.BlockSpec(memory_space=pl.ANY)
    return pl.pallas_call(
        copy_kernel,
        name="copy_out",
        out_shape=[jax.ShapeDtypeStruct(a.shape, a.dtype) for a in arrays],
        in_specs=[hbm] * len(arrays),
        out_specs=[hbm] * len(arrays),
        scratch_shapes=[pltpu.VMEM(a.shape, a.dtype) for a in arrays] + [pltpu.SemaphoreType.DMA((len(arrays),))] * 2,
        compiler_params=pltpu.CompilerParams(vmem_limit_bytes=67043328),
    )(*arrays)


def solution(mesh):
    row_spec = P(('dp', 'tp'), None)
    in_specs = (row_spec, row_spec, row_spec, P(None), P(None), P(None, 'tp'), P('tp', None, None), P(None, 'tp'), P('tp', None))
    out_specs = (row_spec, P('dp', 'tp'), P(('dp', 'tp'), None, None), P('dp', 'tp'), P(('dp', 'tp'), None))

    def device_step(in_rows, mid_rows, gout_rows, ln1_gain, ln2_gain, wqkv_loc, wout_loc, wfc1_loc, wfc2_loc):
        grad_in, grad_wqkv, grad_wout, grad_wfc1, grad_wfc2 = copy_out(*layer_grads(mid_rows, gout_rows, in_rows, ln1_gain.reshape(1, 1024), ln2_gain.reshape(1, 1024), wqkv_loc, wfc1_loc, wfc2_loc, wout_loc.reshape(256, 1024)))
        return grad_in, grad_wqkv, grad_wout.reshape(4, 64, 1024), grad_wfc1, grad_wfc2

    return jax.shard_map(device_step, mesh=mesh, in_specs=in_specs, out_specs=out_specs, check_vma=False)
```

```python
import jax
import jax.numpy as jnp
from jax import lax
from jax.experimental import pallas as pl
from jax.experimental.pallas import tpu as pltpu
from jax.sharding import PartitionSpec as P

LN_EPS = 1e-5
GELU_COEF = 0.044715
GELU_SCALE = 0.7978845608028654
LOG2E = 1.4426950408889634
F32 = jnp.float32
BF16 = jnp.bfloat16
BLK = 512
HALF = 256


def ln_forward(rows):
    row_mean = jnp.mean(rows, axis=-1, keepdims=True)
    centered = rows - row_mean
    row_rstd = lax.rsqrt(jnp.mean(centered * centered, axis=-1, keepdims=True) + LN_EPS)
    return centered * row_rstd, row_rstd


def ln_backward(x_hat, row_rstd, ln_gain, grad_norm):
    grad_hat = grad_norm * ln_gain
    proj_one = jnp.mean(grad_hat, axis=-1, keepdims=True)
    proj_two = jnp.mean(grad_hat * x_hat, axis=-1, keepdims=True)
    return row_rstd * (grad_hat - proj_one - x_hat * proj_two)


def gelu_pair(pre_act):
    tanh_val = jnp.tanh(GELU_SCALE * (pre_act + GELU_COEF * pre_act * pre_act * pre_act))
    gelu_val = 0.5 * pre_act * (1.0 + tanh_val)
    gelu_der = 0.5 * (1.0 + tanh_val) + 0.5 * pre_act * (1.0 - tanh_val * tanh_val) * GELU_SCALE * (1.0 + 3.0 * GELU_COEF * pre_act * pre_act)
    return gelu_val, gelu_der


def nn(a, b):
    return lax.dot_general(a, b, (((1,), (0,)), ((), ())), preferred_element_type=F32)


def nt(a, b):
    return lax.dot_general(a, b, (((1,), (1,)), ((), ())), preferred_element_type=F32)


def qkv_block(i, n1, wqkvt, ct, nat):
    sl = pl.ds(pl.multiple_of(i * BLK, BLK), BLK)
    for n in range(4):
        c = nt(wqkvt[n * 192:(n + 1) * 192, :], n1[sl, :]).astype(BF16)
        q = c[0:64, :] * jnp.asarray(0.125, BF16)
        ct[n * 192:n * 192 + 64, sl] = q
        ct[n * 192 + 64:n * 192 + 192, sl] = c[64:192, :]
        nat[2 * n, sl, :] = c[64:128, :].T
        nat[2 * n + 1, sl, :] = c[128:192, :].T


def fwd_init(ot, stat):
    ot[...] = jnp.zeros_like(ot)
    stat[0:4, :] = jnp.full((4, stat.shape[1]), -1e30, F32)
    stat[4:16, :] = jnp.zeros((12, stat.shape[1]), F32)


def fwd_tile(ki, qi, diag, ct, nat, ot, stat):
    qs = pl.ds(pl.multiple_of(qi * BLK, BLK), BLK)
    ks = pl.ds(pl.multiple_of(ki * BLK, BLK), BLK)
    for h in range(4):
        s = nn(nat[2 * h, ks, :], ct[3 * h * 64:3 * h * 64 + 64, qs])
        if diag:
            key = lax.broadcasted_iota(jnp.int32, (BLK, BLK), 0)
            query = lax.broadcasted_iota(jnp.int32, (BLK, BLK), 1)
            s = jnp.where(key <= query, s, -1e30)
        m_old = stat[h:h + 1, qs]
        m_new = jnp.maximum(m_old, jnp.max(s, axis=0, keepdims=True))
        alpha = jnp.exp2((m_old - m_new) * LOG2E)
        e = jnp.exp2((s - m_new) * LOG2E)
        stat[h:h + 1, qs] = m_new
        stat[4 + h:5 + h, qs] = stat[4 + h:5 + h, qs] * alpha + jnp.sum(e, axis=0, keepdims=True)
        hs = slice(h * 64, (h + 1) * 64)
        vt = ct[(3 * h + 2) * 64:(3 * h + 3) * 64, ks]
        ot[hs, qs] = ot[hs, qs] * alpha + nn(vt, e.astype(BF16))


def fwd_finish(ot, stat):
    for h in range(4):
        inv = 1.0 / stat[4 + h:5 + h, :]
        stat[4 + h:5 + h, :] = inv
        ot[h * 64:(h + 1) * 64, :] = ot[h * 64:(h + 1) * 64, :] * inv


def do_block(i, e, wo, ot, dot_t, stat):
    sl = pl.ds(pl.multiple_of(i * HALF, HALF), HALF)
    d = nt(wo[...], e[sl, :]).astype(BF16)
    dot_t[:, sl] = d
    for h in range(4):
        part = d[h * 64:(h + 1) * 64, :]
        stat[8 + h:9 + h, sl] = jnp.sum(part.astype(F32) * ot[h * 64:(h + 1) * 64, sl], axis=0, keepdims=True)


def attn_bwd_tile(k0, ksize, q0, qsize, diag, ct, nat, dot_t, stat, dqt, dkt, dvt):
    ks = pl.ds(pl.multiple_of(k0, HALF), ksize)
    qs = pl.ds(pl.multiple_of(q0, HALF), qsize)
    for h in range(4):
        s = nn(nat[2 * h, ks, :], ct[3 * h * 64:3 * h * 64 + 64, qs])
        r = nn(nat[2 * h + 1, ks, :], dot_t[h * 64:(h + 1) * 64, qs])
        p = jnp.exp2((s - stat[h:h + 1, qs]) * LOG2E) * stat[4 + h:5 + h, qs]
        if diag:
            key = lax.broadcasted_iota(jnp.int32, (ksize, qsize), 0)
            query = lax.broadcasted_iota(jnp.int32, (ksize, qsize), 1)
            p = jnp.where(key <= query, p, 0.0)
        ds = (p * (r - stat[8 + h:9 + h, qs])).astype(BF16)
        hs = slice(h * 64, (h + 1) * 64)
        dvt[hs, ks] += nt(dot_t[hs, qs], p.astype(BF16))
        dkt[hs, ks] += nt(ct[3 * h * 64:3 * h * 64 + 64, qs], ds)
        dqt[hs, qs] += nn(ct[(3 * h + 1) * 64:(3 * h + 2) * 64, ks], ds)


def pack_dc(i, dqt, dkt, dvt, dct):
    sl = pl.ds(pl.multiple_of(i * BLK, BLK), BLK)
    for h in range(4):
        dct[3 * h * 64:3 * h * 64 + 64, sl] = (dqt[h * 64:(h + 1) * 64, sl] * 0.125).astype(BF16)
        dct[(3 * h + 1) * 64:(3 * h + 2) * 64, sl] = dkt[h * 64:(h + 1) * 64, sl].astype(BF16)
        dct[(3 * h + 2) * 64:(3 * h + 3) * 64, sl] = dvt[h * 64:(h + 1) * 64, sl].astype(BF16)


MESH_ID = pl.DeviceIdType.MESH


def place():
    me = lax.axis_index('tp')
    chip = me // 2
    core = me - chip * 2
    return me, chip, core, chip * 2 + (1 - core), (1 - chip) * 2 + core, (1 - chip) * 2 + (1 - core)


def entry_barrier(others):
    barrier = pltpu.get_barrier_semaphore()
    for other in others:
        pl.semaphore_signal(barrier, inc=1, device_id={'tp': other}, device_id_type=MESH_ID)
    pl.semaphore_wait(barrier, 3)


def send(src, dst, ssem, rsem, to):
    return pltpu.make_async_remote_copy(src_ref=src, dst_ref=dst, send_sem=ssem, recv_sem=rsem, device_id={'tp': to}, device_id_type=MESH_ID)


def rows(start, size):
    return pl.ds(pl.multiple_of(start, size), size)


def tn(a, b):
    return lax.dot_general(a, b, (((0,), (0,)), ((), ())), preferred_element_type=F32)


def ln_rows(src, gain, dst, start):
    @pl.loop(0, 4)
    def _(i):
        hat, _ = ln_forward(src[rows(i * 128, 128), :].astype(F32))
        dst[rows(start + i * 128, 128), :] = (hat * gain[...]).astype(BF16)


def mlp_rows(start, n2, dy, w1, w2t, act, da):
    sl = rows(start, HALF)
    for c in range(4):
        cs = slice(c * 256, (c + 1) * 256)
        gelu_val, gelu_der = gelu_pair(nn(n2[sl, :], w1[:, cs]))
        act[sl, cs] = gelu_val.astype(BF16)
        da[sl, cs] = (nn(dy[sl, :], w2t[:, cs]) * gelu_der).astype(BF16)


def layer_kernel(h1_hbm, dy_hbm, x_hbm, g1, g2, wqkv_hbm, w1_hbm, w2_hbm, wo_hbm,
                 dx_hbm, dwqkv_hbm, dwo_hbm, dw1_hbm, dw2_hbm,
                 n2, dy, n1, w1_pair, da_pair, d2_send, d2_recv, d1_recv, w_pair, dct_far, dct_own, wqkvt, dh1, ct, nat, ot, stat,
                 lsem, ssem, rsem, free_sem):
    me, chip, core, pair, peer, diag = place()
    own = rows(me * BLK, BLK)
    e = n2

    def chunk_copy(ref, block, n, first, to):
        sl = rows(block * BLK + n * HALF, HALF)
        return send(ref.at[sl, :], ref.at[sl, :], ssem.at[first + n], rsem.at[first + n], to)

    def d2_far(n):
        return send(d2_send.at[n], d2_recv.at[n], ssem.at[19 + n], rsem.at[19 + n], peer)

    def e_half(block, part_no):
        return e.at[rows(block * BLK + part_no * HALF, HALF), :]

    def e_pair(part_no):
        ref = e_half(me, part_no)
        return send(ref, ref, ssem.at[21 + part_no], rsem.at[21 + part_no], pair)

    def from_pair(part_no):
        ref = e_half(pair, part_no)
        return send(ref, ref, ssem.at[21 + part_no], rsem.at[21 + part_no], pair)

    def e_chunk(block, part_no, who):
        return e.at[rows(block * BLK + part_no * HALF + who * 128, 128), :]

    def e_peer(j):
        ref = e_chunk(chip * 2 + 1 - j // 2, j % 2, core)
        return send(ref, ref, ssem.at[23 + j], rsem.at[23 + j], peer)

    def from_peer(j):
        ref = e_chunk((1 - chip) * 2 + 1 - j // 2, j % 2, core)
        return send(ref, ref, ssem.at[23 + j], rsem.at[23 + j], peer)

    def relay(j, who):
        ref = e_chunk((1 - chip) * 2 + 1 - j // 2, j % 2, who)
        return send(ref, ref, ssem.at[33 + j], rsem.at[33 + j], pair)

    w_swap = send(wqkvt, w_pair, ssem.at[29], rsem.at[29], pair)

    def phase_one(w1, w2t, wqkv, act, da, h1, x, dw1, dw2):
        local = []
        for n, (src, dst) in enumerate(((dy_hbm, dy.at[own, :]), (h1_hbm, h1), (x_hbm, x), (w1_hbm, w1), (w2_hbm, dw2), (wqkv_hbm, wqkv))):
            copy = pltpu.make_async_copy(src, dst, lsem.at[n])
            local.append(copy)
        l_dy, l_h1, l_x, l_w1, l_w2, l_wqkv = local
        for copy in (l_dy, l_h1, l_x):
            copy.start()

        entry_barrier((pair, peer, diag))

        first_rows = rows(me * BLK, HALF)
        send(dy_hbm.at[0:HALF, :], dy.at[first_rows, :], ssem.at[6], rsem.at[6], peer).start()
        for copy in (l_w1, l_w2, l_wqkv):
            copy.start()
        to_pair = [send(ref.at[own, :], ref.at[own, :], ssem.at[n], rsem.at[n], pair) for n, ref in enumerate((n2, dy, n1))]
        to_pair.append(send(w1, w1_pair, ssem.at[3], rsem.at[3], pair))
        l_dy.wait()
        to_pair[1].start()
        l_h1.wait()
        ln_rows(h1, g2, n2, me * BLK)
        l_x.wait()
        ln_rows(x, g1, n1, me * BLK)
        chunk_copy(n2, me, 0, 4, peer).start()
        chunk_copy(dy, me, 1, 6, peer).start()
        chunk_copy(n2, me, 1, 4, peer).start()
        for n in range(2):
            chunk_copy(n1, me, n, 8, peer).start()
        to_pair[0].start()
        to_pair[2].start()
        l_w1.wait()
        to_pair[3].start()

        l_w2.wait()
        w2t[...] = dw2[...].T

        @pl.loop(0, 4)
        def _(i):
            @pl.when(i == 2)
            def _():
                to_pair[0].wait_recv()
                to_pair[1].wait_recv()

            second = i // 2
            mlp_rows((me + second * (pair - me)) * BLK + (i - 2 * second) * HALF, n2, dy, w1, w2t, act, da)

        da_swap = send(da.at[rows(pair * BLK, BLK), :], da_pair.at[0:BLK, :], ssem.at[16], rsem.at[16], pair)
        da_swap.start()
        l_wqkv.wait()
        wqkvt[...] = wqkv[...].T
        fwd_init(ot, stat)
        to_pair[2].wait_recv()

        @pl.loop(0, 2)
        def _(n):
            qkv_block(chip * 2 + n, n1, wqkvt, ct, nat)

        w_swap.start()

        def da_far(n):
            return send(da.at[rows(diag * BLK + n * HALF, HALF), :], da_pair.at[rows(BLK + n * HALF, HALF), :], ssem.at[17 + n], rsem.at[17 + n], pair)

        to_pair[3].wait_recv()

        @pl.loop(0, 2)
        def _(n):
            chunk_copy(dy, peer, n, 6, peer).wait_recv()
            chunk_copy(dy, peer, n, 12, pair).start()
            chunk_copy(n2, peer, n, 4, peer).wait_recv()
            chunk_copy(n2, peer, n, 10, pair).start()

            @pl.loop(0, 2)
            def _(j):
                @pl.when(j == 1)
                def _():
                    chunk_copy(n2, diag, n, 10, pair).wait_recv()
                    chunk_copy(dy, diag, n, 12, pair).wait_recv()

                mlp_rows((peer + j * (diag - peer)) * BLK + n * HALF, n2, dy, w1, w2t, act, da)

            da_far(n).start()
            first = nt(da[rows(peer * BLK + n * HALF, HALF), :], w1[...])
            da_far(n).wait_recv()
            d2_send[n] = (first + nt(da_pair[rows(BLK + n * HALF, HALF), :], w1_pair[...])).astype(BF16)
            d2_far(n).start()

        da_swap.wait_recv()

        @pl.loop(0, 2)
        def _(i):
            sl = rows(i * HALF, HALF)
            dh1[sl, :] = nt(da[rows(me * BLK + i * HALF, HALF), :], w1[...]) + nt(da_pair[sl, :], w1_pair[...])

        outs = [pltpu.make_async_copy(src, dst, lsem.at[6 + n]) for n, (src, dst) in enumerate(((dw1, dw1_hbm), (dw2, dw2_hbm)))]

        def mid_grad(n):
            d2_far(n).wait_recv()
            sl = rows(n * HALF, HALF)
            hat, rstd = ln_forward(h1[sl, :].astype(F32))
            rows_n = rows(me * BLK + n * HALF, HALF)
            grad = dy[rows_n, :].astype(F32) + ln_backward(hat, rstd, g2[...], dh1[sl, :] + d2_recv[n].astype(F32))
            dh1[sl, :] = grad
            e[rows_n, :] = grad.astype(BF16)
            e_pair(n).start()
            if n == 0:
                from_pair(0).wait_recv()
                e_peer(0).start()
            else:
                @pl.when(core == 1)
                def _():
                    e_peer(1).start()

                from_pair(1).wait_recv()

                @pl.when(core == 0)
                def _():
                    e_peer(1).start()

                e_peer(2).start()
                e_peer(3).start()

        @pl.loop(0, 6)
        def _(i):
            @pl.when(i == 4)
            def _():
                pl.semaphore_wait(free_sem, 2)
                mid_grad(0)

            @pl.when(i == 2)
            def _():
                @pl.loop(0, 4)
                def _(j):
                    sl = rows(j * 256, 256)
                    dw2[sl, :] = tn(act[:, sl], dy[...]).astype(BF16)
                    dw1[sl, :] = tn(n2[:, sl], da[...]).astype(BF16)

                for copy in outs:
                    copy.start()
                to_pair[0].wait_send()
                for n in range(2):
                    chunk_copy(n2, me, n, 4, peer).wait_send()
                    chunk_copy(n2, peer, n, 10, pair).wait_send()
                for other in (pair, peer):
                    pl.semaphore_signal(free_sem, inc=1, device_id={'tp': other}, device_id_type=MESH_ID)
                for n in range(2):
                    chunk_copy(n1, peer, n, 8, peer).wait_recv()
                    chunk_copy(n1, peer, n, 14, pair).start()

                @pl.loop(0, 2)
                def _(j):
                    @pl.when(j == 1)
                    def _():
                        for n in range(2):
                            chunk_copy(n1, diag, n, 14, pair).wait_recv()

                    qkv_block(peer + j * (diag - peer), n1, wqkvt, ct, nat)

            group = i // 2
            far = group % 2
            qi = far * 2 + chip * 2 - 4 * far * chip + i - 2 * group
            low = (1 - far) * (1 - group // 2) * chip * 2
            high = qi + (group // 2) * (chip * 2 - qi)

            @pl.loop(low, high)
            def _(ki):
                fwd_tile(ki, qi, False, ct, nat, ot, stat)

            @pl.when(group < 2)
            def _():
                fwd_tile(qi, qi, True, ct, nat, ot, stat)

        fwd_finish(ot, stat)
        for copy in outs:
            copy.wait()
        for copy in to_pair[1:] + [da_swap]:
            copy.wait_send()
        for n in range(2):
            for ref, block, first, to in ((dy, me, 6, peer), (n1, me, 8, peer), (dy, peer, 12, pair), (n1, peer, 14, pair)):
                chunk_copy(ref, block, n, first, to).wait_send()
            da_far(n).wait_send()
        mid_grad(1)

    pl.run_scoped(
        phase_one,
        w1=pltpu.VMEM((1024, 1024), BF16),
        w2t=pltpu.VMEM((1024, 1024), BF16),
        wqkv=pltpu.VMEM((1024, 768), BF16),
        act=pltpu.VMEM((4 * BLK, 1024), BF16),
        da=pltpu.VMEM((4 * BLK, 1024), BF16),
        h1=pltpu.VMEM((BLK, 1024), BF16),
        x=pltpu.VMEM((BLK, 1024), BF16),
        dw1=pltpu.VMEM((1024, 1024), BF16),
        dw2=pltpu.VMEM((1024, 1024), BF16),
    )

    def phase_two(dot_t, dqt, dkt, dvt, wo, part, x, dx, dwqkv, dwo, dct):
        l_wo = pltpu.make_async_copy(wo_hbm, wo, lsem.at[8])
        l_wo.start()
        l_x = pltpu.make_async_copy(x_hbm, x, lsem.at[9])
        l_x.start()
        dkt[...] = jnp.zeros_like(dkt)
        dvt[...] = jnp.zeros_like(dvt)
        dqt[...] = jnp.zeros_like(dqt)
        for n in range(2):
            d2_far(n).wait_send()
        l_wo.wait()

        @pl.loop(0, 4)
        def _(n):
            do_block(chip * 4 + n, e, wo, ot, dot_t, stat)

        w_swap.wait_recv()

        def swap_far(n, mine_or_theirs):
            block = (1 - chip) * 2 + 1 - n
            return send(dct.at[:, rows(block * BLK + mine_or_theirs * HALF, HALF)], dct_far.at[n], ssem.at[27 + n], rsem.at[27 + n], pair)

        def d1_far(n, piece):
            sl = rows(piece * 64, 64)
            return send(d2_send.at[n, sl, :], d1_recv.at[core, sl, :], ssem.at[39 + n + 2 * piece], rsem.at[39 + core + 2 * piece], (1 - chip) * 2 + 1 - n)

        def take_far(n):
            for half in range(2):
                from_peer(2 * n + half).wait_recv()
                relay(2 * n + half, core).start()

        def far_do(n):
            @pl.loop(0, 2)
            def _(half):
                relay(2 * n + half, 1 - core).wait_recv()
                do_block(((1 - chip) * 2 + 1 - n) * 2 + half, e, wo, ot, dot_t, stat)

        @pl.loop(0, 6)
        def _(i):
            group = i // 2
            far = group % 2
            n = i - 2 * group
            qi = (1 - far) * (chip * 2 + n) + far * ((1 - chip) * 2 + 1 - n)
            low = (group // 2) * chip * 2
            high = far * qi + (1 - far) * ((1 - group // 2) * ((1 - chip) * qi + chip * 2) + (group // 2) * chip * qi)

            @pl.when(i == 2)
            def _():
                take_far(0)
                far_do(0)

            @pl.loop(low, high)
            def _(ki):
                attn_bwd_tile(ki * BLK, BLK, qi * BLK, BLK, False, ct, nat, dot_t, stat, dqt, dkt, dvt)

            @pl.when(far + (1 - far) * ((1 - group // 2) * (1 - chip) + (group // 2) * chip) == 1)
            def _():
                attn_bwd_tile(qi * BLK, HALF, qi * BLK, BLK, True, ct, nat, dot_t, stat, dqt, dkt, dvt)
                attn_bwd_tile(qi * BLK + HALF, HALF, qi * BLK + HALF, HALF, True, ct, nat, dot_t, stat, dqt, dkt, dvt)

            @pl.when(i == 2)
            def _():
                take_far(1)

            @pl.when(far == 1)
            def _():
                pack_dc(qi, dqt, dkt, dvt, dct)
                swap_far(n, 1 - core).start()
                part[0:HALF, :] = nn(dct[:, rows(qi * BLK + core * HALF, HALF)].T, wqkvt[...])

                swap_far(n, core).wait_recv()

                @pl.loop(0, 2)
                def _(piece):
                    sl = rows(piece * 128, 128)
                    d2_send[n, sl, :] = (part[sl, :] + nn(dct_far[n, :, sl].T, w_pair[...])).astype(BF16)
                    d1_far(n, 2 * piece).start()
                    d1_far(n, 2 * piece + 1).start()

                @pl.when(n == 0)
                def _():
                    far_do(1)

        @pl.loop(0, 2)
        def _(n):
            pack_dc(chip * 2 + n, dqt, dkt, dvt, dct)

        swap = send(dct.at[:, rows(pair * BLK, BLK)], dct_own, ssem.at[32], rsem.at[32], pair)
        swap.start()
        part[...] = nn(dct[:, own].T, wqkvt[...])
        swap.wait_recv()
        part[...] += nn(dct_own[...].T, w_pair[...])

        @pl.loop(0, 4)
        def _(i):
            sl = rows(i * 256, 256)
            dwo[:, sl] = nn(ot[...].astype(BF16), e[:, sl]).astype(BF16)
            dwqkv[sl, :] = nn(dct[...], n1[:, sl]).astype(BF16).T

        outs = [pltpu.make_async_copy(src, dst, lsem.at[10 + n]) for n, (src, dst) in enumerate(((dwqkv, dwqkv_hbm), (dwo, dwo_hbm)))]
        outs[0].start()
        outs[1].start()
        l_x.wait()

        def dx_out(k):
            sl = rows(k * 64, 64)
            return pltpu.make_async_copy(dx.at[sl, :], dx_hbm.at[sl, :], lsem.at[12 + k])

        @pl.loop(0, 8)
        def _(i):
            piece = i // 2
            n = i - 2 * piece
            arrived = rows(piece * 64, 64)
            send(d2_send.at[n, arrived, :], d1_recv.at[n, arrived, :], ssem.at[39 + n + 2 * piece], rsem.at[39 + n + 2 * piece], peer).wait_recv()
            sl = rows(n * HALF + piece * 64, 64)
            hat, rstd = ln_forward(x[sl, :].astype(F32))
            grad = part[sl, :] + d1_recv[n, arrived, :].astype(F32)
            dx[sl, :] = (dh1[sl, :] + ln_backward(hat, rstd, g1[...], grad)).astype(BF16)
            dx_out(n * 4 + piece).start()

        for j in range(4):
            e_peer(j).wait_send()
            relay(j, core).wait_send()
        for n in range(2):
            e_pair(n).wait_send()
            swap_far(n, 1 - core).wait_send()
            for piece in range(4):
                d1_far(n, piece).wait_send()
        w_swap.wait_send()
        swap.wait_send()
        for copy in outs + [dx_out(k) for k in range(8)]:
            copy.wait()

    tokens = 4 * BLK
    pl.run_scoped(
        phase_two,
        dot_t=pltpu.VMEM((256, tokens), BF16),
        dqt=pltpu.VMEM((256, tokens), F32),
        dkt=pltpu.VMEM((256, tokens), F32),
        dvt=pltpu.VMEM((256, tokens), F32),
        wo=pltpu.VMEM((256, 1024), BF16),
        part=pltpu.VMEM((BLK, 1024), F32),
        x=pltpu.VMEM((BLK, 1024), BF16),
        dx=pltpu.VMEM((BLK, 1024), BF16),
        dwqkv=pltpu.VMEM((1024, 768), BF16),
        dwo=pltpu.VMEM((256, 1024), BF16),
        dct=pltpu.VMEM((768, tokens), BF16),
    )


def layer_grads(h1, dy, x, g1, g2, wqkv, w1, w2, wo):
    tokens = 4 * BLK
    vmem = pltpu.VMEM
    shape = jax.ShapeDtypeStruct
    hbm = pl.BlockSpec(memory_space=pl.ANY)
    return pl.pallas_call(
        layer_kernel,
        name="layer_grads",
        out_shape=(shape((BLK, 1024), BF16), shape((1024, 768), BF16), shape((256, 1024), BF16), shape((1024, 1024), BF16), shape((1024, 1024), BF16)),
        in_specs=[hbm] * 3 + [pl.BlockSpec(memory_space=vmem)] * 2 + [hbm] * 4,
        out_specs=[hbm] * 5,
        scratch_shapes=[
            vmem((tokens, 1024), BF16),
            vmem((tokens, 1024), BF16),
            vmem((tokens, 1024), BF16),
            vmem((1024, 1024), BF16),
            vmem((2 * BLK, 1024), BF16),
            vmem((2, HALF, 1024), BF16),
            vmem((2, HALF, 1024), BF16),
            vmem((2, HALF, 1024), BF16),
            vmem((768, 1024), BF16),
            vmem((2, 768, HALF), BF16),
            vmem((768, BLK), BF16),
            vmem((768, 1024), BF16),
            vmem((BLK, 1024), F32),
            vmem((768, tokens), BF16),
            vmem((8, tokens, 64), BF16),
            vmem((256, tokens), F32),
            vmem((16, tokens), F32),
            pltpu.SemaphoreType.DMA((20,)),
            pltpu.SemaphoreType.DMA((47,)),
            pltpu.SemaphoreType.DMA((47,)),
            pltpu.SemaphoreType.REGULAR,
        ],
        compiler_params=pltpu.CompilerParams(collective_id=0, has_side_effects=True, vmem_limit_bytes=67043328),
        cost_estimate=pl.CostEstimate(flops=80_000_000_000, bytes_accessed=40_000_000, transcendentals=40_000_000),
    )(h1, dy, x, g1, g2, wqkv, w1, w2, wo)


def copy_kernel(*refs):
    count = (len(refs) - 2) // 3
    srcs, dsts, bufs, in_sem, out_sem = refs[:count], refs[count:2 * count], refs[2 * count:3 * count], refs[-2], refs[-1]
    reads = [pltpu.make_async_copy(src, buf, in_sem.at[n]) for n, (src, buf) in enumerate(zip(srcs, bufs))]
    writes = [pltpu.make_async_copy(buf, dst, out_sem.at[n]) for n, (dst, buf) in enumerate(zip(dsts, bufs))]
    for copy in reads:
        copy.start()
    for read, write in zip(reads, writes):
        read.wait()
        write.start()
    for copy in writes:
        copy.wait()


def copy_out(*arrays):
    hbm = pl.BlockSpec(memory_space=pl.ANY)
    return pl.pallas_call(
        copy_kernel,
        name="copy_out",
        out_shape=[jax.ShapeDtypeStruct(a.shape, a.dtype) for a in arrays],
        in_specs=[hbm] * len(arrays),
        out_specs=[hbm] * len(arrays),
        scratch_shapes=[pltpu.VMEM(a.shape, a.dtype) for a in arrays] + [pltpu.SemaphoreType.DMA((len(arrays),))] * 2,
        compiler_params=pltpu.CompilerParams(vmem_limit_bytes=67043328),
    )(*arrays)


def solution(mesh):
    row_spec = P(('dp', 'tp'), None)
    in_specs = (row_spec, row_spec, row_spec, P(None), P(None), P(None, 'tp'), P('tp', None, None), P(None, 'tp'), P('tp', None))
    out_specs = (row_spec, P('dp', 'tp'), P(('dp', 'tp'), None, None), P('dp', 'tp'), P(('dp', 'tp'), None))

    def device_step(in_rows, mid_rows, gout_rows, ln1_gain, ln2_gain, wqkv_loc, wout_loc, wfc1_loc, wfc2_loc):
        grad_in, grad_wqkv, grad_wout, grad_wfc1, grad_wfc2 = copy_out(*layer_grads(mid_rows, gout_rows, in_rows, ln1_gain.reshape(1, 1024), ln2_gain.reshape(1, 1024), wqkv_loc, wfc1_loc, wfc2_loc, wout_loc.reshape(256, 1024)))
        return grad_in, grad_wqkv, grad_wout.reshape(4, 64, 1024), grad_wfc1, grad_wfc2

    return jax.shard_map(device_step, mesh=mesh, in_specs=in_specs, out_specs=out_specs, check_vma=False)
```
